256 devices in a mesh: gx: 4 (over z_lo), gy: 8 (over y, core), gz: 8 (over z_hi, x).
Axes of the slice: x: 4, y: 4, z: 8 (z_hi: 2, z_lo: 4; z = z_hi * 4 + z_lo), core: 2. Of those that a mesh axis runs over, the one named last changes fastest.
Arguments:
- rhs: float32 [128, 256, 1024], P('gx', 'gy', 'gz'), may hold values from -8 to 8
- accumulation: float32 [128, 256, 1024], P('gx', 'gy', 'gz'), may hold values from 0.05 to 0.5
- permeability: float32 [3, 128, 256, 1024], P(None, 'gx', 'gy', 'gz'), may hold values from 0.1 to 10
- nnc_cell: int32 [4, 8, 8, 512], P('gx', 'gy', 'gz'), may hold values from 0 to 4095, as said below
- nnc_remote: int32 [4, 8, 8, 512], P('gx', 'gy', 'gz'), may hold values from 0 to 32767, as said below
- nnc_mask: int32 [4, 8, 8, 512], P('gx', 'gy', 'gz'), may hold values from 0 to 1, as said below
- nnc_trans: float32 [4, 8, 8, 512], P('gx', 'gy', 'gz'), may hold values from 0.5 to 4
Outputs:
- correction: float32 [128, 256, 1024], P('gx', 'gy', 'gz')
The draws below stay inside these ranges and needn't reach their ends.
Inputs may be any that keep to these rules, and one draw needn't show every extreme that they name: `nnc_cell`: x * 128 + z of a cell with local x and local layer z on the device's first y layer. `nnc_remote`: x * 1024 + z2, with x the same local x as nnc_cell and z2 a global layer, naming a cell on the last y layer of the device below in y. `nnc_mask`: each device's live slots come first, then zeros; every slot is 0 on devices of the first gy index; the device last along every axis has all slots live.
All inputs are finite; a program needn't handle non-finite values.
Results may differ from the reference program's by a relative error of at most 0.00002.
Values sent between devices are 32-bit elements; how exact they have to be, the bound alone decides.
No kernel may reach another device: no remote copies, remote signals or barrier semaphores. Data moves between devices by JAX's collectives and lax.ppermute only.
A program may use at most 64 MiB of HBM per device.

```python
import math
import jax
import jax.numpy as jnp

CX = 32
CY = 32
CZ = 128
FSLOT = 512
SWEEPS = 6
TILES_X = 4
TILES_Y = 8
TILES_Z = 8
NX = 128
NY = 256
NZ = 1024


def fault_lists(key):
    base = jax.random.fold_in(key, 17)
    keys = jax.random.split(base, 5)
    shape = (TILES_X, TILES_Y, TILES_Z, FSLOT)
    column_x = jax.random.randint(keys[0], shape, 0, CX)
    layer_z = jax.random.randint(keys[1], shape, 0, CZ)
    throw = jax.random.randint(keys[2], (TILES_X, TILES_Y, TILES_Z, 1), -(TILES_Z - 1), TILES_Z)
    jitter = jax.random.randint(keys[3], shape, -(CZ // 2), CZ // 2 + 1)
    tile_z = jnp.arange(TILES_Z, dtype=jnp.int32).reshape(1, 1, TILES_Z, 1)
    remote_z = jnp.clip(tile_z * CZ + layer_z + throw * CZ + jitter, 0, NZ - 1)
    live = jax.random.randint(keys[4], (TILES_X, TILES_Y, TILES_Z, 1), FSLOT // 4, FSLOT + 1)
    live = live.at[TILES_X - 1, TILES_Y - 1, TILES_Z - 1, 0].set(FSLOT)
    tile_y = jnp.arange(TILES_Y, dtype=jnp.int32).reshape(1, TILES_Y, 1, 1)
    slots = jnp.arange(FSLOT, dtype=jnp.int32).reshape(1, 1, 1, FSLOT)
    mask = ((slots < live) & (tile_y > 0)).astype(jnp.int32)
    cells = (column_x * CZ + layer_z).astype(jnp.int32)
    remote = (column_x * NZ + remote_z).astype(jnp.int32)
    return (cells, remote, mask)


def draw_nnc_cell(key, part):
    return fault_lists(key)[0]


def draw_nnc_remote(key, part):
    return fault_lists(key)[1]


def draw_nnc_mask(key, part):
    return fault_lists(key)[2]


def block_scale(stream_key, shape, cuts, low, top_value):
    loudness = 1.0
    for axis_at, parts in cuts:
        steps = jax.random.uniform(jax.random.fold_in(jax.random.fold_in(stream_key, 6), axis_at), (parts,), jnp.float32, low / len(cuts), top_value / len(cuts))
        loudness = loudness * jnp.repeat(jnp.exp(steps), shape[axis_at] // parts).reshape((-1,) + (1,) * (len(shape) - 1 - axis_at))
    return loudness


def normal_values(own_key, extent, width, reach, cuts=(), kind=jnp.bfloat16):
    drawn = width * jax.random.normal(own_key, extent, jnp.float32)
    if cuts:
        drawn = drawn * block_scale(own_key, extent, cuts, -0.22, 0.18)
    return jnp.clip(drawn, -reach, reach).astype(kind)


def setup_inputs(seed: int = 0) -> dict:
    streams_of = jax.random.split(jax.random.key(seed), 8)
    return {
        "rhs": normal_values(streams_of[0], (NX, NY, NZ), 1.0, 8.0, ((0, 4), (1, 8), (2, 8)), jnp.float32),
        "accumulation": jnp.clip(jnp.exp(math.log(0.5) - 2.3025851 * jax.random.uniform(streams_of[1], (NX, NY, NZ), jnp.float32) ** block_scale(streams_of[1], (NX, NY, NZ), ((0, 4), (1, 8), (2, 8)), -0.2, 0.2)), 0.05, 0.5),
        "permeability": jnp.clip(jnp.exp(math.log(10.0) - 4.6051702 * jax.random.uniform(streams_of[2], (3, NX, NY, NZ), jnp.float32) ** block_scale(streams_of[2], (3, NX, NY, NZ), ((1, 4), (2, 8), (3, 8)), -0.2, 0.2)), 0.1, 10.0),
        "nnc_cell": draw_nnc_cell(jax.random.fold_in(streams_of[7], 71), 0),
        "nnc_remote": draw_nnc_remote(jax.random.fold_in(streams_of[7], 71), 0),
        "nnc_mask": draw_nnc_mask(jax.random.fold_in(streams_of[7], 71), 0),
        "nnc_trans": jnp.clip(jnp.exp(math.log(4.0) - 2.0794415 * jax.random.uniform(streams_of[6], (TILES_X, TILES_Y, TILES_Z, FSLOT), jnp.float32) ** block_scale(streams_of[6], (TILES_X, TILES_Y, TILES_Z, FSLOT), ((0, 4), (1, 8), (2, 8)), -0.2, 0.2)), 0.5, 4.0),
    }


lam_low = 0.1
lam_high = 2.0


def harmonic(left, right):
    return 2.0 * (left * right) / (left + right)


def neighbours(padded):
    return (padded[2:, 1:-1, 1:-1], padded[:-2, 1:-1, 1:-1],
            padded[1:-1, 2:, 1:-1], padded[1:-1, :-2, 1:-1],
            padded[1:-1, 1:-1, 2:], padded[1:-1, 1:-1, :-2])


def reference(rhs, accumulation, permeability, nnc_cell, nnc_remote, nnc_mask, nnc_trans):
    padded_perm = jnp.pad(permeability, ((0, 0), (1, 1), (1, 1), (1, 1)))
    transmit = []
    for index in range(6):
        axis_perm = neighbours(padded_perm[index // 2])[index]
        transmit.append(harmonic(permeability[index // 2], axis_perm))
    shape = nnc_cell.shape
    tile_x = jnp.arange(shape[0], dtype=jnp.int32).reshape(-1, 1, 1, 1)
    tile_y = jnp.arange(shape[1], dtype=jnp.int32).reshape(1, -1, 1, 1)
    tile_z = jnp.arange(shape[2], dtype=jnp.int32).reshape(1, 1, -1, 1)
    total = NX * NY * NZ
    cell_a = ((tile_x * CX + nnc_cell // CZ) * NY + tile_y * CY) * NZ + tile_z * CZ + nnc_cell % CZ
    cell_b = ((tile_x * CX + nnc_remote // NZ) * NY + tile_y * CY - 1) * NZ + nnc_remote % NZ
    cell_b = jnp.where(tile_y > 0, cell_b, 0)
    cell_a = cell_a.reshape(-1).astype(jnp.int32)
    cell_b = cell_b.reshape(-1).astype(jnp.int32)
    weight = (nnc_trans * nnc_mask.astype(jnp.float32)).reshape(-1)

    def operate(field):
        beside = neighbours(jnp.pad(field, 1))
        result = accumulation * field
        for index in range(6):
            result = result + transmit[index] * (field - beside[index])
        flat = field.reshape(-1)
        flux = weight * (flat[cell_a] - flat[cell_b])
        extra = jnp.zeros((total,), jnp.float32).at[cell_a].add(flux).at[cell_b].add(-flux)
        return result + extra.reshape(field.shape)

    diag_extra = jnp.zeros((total,), jnp.float32).at[cell_a].add(weight).at[cell_b].add(weight)
    diagonal = accumulation + sum(transmit) + diag_extra.reshape(rhs.shape)
    inverse = 1.0 / diagonal
    theta = (lam_high + lam_low) / 2.0
    delta = (lam_high - lam_low) / 2.0
    sigma = theta / delta
    rho_prev = 1.0 / sigma
    residual = rhs
    direction = inverse * residual / theta
    correction = jnp.zeros_like(rhs)
    for sweep in range(SWEEPS):
        correction = correction + direction
        if sweep < SWEEPS - 1:
            residual = residual - operate(direction)
            rho_next = 1.0 / (2.0 * sigma - rho_prev)
            direction = rho_next * rho_prev * direction + (2.0 * rho_next / delta) * inverse * residual
            rho_prev = rho_next
    return correction
```

```python
import jax
import jax.numpy as jnp
from jax import lax
from jax.experimental import pallas as pl
from jax.experimental.pallas import tpu as pltpu
from jax.sharding import PartitionSpec as P

SWEEPS = 6
lam_low = 0.1
lam_high = 2.0
theta = (lam_high + lam_low) / 2.0
delta = (lam_high - lam_low) / 2.0
sigma = theta / delta

H = 8
f32 = jnp.float32
bf16 = jnp.bfloat16


def harmonic(left, right):
    total = left + right
    live = total > 0.0
    return jnp.where(live, 2.0 * (left * right) / jnp.where(live, total, 1.0), 0.0)


def split3(v):
    hi = v.astype(bf16).astype(f32)
    rest = v - hi
    mid = rest.astype(bf16).astype(f32)
    return hi, mid, rest - mid


def dot(a, b, dims):
    return lax.dot_general(a, b, (dims, ((), ())), preferred_element_type=f32)


def lane_iota(shape):
    return lax.broadcasted_iota(jnp.int32, shape, len(shape) - 1)


def hits(col_ref, q, which):
    codes = col_ref[q, :, which : which + 1]
    return lane_iota((codes.shape[0], 128)).astype(f32) == codes


def rows_hit(row_ref, q, which, count):
    codes = row_ref[q, which : which + 1, :]
    rows = lax.broadcasted_iota(jnp.int32, (count, codes.shape[1]), 0).astype(f32)
    return jnp.where(rows == codes, 1.0, 0.0).astype(bf16)


def scatter(u, lane_hit, row_hit):
    parts = [jnp.where(lane_hit, p, 0.0).astype(bf16) for p in split3(u)]
    out = dot(row_hit, jnp.concatenate(parts, axis=1), ((1,), (0,)))
    return out[:, :128] + out[:, 128:256] + out[:, 256:]


def gather(table, lane_hit, codes):
    rows = table.shape[0]
    pick = jnp.where(lane_hit, 1.0, 0.0).astype(bf16)
    parts = [p.astype(bf16) for p in split3(table)]
    if rows % 128 == 0:
        got = sum(dot(pick, p, ((1,), (1,))) for p in parts)
        lanes = lane_iota(got.shape)
    else:
        got = dot(pick, jnp.concatenate(parts, axis=0), ((1,), (1,)))
        lanes = lane_iota(got.shape) % rows
    return jnp.sum(jnp.where(lanes.astype(f32) == codes, got, 0.0), axis=1, keepdims=True)


def pack_faces(faces, slab, x):
    cx, half = 32, faces.shape[0]
    lane = lane_iota(faces.shape)
    for part in range(2):
        rows = slab[part * half : (part + 1) * half]
        faces = jnp.where(lane == 2 * cx * part + x, rows[:, 0:1], faces)
        faces = jnp.where(lane == 2 * cx * part + cx + x, rows[:, 127:128], faces)
    return faces


def unpacked(low_faces, high_faces, slab, x):
    cx = 32
    lane = lane_iota(slab.shape)

    def column(faces, first, to):
        return jnp.concatenate(
            [pltpu.roll(faces, (to - first - 2 * cx * part - x) % 128, 1) for part in range(2)],
            axis=0,
        )

    low = jnp.where(lane == 0, column(low_faces, cx, 128), pltpu.roll(slab, 1, 1))
    high = jnp.where(lane == 127, column(high_faces, 0, 127 + 128), pltpu.roll(slab, 127, 1))
    return low, high


def put_partials(out_ref, base, tiles, q, col_ref, row_ref, u, cx):
    sums = scatter(u, hits(col_ref, q, 2), rows_hit(row_ref, q, 1, tiles * cx))
    for t in range(tiles):
        out_ref[t, base + q * cx : base + (q + 1) * cx, :] = sums[t * cx : (t + 1) * cx]


def first_kernel(own_k, before, after, col_ref, row_ref, out_ref):
    tiles = out_ref.shape[0]
    cx = own_k.shape[1]

    def body(x, faces):
        at = pl.multiple_of((4 * cx + x) * H, H)
        slab = jnp.concatenate([before[pl.ds(at, H), :], own_k[2, x], after[pl.ds(at, H), :]], axis=0)
        return pack_faces(faces, slab, x)

    half = (own_k.shape[2] + 2 * H) // 2
    faces = lax.fori_loop(0, cx, body, jnp.zeros((half, 128), f32))
    for t in range(tiles):
        out_ref[t, 0:half, :] = faces
    for q in range(2):
        put_partials(out_ref, half, tiles, q, col_ref, row_ref, col_ref[q, :, 4:5], cx)


def emit(a8_ref, planes, faces, col_ref, row_ref):
    tiles = a8_ref.shape[0]
    cx = planes.shape[1]
    half = faces.shape[0]
    for t in range(tiles):
        a8_ref[t, 0:cx, :] = planes[0]
        a8_ref[t, cx : 2 * cx, :] = planes[2]
        a8_ref[t, 2 * cx : 2 * cx + half, :] = faces
    for q in range(2):
        near = gather(planes[1 + 2 * q], hits(col_ref, q, 0), col_ref[q, :, 1:2])
        put_partials(a8_ref, 2 * cx + half, tiles, q, col_ref, row_ref, col_ref[q, :, 4:5] * near, cx)


def keep_planes(planes, slab, x):
    last = slab.shape[0] - H - 1
    for n, y in enumerate((H - 1, H, last, last + 1)):
        planes[n, pl.ds(x, 1), :] = slab[y : y + 1, :]


def with_fault(total, fault, x):
    y = lax.broadcasted_iota(jnp.int32, total.shape, 0)
    last = total.shape[0] - H - 1
    extra = jnp.zeros_like(total)
    for n, at in enumerate((H - 1, H, last, last + 1)):
        extra = jnp.where(y == at, fault[n, pl.ds(x, 1), :], extra)
    return total + extra


def neighbour_faces(l_ref, a8, base, half):
    tiles = a8.shape[0]
    l = l_ref[0]
    low = a8[jnp.maximum(l - 1, 0), base : base + half, :]
    high = a8[jnp.minimum(l + 1, tiles - 1), base : base + half, :]
    return low, high


def setup_kernel(l_ref, rhs, acc, perm, before, after, kx_low, kx_high, a8, col_ref, row_ref,
                 inv, z_out, d_out, tx, tym, typ, tzm, tzp, xf, a8_out, planes, fault):
    cx, cy = rhs.shape[0], rhs.shape[1]
    ye = cy + 2 * H
    half = ye // 2
    tiles = a8.shape[0]
    l = l_ref[0]
    low_faces, high_faces = neighbour_faces(l_ref, a8, 0, half)
    low_faces = jnp.where(l > 0, low_faces, 0.0)
    high_faces = jnp.where(l < tiles - 1, high_faces, 0.0)
    for q in range(2):
        base = half + q * cx
        far = a8[0, base : base + cx, :]
        for t in range(1, tiles):
            far = far + a8[t, base : base + cx, :]
        fault[2 * q] = far
        near = scatter(col_ref[q, :, 4:5], hits(col_ref, q, 0), rows_hit(row_ref, q, 0, cx))
        fault[2 * q + 1] = near

    def ext(a, own, x):
        at = pl.multiple_of((a * cx + x) * H, H)
        return jnp.concatenate([before[pl.ds(at, H), :], own, after[pl.ds(at, H), :]], axis=0)

    def body(x, carry):
        faces, t_low, kx = carry
        nxt = jnp.minimum(x + 1, cx - 1)
        kx_next = jnp.where(x == cx - 1, kx_high[...], ext(2, perm[0, nxt], nxt))
        ky = ext(3, perm[1, x], x)
        kz = ext(4, perm[2, x], x)
        t_high = harmonic(kx, kx_next)
        ym = harmonic(ky, pltpu.roll(ky, 1, 0))
        yp = harmonic(ky, pltpu.roll(ky, ye - 1, 0))
        kz_low, kz_high = unpacked(low_faces, high_faces, kz, x)
        zm = harmonic(kz, kz_low)
        zp = harmonic(kz, kz_high)
        diag = ext(1, acc[x], x) + t_low + t_high + ym + yp + zm + zp
        diag = with_fault(diag, fault, x)
        live = diag > 0.0
        inverse = jnp.where(live, 1.0 / jnp.where(live, diag, 1.0), 0.0)
        z = inverse * ext(0, rhs[x], x)
        d = z / theta
        inv[x] = inverse
        z_out[x] = z
        d_out[x] = d
        tx[x] = t_low
        tx[x + 1] = t_high
        tym[x] = ym
        typ[x] = yp
        tzm[x] = zm
        tzp[x] = zp
        keep_planes(planes, d, x)
        return pack_faces(faces, d, x), t_high, kx_next

    kx0 = ext(2, perm[0, 0], 0)
    init = (jnp.zeros((half, 128), f32), harmonic(kx_low[...], kx0), kx0)
    faces, _, _ = lax.fori_loop(0, cx, body, init)
    xf[0] = d_out[0]
    xf[1] = d_out[cx - 1]
    emit(a8_out, planes, faces, col_ref, row_ref)


def sweep_kernel(c1, c2, first, last, l_ref, d_in, z_in, *refs):
    refs = list(refs)
    corr_in = None if first else refs.pop(0)
    xlow, xhigh, a8, inv, tx, tym, typ, tzm, tzp, col_ref, row_ref = refs[:11]
    outs = refs[11:]
    if last:
        corr_out, fault = outs
    else:
        d_out, z_out, corr_out, xf, a8_out, planes, fault = outs
    cx, ye = d_in.shape[0], d_in.shape[1]
    cy = ye - 2 * H
    half = ye // 2
    tiles = a8.shape[0]
    low_faces, high_faces = neighbour_faces(l_ref, a8, 2 * cx, half)
    for q in range(2):
        base = 2 * cx + half + q * cx
        far = a8[0, base : base + cx, :]
        for t in range(1, tiles):
            far = far + a8[t, base : base + cx, :]
        fault[2 * q] = far
        table = jnp.concatenate([a8[t, q * cx : (q + 1) * cx, :] for t in range(tiles)], axis=0)
        got = gather(table, hits(col_ref, q, 2), col_ref[q, :, 3:4])
        fault[2 * q + 1] = scatter(
            col_ref[q, :, 4:5] * got, hits(col_ref, q, 0), rows_hit(row_ref, q, 0, cx)
        )

    def body(x, carry):
        faces, d_prev, d = carry
        d_next = jnp.where(x == cx - 1, xhigh[...], d_in[jnp.minimum(x + 1, cx - 1)])
        z_low, z_high = unpacked(low_faces, high_faces, d, x)
        flow = tx[x] * d_prev + tx[x + 1] * d_next
        flow = flow + (tym[x] * pltpu.roll(d, 1, 0) + typ[x] * pltpu.roll(d, ye - 1, 0))
        flow = flow + (tzm[x] * z_low + tzp[x] * z_high)
        flow = with_fault(flow, fault, x)
        z = z_in[x] - d + inv[x] * flow
        new = c1 * d + c2 * z
        before = d[H : H + cy] if first else corr_in[x]
        corr_out[x] = before + new[H : H + cy]
        if last:
            return faces, d, d_next
        d_out[x] = new
        z_out[x] = z
        keep_planes(planes, new, x)
        return pack_faces(faces, new, x), d, d_next

    init = (jnp.zeros((half, 128), f32), xlow[...], d_in[0])
    faces, _, _ = lax.fori_loop(0, cx, body, init)
    if not last:
        xf[0] = d_out[0]
        xf[1] = d_out[cx - 1]
        emit(a8_out, planes, faces, col_ref, row_ref)


VMEM = pl.BlockSpec(memory_space=pltpu.VMEM)
SMEM = pl.BlockSpec(memory_space=pltpu.SMEM)


def steps(axis):
    peers = lax.axis_size(axis)
    up = [(i, i + 1) for i in range(peers - 1)]
    return up, [(j, i) for i, j in up]


def local(rhs, accumulation, permeability, nnc_cell, nnc_remote, nnc_mask, nnc_trans):
    cx, cy, cz = rhs.shape
    tiles = lax.axis_size("gz")
    slots = nnc_cell.shape[-1]
    ye = cy + 2 * H
    half = ye // 2
    up_y, down_y = steps("gy")
    up_x, down_x = steps("gx")

    def struct(*shape):
        return jax.ShapeDtypeStruct(shape, f32)

    weight = nnc_trans.reshape(-1) * nnc_mask.reshape(-1).astype(f32)
    mine = jnp.stack([nnc_cell.reshape(-1).astype(f32), nnc_remote.reshape(-1).astype(f32), weight])
    bottom = [rhs[None, :, :H], accumulation[None, :, :H], permeability[:, :, :H]]
    top = [rhs[None, :, cy - H :], accumulation[None, :, cy - H :], permeability[:, :, cy - H :]]
    bottom = jnp.concatenate(bottom, axis=0).reshape(-1, cz)
    top = jnp.concatenate(top, axis=0).reshape(-1, cz)
    flat = jnp.pad(mine.reshape(-1, cz), ((0, 4), (0, 0)))
    before = lax.ppermute(top, "gy", up_y)
    after = lax.ppermute(jnp.concatenate([bottom, flat], axis=0), "gy", down_y)
    count = bottom.shape[0]
    above = after[count : count + 3 * slots // cz].reshape(3, slots)
    lists = jnp.stack([mine, above])
    cell = lists[:, 0].astype(jnp.int32)
    remote = lists[:, 1].astype(jnp.int32)
    column = cz * tiles
    far_z = remote % column
    own_x = (cell // cz).astype(f32)
    far_code = ((far_z // cz) * cx + remote // column).astype(f32)
    col = jnp.stack(
        [(cell % cz).astype(f32), own_x, (far_z % cz).astype(f32), far_code, lists[:, 2]], axis=-1
    )
    row = jnp.stack([own_x, far_code], axis=1)

    l = lax.axis_index("gz").reshape(1).astype(jnp.int32)
    a8 = pl.pallas_call(
        first_kernel, out_shape=struct(tiles, half + 2 * cx, cz), in_specs=[VMEM] * 5, out_specs=VMEM
    )(permeability, before, after, col, row)

    def kx_face(x):
        at = (2 * cx + x) * H
        return jnp.concatenate([before[at : at + H], permeability[0, x], after[at : at + H]], axis=0)

    kx_low = lax.ppermute(kx_face(cx - 1), "gx", up_x)
    kx_high = lax.ppermute(kx_face(0), "gx", down_x)
    a8 = lax.all_to_all(a8, "gz", 0, 0, tiled=True)

    big = struct(cx, ye, cz)
    tall = struct(cx + 1, ye, cz)
    sent = struct(tiles, 4 * cx + half, cz)
    edge = struct(2, ye, cz)
    scratch = [pltpu.VMEM((4, cx, cz), f32)]
    inv, z, d, tx, tym, typ, tzm, tzp, xf, a8 = pl.pallas_call(
        setup_kernel,
        out_shape=(big, big, big, tall, big, big, big, big, edge, sent),
        in_specs=[SMEM] + [VMEM] * 10,
        out_specs=(VMEM,) * 10,
        scratch_shapes=scratch * 2,
    )(l, rhs, accumulation, permeability, before, after, kx_low, kx_high, a8, col, row)

    rho = 1.0 / sigma
    corr = None
    for sweep in range(1, SWEEPS):
        first, last = sweep == 1, sweep == SWEEPS - 1
        rho_next = 1.0 / (2.0 * sigma - rho)
        c1, c2 = rho_next * rho, 2.0 * rho_next / delta
        rho = rho_next
        xlow = lax.ppermute(xf[1], "gx", up_x)
        xhigh = lax.ppermute(xf[0], "gx", down_x)
        a8 = lax.all_to_all(a8, "gz", 0, 0, tiled=True)
        args = [l, d, z] + ([] if first else [corr])
        args += [xlow, xhigh, a8, inv, tx, tym, typ, tzm, tzp, col, row]

        def kernel(*refs, c1=c1, c2=c2, first=first, last=last):
            sweep_kernel(c1, c2, first, last, *refs)

        small = struct(cx, cy, cz)
        out = pl.pallas_call(
            kernel,
            out_shape=small if last else (big, big, small, edge, sent),
            in_specs=[SMEM] + [VMEM] * (len(args) - 1),
            out_specs=VMEM if last else (VMEM,) * 5,
            scratch_shapes=scratch if last else scratch * 2,
        )(*args)
        if last:
            corr = out
        else:
            d, z, corr, xf, a8 = out
    return corr


def solution(mesh):
    split = P("gx", "gy", "gz")
    slots = P("gx", "gy", "gz", None)
    return jax.shard_map(
        local,
        mesh=mesh,
        in_specs=(split, split, P(None, "gx", "gy", "gz"), slots, slots, slots, slots),
        out_specs=split,
        check_vma=False,
    )
```

```python
import jax
import jax.numpy as jnp
from jax import lax
from jax.experimental import pallas as pl
from jax.experimental.pallas import tpu as pltpu
from jax.sharding import PartitionSpec as P

SWEEPS = 6
lam_low = 0.1
lam_high = 2.0
theta = (lam_high + lam_low) / 2.0
delta = (lam_high - lam_low) / 2.0
sigma = theta / delta

H = 8
f32 = jnp.float32
bf16 = jnp.bfloat16


def harmonic(left, right):
    total = left + right
    live = total > 0.0
    return jnp.where(live, 2.0 * (left * right) / jnp.where(live, total, 1.0), 0.0)


def split3(v):
    hi = v.astype(bf16).astype(f32)
    rest = v - hi
    mid = rest.astype(bf16).astype(f32)
    return hi, mid, rest - mid


def dot(a, b, dims):
    return lax.dot_general(a, b, (dims, ((), ())), preferred_element_type=f32)


def lane_iota(shape):
    return lax.broadcasted_iota(jnp.int32, shape, len(shape) - 1)


def hits(col_ref, q, which):
    codes = col_ref[q, :, which : which + 1]
    return lane_iota((codes.shape[0], 128)).astype(f32) == codes


def rows_hit(row_ref, q, which, count):
    codes = row_ref[q, which : which + 1, :]
    rows = lax.broadcasted_iota(jnp.int32, (count, codes.shape[1]), 0).astype(f32)
    return jnp.where(rows == codes, 1.0, 0.0).astype(bf16)


def scatter(u, lane_hit, row_hit):
    parts = [jnp.where(lane_hit, p, 0.0).astype(bf16) for p in split3(u)]
    out = dot(row_hit, jnp.concatenate(parts, axis=1), ((1,), (0,)))
    return out[:, :128] + out[:, 128:256] + out[:, 256:]


def gather(table, lane_hit, codes):
    rows = table.shape[0]
    pick = jnp.where(lane_hit, 1.0, 0.0).astype(bf16)
    parts = [p.astype(bf16) for p in split3(table)]
    if rows % 128 == 0:
        got = sum(dot(pick, p, ((1,), (1,))) for p in parts)
        lanes = lane_iota(got.shape)
    else:
        got = dot(pick, jnp.concatenate(parts, axis=0), ((1,), (1,)))
        lanes = lane_iota(got.shape) % rows
    return jnp.sum(jnp.where(lanes.astype(f32) == codes, got, 0.0), axis=1, keepdims=True)


def pack_faces(faces, slab, x):
    cx, half = 32, faces.shape[0]
    lane = lane_iota(faces.shape)
    for part in range(2):
        rows = slab[part * half : (part + 1) * half]
        faces = jnp.where(lane == 2 * cx * part + x, rows[:, 0:1], faces)
        faces = jnp.where(lane == 2 * cx * part + cx + x, rows[:, 127:128], faces)
    return faces


def unpacked(low_faces, high_faces, slab, x):
    cx = 32
    lane = lane_iota(slab.shape)

    def column(faces, first, to):
        return jnp.concatenate(
            [pltpu.roll(faces, (to - first - 2 * cx * part - x) % 128, 1) for part in range(2)],
            axis=0,
        )

    low = jnp.where(lane == 0, column(low_faces, cx, 128), pltpu.roll(slab, 1, 1))
    high = jnp.where(lane == 127, column(high_faces, 0, 127 + 128), pltpu.roll(slab, 127, 1))
    return low, high


def put_partials(out_ref, base, tiles, q, col_ref, row_ref, u, cx):
    sums = scatter(u, hits(col_ref, q, 2), rows_hit(row_ref, q, 1, tiles * cx))
    for t in range(tiles):
        out_ref[t, base + q * cx : base + (q + 1) * cx, :] = sums[t * cx : (t + 1) * cx]


def first_kernel(own_k, before, after, col_ref, row_ref, out_ref, kx_first, kx_last):
    tiles = out_ref.shape[0]
    cx = own_k.shape[1]

    def body(x, faces):
        at = pl.multiple_of((4 * cx + x) * H, H)
        slab = jnp.concatenate([before[pl.ds(at, H), :], own_k[2, x], after[pl.ds(at, H), :]], axis=0)
        return pack_faces(faces, slab, x)

    for x, face in ((0, kx_first), (cx - 1, kx_last)):
        at = (2 * cx + x) * H
        face[...] = jnp.concatenate([before[at : at + H, :], own_k[0, x], after[at : at + H, :]], axis=0)
    half = (own_k.shape[2] + 2 * H) // 2
    faces = lax.fori_loop(0, cx, body, jnp.zeros((half, 128), f32), unroll=4)
    for t in range(tiles):
        out_ref[t, 0:half, :] = faces
    for q in range(2):
        put_partials(out_ref, half, tiles, q, col_ref, row_ref, col_ref[q, :, 4:5], cx)


def emit(a8_ref, planes, faces, col_ref, row_ref):
    tiles = a8_ref.shape[0]
    cx = planes.shape[1]
    half = faces.shape[0]
    for t in range(tiles):
        a8_ref[t, 0:cx, :] = planes[0]
        a8_ref[t, cx : 2 * cx, :] = planes[2]
        a8_ref[t, 2 * cx : 2 * cx + half, :] = faces
    for q in range(2):
        near = gather(planes[1 + 2 * q], hits(col_ref, q, 0), col_ref[q, :, 1:2])
        put_partials(a8_ref, 2 * cx + half, tiles, q, col_ref, row_ref, col_ref[q, :, 4:5] * near, cx)


def keep_planes(planes, slab, x):
    last = slab.shape[0] - H - 1
    for n, y in enumerate((H - 1, H, last, last + 1)):
        planes[n, pl.ds(x, 1), :] = slab[y : y + 1, :]


def with_fault(total, fault, x):
    y = lax.broadcasted_iota(jnp.int32, total.shape, 0)
    last = total.shape[0] - H - 1
    extra = jnp.zeros_like(total)
    for n, at in enumerate((H - 1, H, last, last + 1)):
        extra = jnp.where(y == at, fault[n, pl.ds(x, 1), :], extra)
    return total + extra


def neighbour_faces(l_ref, a8, base, half):
    tiles = a8.shape[0]
    l = l_ref[0]
    low = a8[jnp.maximum(l - 1, 0), base : base + half, :]
    high = a8[jnp.minimum(l + 1, tiles - 1), base : base + half, :]
    return low, high


def setup_kernel(l_ref, rhs, acc, perm, before, after, kx_low, kx_high, a8, col_ref, row_ref,
                 inv, z_out, d_out, tx, tym, typ, tzm, tzp, d_first, d_last, a8_out, planes, fault):
    cx, cy = rhs.shape[0], rhs.shape[1]
    ye = cy + 2 * H
    half = ye // 2
    tiles = a8.shape[0]
    l = l_ref[0]
    low_faces, high_faces = neighbour_faces(l_ref, a8, 0, half)
    low_faces = jnp.where(l > 0, low_faces, 0.0)
    high_faces = jnp.where(l < tiles - 1, high_faces, 0.0)
    for q in range(2):
        base = half + q * cx
        far = a8[0, base : base + cx, :]
        for t in range(1, tiles):
            far = far + a8[t, base : base + cx, :]
        fault[2 * q] = far
        near = scatter(col_ref[q, :, 4:5], hits(col_ref, q, 0), rows_hit(row_ref, q, 0, cx))
        fault[2 * q + 1] = near

    def ext(a, own, x):
        at = pl.multiple_of((a * cx + x) * H, H)
        return jnp.concatenate([before[pl.ds(at, H), :], own, after[pl.ds(at, H), :]], axis=0)

    def body(x, carry):
        faces, t_low, kx = carry
        nxt = jnp.minimum(x + 1, cx - 1)
        kx_next = jnp.where(x == cx - 1, kx_high[...], ext(2, perm[0, nxt], nxt))
        ky = ext(3, perm[1, x], x)
        kz = ext(4, perm[2, x], x)
        t_high = harmonic(kx, kx_next)
        ym = harmonic(ky, pltpu.roll(ky, 1, 0))
        yp = harmonic(ky, pltpu.roll(ky, ye - 1, 0))
        kz_low, kz_high = unpacked(low_faces, high_faces, kz, x)
        zm = harmonic(kz, kz_low)
        zp = harmonic(kz, kz_high)
        diag = ext(1, acc[x], x) + t_low + t_high + ym + yp + zm + zp
        diag = with_fault(diag, fault, x)
        live = diag > 0.0
        inverse = jnp.where(live, 1.0 / jnp.where(live, diag, 1.0), 0.0)
        z = inverse * ext(0, rhs[x], x)
        d = z / theta
        inv[x] = inverse
        z_out[x] = z
        d_out[x] = d
        tx[x] = t_low
        tx[x + 1] = t_high
        tym[x] = ym
        typ[x] = yp
        tzm[x] = zm
        tzp[x] = zp
        keep_planes(planes, d, x)
        return pack_faces(faces, d, x), t_high, kx_next

    kx0 = ext(2, perm[0, 0], 0)
    init = (jnp.zeros((half, 128), f32), harmonic(kx_low[...], kx0), kx0)
    faces, _, _ = lax.fori_loop(0, cx, body, init, unroll=4)
    d_first[...] = d_out[0]
    d_last[...] = d_out[cx - 1]
    emit(a8_out, planes, faces, col_ref, row_ref)


def sweep_kernel(c1, c2, first, last, l_ref, d_in, z_in, *refs):
    refs = list(refs)
    corr_in = None if first else refs.pop(0)
    xlow, xhigh, a8, inv, tx, tym, typ, tzm, tzp, col_ref, row_ref = refs[:11]
    outs = refs[11:]
    if last:
        corr_out, fault = outs
    else:
        d_out, z_out, corr_out, d_first, d_last, a8_out, planes, fault = outs
    cx, ye = d_in.shape[0], d_in.shape[1]
    cy = ye - 2 * H
    half = ye // 2
    tiles = a8.shape[0]
    low_faces, high_faces = neighbour_faces(l_ref, a8, 2 * cx, half)
    for q in range(2):
        base = 2 * cx + half + q * cx
        far = a8[0, base : base + cx, :]
        for t in range(1, tiles):
            far = far + a8[t, base : base + cx, :]
        fault[2 * q] = far
        table = jnp.concatenate([a8[t, q * cx : (q + 1) * cx, :] for t in range(tiles)], axis=0)
        got = gather(table, hits(col_ref, q, 2), col_ref[q, :, 3:4])
        fault[2 * q + 1] = scatter(
            col_ref[q, :, 4:5] * got, hits(col_ref, q, 0), rows_hit(row_ref, q, 0, cx)
        )

    def body(x, carry):
        faces, d_prev, d = carry
        d_next = jnp.where(x == cx - 1, xhigh[...], d_in[jnp.minimum(x + 1, cx - 1)])
        z_low, z_high = unpacked(low_faces, high_faces, d, x)
        flow = tx[x] * d_prev + tx[x + 1] * d_next
        flow = flow + (tym[x] * pltpu.roll(d, 1, 0) + typ[x] * pltpu.roll(d, ye - 1, 0))
        flow = flow + (tzm[x] * z_low + tzp[x] * z_high)
        flow = with_fault(flow, fault, x)
        z = z_in[x] - d + inv[x] * flow
        new = c1 * d + c2 * z
        before = d[H : H + cy] if first else corr_in[x]
        corr_out[x] = before + new[H : H + cy]
        if last:
            return faces, d, d_next
        d_out[x] = new
        z_out[x] = z
        keep_planes(planes, new, x)
        return pack_faces(faces, new, x), d, d_next

    init = (jnp.zeros((half, 128), f32), xlow[...], d_in[0])
    faces, _, _ = lax.fori_loop(0, cx, body, init, unroll=4)
    if not last:
        d_first[...] = d_out[0]
        d_last[...] = d_out[cx - 1]
        emit(a8_out, planes, faces, col_ref, row_ref)


VMEM = pl.BlockSpec(memory_space=pltpu.VMEM)
SMEM = pl.BlockSpec(memory_space=pltpu.SMEM)
PARAMS = pltpu.CompilerParams(vmem_limit_bytes=24 << 20)


def steps(axis):
    peers = lax.axis_size(axis)
    up = [(i, i + 1) for i in range(peers - 1)]
    return up, [(j, i) for i, j in up]


def local(rhs, accumulation, permeability, nnc_cell, nnc_remote, nnc_mask, nnc_trans):
    cx, cy, cz = rhs.shape
    tiles = lax.axis_size("gz")
    slots = nnc_cell.shape[-1]
    ye = cy + 2 * H
    half = ye // 2
    up_y, down_y = steps("gy")
    up_x, down_x = steps("gx")

    def struct(*shape):
        return jax.ShapeDtypeStruct(shape, f32)

    weight = nnc_trans.reshape(-1) * nnc_mask.reshape(-1).astype(f32)
    mine = jnp.stack([nnc_cell.reshape(-1).astype(f32), nnc_remote.reshape(-1).astype(f32), weight])
    bottom = [rhs[None, :, :H], accumulation[None, :, :H], permeability[:, :, :H]]
    top = [rhs[None, :, cy - H :], accumulation[None, :, cy - H :], permeability[:, :, cy - H :]]
    bottom = jnp.concatenate(bottom, axis=0).reshape(-1, cz)
    top = jnp.concatenate(top, axis=0).reshape(-1, cz)
    flat = jnp.pad(mine.reshape(-1, cz), ((0, 4), (0, 0)))
    before = lax.ppermute(top, "gy", up_y)
    after = lax.ppermute(jnp.concatenate([bottom, flat], axis=0), "gy", down_y)
    count = bottom.shape[0]
    above = after[count : count + 3 * slots // cz].reshape(3, slots)
    lists = jnp.stack([mine, above])
    cell = lists[:, 0].astype(jnp.int32)
    remote = lists[:, 1].astype(jnp.int32)
    column = cz * tiles
    far_z = remote % column
    own_x = (cell // cz).astype(f32)
    far_code = ((far_z // cz) * cx + remote // column).astype(f32)
    col = jnp.stack(
        [(cell % cz).astype(f32), own_x, (far_z % cz).astype(f32), far_code, lists[:, 2]], axis=-1
    )
    row = jnp.stack([own_x, far_code], axis=1)

    edge = struct(ye, cz)
    a8, kx_first, kx_last = pl.pallas_call(
        first_kernel,
        out_shape=(struct(tiles, half + 2 * cx, cz), edge, edge),
        in_specs=[VMEM] * 5,
        out_specs=(VMEM,) * 3,
        compiler_params=PARAMS,
    )(permeability, before, after, col, row)
    kx_low = lax.ppermute(kx_last, "gx", up_x)
    kx_high = lax.ppermute(kx_first, "gx", down_x)
    l = lax.axis_index("gz").reshape(1).astype(jnp.int32)
    l, a8, kx_low, kx_high = lax.optimization_barrier((l, a8, kx_low, kx_high))
    a8 = lax.all_to_all(a8, "gz", 0, 0, tiled=True)

    big = struct(cx, ye, cz)
    tall = struct(cx + 1, ye, cz)
    sent = struct(tiles, 4 * cx + half, cz)
    scratch = [pltpu.VMEM((4, cx, cz), f32)]
    inv, z, d, tx, tym, typ, tzm, tzp, d_first, d_last, a8 = pl.pallas_call(
        setup_kernel,
        out_shape=(big, big, big, tall, big, big, big, big, edge, edge, sent),
        in_specs=[SMEM] + [VMEM] * 10,
        out_specs=(VMEM,) * 11,
        scratch_shapes=scratch * 2,
        compiler_params=PARAMS,
    )(l, rhs, accumulation, permeability, before, after, kx_low, kx_high, a8, col, row)

    rho = 1.0 / sigma
    corr = None
    for sweep in range(1, SWEEPS):
        first, last = sweep == 1, sweep == SWEEPS - 1
        rho_next = 1.0 / (2.0 * sigma - rho)
        c1, c2 = rho_next * rho, 2.0 * rho_next / delta
        rho = rho_next
        xlow = lax.ppermute(d_last, "gx", up_x)
        xhigh = lax.ppermute(d_first, "gx", down_x)
        a8, xlow, xhigh = lax.optimization_barrier((a8, xlow, xhigh))
        a8 = lax.all_to_all(a8, "gz", 0, 0, tiled=True)
        args = [l, d, z] + ([] if first else [corr])
        args += [xlow, xhigh, a8, inv, tx, tym, typ, tzm, tzp, col, row]

        def kernel(*refs, c1=c1, c2=c2, first=first, last=last):
            sweep_kernel(c1, c2, first, last, *refs)

        small = struct(cx, cy, cz)
        out = pl.pallas_call(
            kernel,
            out_shape=small if last else (big, big, small, edge, edge, sent),
            in_specs=[SMEM] + [VMEM] * (len(args) - 1),
            out_specs=VMEM if last else (VMEM,) * 6,
            scratch_shapes=scratch if last else scratch * 2,
            compiler_params=PARAMS,
        )(*args)
        if last:
            corr = out
        else:
            d, z, corr, d_first, d_last, a8 = out
    return corr


def solution(mesh):
    split = P("gx", "gy", "gz")
    slots = P("gx", "gy", "gz", None)
    return jax.shard_map(
        local,
        mesh=mesh,
        in_specs=(split, split, P(None, "gx", "gy", "gz"), slots, slots, slots, slots),
        out_specs=split,
        check_vma=False,
    )
```

```python
import jax
import jax.numpy as jnp
from jax import lax
from jax.experimental import pallas as pl
from jax.experimental.pallas import tpu as pltpu
from jax.sharding import PartitionSpec as P

SWEEPS = 6
lam_low = 0.1
lam_high = 2.0
theta = (lam_high + lam_low) / 2.0
delta = (lam_high - lam_low) / 2.0
sigma = theta / delta

H = 8
f32 = jnp.float32
bf16 = jnp.bfloat16


def harmonic(left, right):
    total = left + right
    live = total > 0.0
    return jnp.where(live, 2.0 * (left * right) / jnp.where(live, total, 1.0), 0.0)


def split3(v):
    hi = v.astype(bf16).astype(f32)
    rest = v - hi
    mid = rest.astype(bf16).astype(f32)
    return hi, mid, rest - mid


def dot(a, b, dims):
    return lax.dot_general(a, b, (dims, ((), ())), preferred_element_type=f32)


def lane_iota(shape):
    return lax.broadcasted_iota(jnp.int32, shape, len(shape) - 1)


def hits(col_ref, q, which):
    codes = col_ref[q, :, which : which + 1]
    return lane_iota((codes.shape[0], 128)).astype(f32) == codes


def rows_hit(row_ref, q, which, count):
    codes = row_ref[q, which : which + 1, :]
    rows = lax.broadcasted_iota(jnp.int32, (count, codes.shape[1]), 0).astype(f32)
    return jnp.where(rows == codes, 1.0, 0.0).astype(bf16)


def scatter(u, lane_hit, row_hit):
    parts = [jnp.where(lane_hit, p, 0.0).astype(bf16) for p in split3(u)]
    out = dot(row_hit, jnp.concatenate(parts, axis=1), ((1,), (0,)))
    return out[:, :128] + out[:, 128:256] + out[:, 256:]


def gather(table, lane_hit, codes):
    rows = table.shape[0]
    pick = jnp.where(lane_hit, 1.0, 0.0).astype(bf16)
    parts = [p.astype(bf16) for p in split3(table)]
    if rows % 128 == 0:
        got = sum(dot(pick, p, ((1,), (1,))) for p in parts)
        lanes = lane_iota(got.shape)
    else:
        got = dot(pick, jnp.concatenate(parts, axis=0), ((1,), (1,)))
        lanes = lane_iota(got.shape) % rows
    return jnp.sum(jnp.where(lanes.astype(f32) == codes, got, 0.0), axis=1, keepdims=True)


def pack_faces(faces, slab, x):
    cx, half = 32, faces.shape[0]
    lane = lane_iota(faces.shape)
    for part in range(2):
        rows = slab[part * half : (part + 1) * half]
        faces = jnp.where(lane == 2 * cx * part + x, rows[:, 0:1], faces)
        faces = jnp.where(lane == 2 * cx * part + cx + x, rows[:, 127:128], faces)
    return faces


def unpacked(low_faces, high_faces, slab, x):
    cx = 32
    lane = lane_iota(slab.shape)

    def column(faces, first, to):
        return jnp.concatenate(
            [pltpu.roll(faces, (to - first - 2 * cx * part - x) % 128, 1) for part in range(2)],
            axis=0,
        )

    low = jnp.where(lane == 0, column(low_faces, cx, 128), pltpu.roll(slab, 1, 1))
    high = jnp.where(lane == 127, column(high_faces, 0, 127 + 128), pltpu.roll(slab, 127, 1))
    return low, high


def put_partials(out_ref, base, tiles, q, col_ref, row_ref, u, cx):
    sums = scatter(u, hits(col_ref, q, 2), rows_hit(row_ref, q, 1, tiles * cx))
    for t in range(tiles):
        out_ref[t, base + q * cx : base + (q + 1) * cx, :] = sums[t * cx : (t + 1) * cx]


def first_kernel(own_k, before, after, col_ref, row_ref, rhs, acc,
                 out_ref, kx_first, kx_last, rhs_out, acc_out, sem):
    moves = [
        pltpu.make_async_copy(rhs, rhs_out, sem.at[0]),
        pltpu.make_async_copy(acc, acc_out, sem.at[1]),
    ]
    for move in moves:
        move.start()
    tiles = out_ref.shape[0]
    cx = own_k.shape[1]

    def body(x, faces):
        at = pl.multiple_of((4 * cx + x) * H, H)
        slab = jnp.concatenate([before[pl.ds(at, H), :], own_k[2, x], after[pl.ds(at, H), :]], axis=0)
        return pack_faces(faces, slab, x)

    for x, face in ((0, kx_first), (cx - 1, kx_last)):
        at = (2 * cx + x) * H
        face[...] = jnp.concatenate([before[at : at + H, :], own_k[0, x], after[at : at + H, :]], axis=0)
    half = (own_k.shape[2] + 2 * H) // 2
    faces = lax.fori_loop(0, cx, body, jnp.zeros((half, 128), f32), unroll=4)
    for t in range(tiles):
        out_ref[t, 0:half, :] = faces
    for q in range(2):
        put_partials(out_ref, half, tiles, q, col_ref, row_ref, col_ref[q, :, 4:5], cx)
    for move in moves:
        move.wait()


def emit(a8_ref, planes, faces, col_ref, row_ref):
    tiles = a8_ref.shape[0]
    cx = planes.shape[1]
    half = faces.shape[0]
    for t in range(tiles):
        a8_ref[t, 0:cx, :] = planes[0]
        a8_ref[t, cx : 2 * cx, :] = planes[2]
        a8_ref[t, 2 * cx : 2 * cx + half, :] = faces
    for q in range(2):
        near = gather(planes[1 + 2 * q], hits(col_ref, q, 0), col_ref[q, :, 1:2])
        put_partials(a8_ref, 2 * cx + half, tiles, q, col_ref, row_ref, col_ref[q, :, 4:5] * near, cx)


def keep_planes(planes, slab, x):
    last = slab.shape[0] - H - 1
    for n, y in enumerate((H - 1, H, last, last + 1)):
        planes[n, pl.ds(x, 1), :] = slab[y : y + 1, :]


def with_fault(total, fault, x):
    y = lax.broadcasted_iota(jnp.int32, total.shape, 0)
    last = total.shape[0] - H - 1
    extra = jnp.zeros_like(total)
    for n, at in enumerate((H - 1, H, last, last + 1)):
        extra = jnp.where(y == at, fault[n, pl.ds(x, 1), :], extra)
    return total + extra


def neighbour_faces(l_ref, a8, base, half):
    tiles = a8.shape[0]
    l = l_ref[0]
    low = a8[jnp.maximum(l - 1, 0), base : base + half, :]
    high = a8[jnp.minimum(l + 1, tiles - 1), base : base + half, :]
    return low, high


def weights_kernel(a8, col_ref, row_ref, fault):
    tiles, rows = a8.shape[0], a8.shape[1]
    cx = fault.shape[1]
    for q in range(2):
        base = rows - (2 - q) * cx
        far = a8[0, base : base + cx, :]
        for t in range(1, tiles):
            far = far + a8[t, base : base + cx, :]
        fault[2 * q] = far
        near = scatter(col_ref[q, :, 4:5], hits(col_ref, q, 0), rows_hit(row_ref, q, 0, cx))
        fault[2 * q + 1] = near


def fault_kernel(a8, col_ref, row_ref, fault):
    tiles, rows = a8.shape[0], a8.shape[1]
    cx = fault.shape[1]
    for q in range(2):
        base = rows - (2 - q) * cx
        far = a8[0, base : base + cx, :]
        for t in range(1, tiles):
            far = far + a8[t, base : base + cx, :]
        fault[2 * q] = far
        table = jnp.concatenate([a8[t, q * cx : (q + 1) * cx, :] for t in range(tiles)], axis=0)
        got = gather(table, hits(col_ref, q, 2), col_ref[q, :, 3:4])
        fault[2 * q + 1] = scatter(
            col_ref[q, :, 4:5] * got, hits(col_ref, q, 0), rows_hit(row_ref, q, 0, cx)
        )


def setup_kernel(l_ref, rhs, acc, perm, before, after, kx_low, kx_high, a8, fault, col_ref, row_ref,
                 inv, z_out, d_out, tx, tym, typ, tzm, tzp, d_first, d_last, a8_out, planes):
    cx, cy = rhs.shape[0], rhs.shape[1]
    ye = cy + 2 * H
    half = ye // 2
    tiles = a8.shape[0]
    l = l_ref[0]
    low_faces, high_faces = neighbour_faces(l_ref, a8, 0, half)
    low_faces = jnp.where(l > 0, low_faces, 0.0)
    high_faces = jnp.where(l < tiles - 1, high_faces, 0.0)

    def ext(a, own, x):
        at = pl.multiple_of((a * cx + x) * H, H)
        return jnp.concatenate([before[pl.ds(at, H), :], own, after[pl.ds(at, H), :]], axis=0)

    def body(x, carry):
        faces, t_low, kx = carry
        nxt = jnp.minimum(x + 1, cx - 1)
        kx_next = jnp.where(x == cx - 1, kx_high[...], ext(2, perm[0, nxt], nxt))
        ky = ext(3, perm[1, x], x)
        kz = ext(4, perm[2, x], x)
        t_high = harmonic(kx, kx_next)
        ym = harmonic(ky, pltpu.roll(ky, 1, 0))
        yp = harmonic(ky, pltpu.roll(ky, ye - 1, 0))
        kz_low, kz_high = unpacked(low_faces, high_faces, kz, x)
        zm = harmonic(kz, kz_low)
        zp = harmonic(kz, kz_high)
        diag = ext(1, acc[x], x) + t_low + t_high + ym + yp + zm + zp
        diag = with_fault(diag, fault, x)
        live = diag > 0.0
        inverse = jnp.where(live, 1.0 / jnp.where(live, diag, 1.0), 0.0)
        z = inverse * ext(0, rhs[x], x)
        d = z / theta
        inv[x] = inverse
        z_out[x] = z
        d_out[x] = d
        tx[x] = t_low
        tx[x + 1] = t_high
        tym[x] = ym
        typ[x] = yp
        tzm[x] = zm
        tzp[x] = zp
        keep_planes(planes, d, x)
        return pack_faces(faces, d, x), t_high, kx_next

    kx0 = ext(2, perm[0, 0], 0)
    init = (jnp.zeros((half, 128), f32), harmonic(kx_low[...], kx0), kx0)
    faces, _, _ = lax.fori_loop(0, cx, body, init, unroll=4)
    d_first[...] = d_out[0]
    d_last[...] = d_out[cx - 1]
    emit(a8_out, planes, faces, col_ref, row_ref)


def sweep_kernel(c1, c2, first, last, l_ref, d_in, z_in, *refs):
    refs = list(refs)
    corr_in = None if first else refs.pop(0)
    xlow, xhigh, a8, fault, inv, tx, tym, typ, tzm, tzp, col_ref, row_ref = refs[:12]
    outs = refs[12:]
    if last:
        (corr_out,) = outs
    else:
        d_out, z_out, corr_out, d_first, d_last, a8_out, planes = outs
    cx, ye = d_in.shape[0], d_in.shape[1]
    cy = ye - 2 * H
    half = ye // 2
    low_faces, high_faces = neighbour_faces(l_ref, a8, 2 * cx, half)

    def body(x, carry):
        faces, d_prev, d = carry
        d_next = jnp.where(x == cx - 1, xhigh[...], d_in[jnp.minimum(x + 1, cx - 1)])
        z_low, z_high = unpacked(low_faces, high_faces, d, x)
        flow = tx[x] * d_prev + tx[x + 1] * d_next
        flow = flow + (tym[x] * pltpu.roll(d, 1, 0) + typ[x] * pltpu.roll(d, ye - 1, 0))
        flow = flow + (tzm[x] * z_low + tzp[x] * z_high)
        flow = with_fault(flow, fault, x)
        z = z_in[x] - d + inv[x] * flow
        new = c1 * d + c2 * z
        before = d[H : H + cy] if first else corr_in[x]
        corr_out[x] = before + new[H : H + cy]
        if last:
            return faces, d, d_next
        d_out[x] = new
        z_out[x] = z
        keep_planes(planes, new, x)
        return pack_faces(faces, new, x), d, d_next

    init = (jnp.zeros((half, 128), f32), xlow[...], d_in[0])
    faces, _, _ = lax.fori_loop(0, cx, body, init, unroll=4)
    if not last:
        d_first[...] = d_out[0]
        d_last[...] = d_out[cx - 1]
        emit(a8_out, planes, faces, col_ref, row_ref)


VMEM = pl.BlockSpec(memory_space=pltpu.VMEM)
SMEM = pl.BlockSpec(memory_space=pltpu.SMEM)
PARAMS = pltpu.CompilerParams(vmem_limit_bytes=24 << 20)


def steps(axis):
    peers = lax.axis_size(axis)
    up = [(i, i + 1) for i in range(peers - 1)]
    return up, [(j, i) for i, j in up]


def exchange(step, a8, first, last, col, row, cx):
    up_x, down_x = steps("gx")
    low = lax.ppermute(last, "gx", up_x)
    high = lax.ppermute(first, "gx", down_x)
    a8 = lax.all_to_all(a8, "gz", 0, 0, tiled=True)
    fault = pl.pallas_call(
        fault_kernel if step else weights_kernel,
        out_shape=jax.ShapeDtypeStruct((4, cx, a8.shape[-1]), f32),
        in_specs=[VMEM] * 3,
        out_specs=VMEM,
        compiler_params=PARAMS,
    )(a8, col, row)
    return a8, low, high, fault


def local(rhs, accumulation, permeability, nnc_cell, nnc_remote, nnc_mask, nnc_trans):
    cx, cy, cz = rhs.shape
    tiles = lax.axis_size("gz")
    slots = nnc_cell.shape[-1]
    ye = cy + 2 * H
    half = ye // 2
    up_y, down_y = steps("gy")

    def struct(*shape):
        return jax.ShapeDtypeStruct(shape, f32)

    weight = nnc_trans.reshape(-1) * nnc_mask.reshape(-1).astype(f32)
    mine = jnp.stack([nnc_cell.reshape(-1).astype(f32), nnc_remote.reshape(-1).astype(f32), weight])
    bottom = [rhs[None, :, :H], accumulation[None, :, :H], permeability[:, :, :H]]
    top = [rhs[None, :, cy - H :], accumulation[None, :, cy - H :], permeability[:, :, cy - H :]]
    bottom = jnp.concatenate(bottom, axis=0).reshape(-1, cz)
    top = jnp.concatenate(top, axis=0).reshape(-1, cz)
    flat = jnp.pad(mine.reshape(-1, cz), ((0, 4), (0, 0)))
    before = lax.ppermute(top, "gy", up_y)
    after = lax.ppermute(jnp.concatenate([bottom, flat], axis=0), "gy", down_y)
    count = bottom.shape[0]
    above = after[count : count + 3 * slots // cz].reshape(3, slots)
    lists = jnp.stack([mine, above])
    cell = lists[:, 0].astype(jnp.int32)
    remote = lists[:, 1].astype(jnp.int32)
    column = cz * tiles
    far_z = remote % column
    own_x = (cell // cz).astype(f32)
    far_code = ((far_z // cz) * cx + remote // column).astype(f32)
    col = jnp.stack(
        [(cell % cz).astype(f32), own_x, (far_z % cz).astype(f32), far_code, lists[:, 2]], axis=-1
    )
    row = jnp.stack([own_x, far_code], axis=1)

    edge = struct(ye, cz)
    l = lax.axis_index("gz").reshape(1).astype(jnp.int32)
    l, col, row = lax.optimization_barrier((l, col, row))
    small = struct(cx, cy, cz)
    a8, kx_first, kx_last, rhs, accumulation = pl.pallas_call(
        first_kernel,
        out_shape=(struct(tiles, half + 2 * cx, cz), edge, edge, small, small),
        in_specs=[VMEM] * 5 + [pl.BlockSpec(memory_space=pltpu.HBM)] * 2,
        out_specs=(VMEM,) * 5,
        scratch_shapes=[pltpu.SemaphoreType.DMA((2,))],
        compiler_params=PARAMS,
    )(permeability, before, after, col, row, rhs, accumulation)
    a8, kx_low, kx_high, fault = exchange(0, a8, kx_first, kx_last, col, row, cx)

    big = struct(cx, ye, cz)
    tall = struct(cx + 1, ye, cz)
    sent = struct(tiles, 4 * cx + half, cz)
    scratch = [pltpu.VMEM((4, cx, cz), f32)]
    inv, z, d, tx, tym, typ, tzm, tzp, d_first, d_last, a8 = pl.pallas_call(
        setup_kernel,
        out_shape=(big, big, big, tall, big, big, big, big, edge, edge, sent),
        in_specs=[SMEM] + [VMEM] * 11,
        out_specs=(VMEM,) * 11,
        scratch_shapes=scratch,
        compiler_params=PARAMS,
    )(l, rhs, accumulation, permeability, before, after, kx_low, kx_high, a8, fault, col, row)

    rho = 1.0 / sigma
    corr = None
    for sweep in range(1, SWEEPS):
        first, last = sweep == 1, sweep == SWEEPS - 1
        rho_next = 1.0 / (2.0 * sigma - rho)
        c1, c2 = rho_next * rho, 2.0 * rho_next / delta
        rho = rho_next
        a8, xlow, xhigh, fault = exchange(sweep, a8, d_first, d_last, col, row, cx)
        args = [l, d, z] + ([] if first else [corr])
        args += [xlow, xhigh, a8, fault, inv, tx, tym, typ, tzm, tzp, col, row]

        def kernel(*refs, c1=c1, c2=c2, first=first, last=last):
            sweep_kernel(c1, c2, first, last, *refs)

        out = pl.pallas_call(
            kernel,
            out_shape=small if last else (big, big, small, edge, edge, sent),
            in_specs=[SMEM] + [VMEM] * (len(args) - 1),
            out_specs=VMEM if last else (VMEM,) * 6,
            scratch_shapes=[] if last else scratch,
            compiler_params=PARAMS,
        )(*args)
        if last:
            corr = out
        else:
            d, z, corr, d_first, d_last, a8 = out
    return corr


def solution(mesh):
    split = P("gx", "gy", "gz")
    slots = P("gx", "gy", "gz", None)
    return jax.shard_map(
        local,
        mesh=mesh,
        in_specs=(split, split, P(None, "gx", "gy", "gz"), slots, slots, slots, slots),
        out_specs=split,
        check_vma=False,
    )
```

```python
import jax
import jax.numpy as jnp
from jax import lax
from jax.experimental import pallas as pl
from jax.experimental.pallas import tpu as pltpu
from jax.sharding import PartitionSpec as P

SWEEPS = 6
lam_low = 0.1
lam_high = 2.0
theta = (lam_high + lam_low) / 2.0
delta = (lam_high - lam_low) / 2.0
sigma = theta / delta

SLOT_ROWS = 4
H = 8
f32 = jnp.float32
bf16 = jnp.bfloat16


def harmonic(left, right):
    total = left + right
    live = total > 0.0
    return jnp.where(live, 2.0 * (left * right) / jnp.where(live, total, 1.0), 0.0)


def split3(v):
    hi = v.astype(bf16).astype(f32)
    rest = v - hi
    mid = rest.astype(bf16).astype(f32)
    return hi, mid, rest - mid


def dot(a, b, dims):
    return lax.dot_general(a, b, (dims, ((), ())), preferred_element_type=f32)


def lane_iota(shape):
    return lax.broadcasted_iota(jnp.int32, shape, len(shape) - 1)


def rows_hit(codes, count):
    shape = (count, codes.shape[1])
    return lax.broadcasted_iota(jnp.int32, shape, 0).astype(f32) == codes


def picks(codes):
    return jnp.where(rows_hit(codes, 128), 1.0, 0.0).astype(bf16)


def thirds(out):
    n = out.shape[0] // 3
    return out[:n] + out[n : 2 * n] + out[2 * n :]


def gather(table, pick, x_hit):
    parts = jnp.concatenate(split3(table), axis=0).astype(bf16)
    got = thirds(dot(parts, pick, ((1,), (0,))))
    return jnp.sum(jnp.where(x_hit, got, 0.0), axis=0, keepdims=True)


def scatter(u, pick, x_hit):
    parts = [jnp.where(x_hit, p, 0.0) for p in split3(u)]
    return thirds(dot(jnp.concatenate(parts, axis=0).astype(bf16), pick, ((1,), (1,))))


def get_rows(ref, t, base, count):
    return jnp.concatenate([ref[t, base + k : base + k + 1, :] for k in range(count)], axis=1)


def put_rows(ref, t, base, values):
    for k in range(values.shape[1] // 128):
        ref[t, base + k : base + k + 1, :] = values[:, 128 * k : 128 * (k + 1)]


NEAR_Z, NEAR_X, WEIGHT, FAR_X, FAR_TILE, FAR_Z = range(6)


def slot_row(row_ref, q, which):
    return row_ref[q, which : which + 1, :]


def pack_faces(faces, slab, x):
    cx, half = 32, faces.shape[0]
    lane = lane_iota(faces.shape)
    for part in range(2):
        rows = slab[part * half : (part + 1) * half]
        faces = jnp.where(lane == 2 * cx * part + x, rows[:, 0:1], faces)
        faces = jnp.where(lane == 2 * cx * part + cx + x, rows[:, 127:128], faces)
    return faces


def unpacked(low_faces, high_faces, slab, x):
    cx = 32
    lane = lane_iota(slab.shape)

    def column(faces, first, to):
        return jnp.concatenate(
            [pltpu.roll(faces, (to - first - 2 * cx * part - x) % 128, 1) for part in range(2)],
            axis=0,
        )

    low = jnp.where(lane == 0, column(low_faces, cx, 128), pltpu.roll(slab, 1, 1))
    high = jnp.where(lane == 127, column(high_faces, 0, 127 + 128), pltpu.roll(slab, 127, 1))
    return low, high


def first_kernel(own_k, before, after, row_ref, rhs, acc,
                 out_ref, kx_first, kx_last, rhs_out, acc_out, sem):
    moves = [
        pltpu.make_async_copy(rhs, rhs_out, sem.at[0]),
        pltpu.make_async_copy(acc, acc_out, sem.at[1]),
    ]
    for move in moves:
        move.start()
    tiles = out_ref.shape[0]
    cx = own_k.shape[1]

    def body(x, faces):
        at = pl.multiple_of((4 * cx + x) * H, H)
        slab = jnp.concatenate([before[pl.ds(at, H), :], own_k[2, x], after[pl.ds(at, H), :]], axis=0)
        return pack_faces(faces, slab, x)

    for x, face in ((0, kx_first), (cx - 1, kx_last)):
        at = (2 * cx + x) * H
        face[...] = jnp.concatenate([before[at : at + H, :], own_k[0, x], after[at : at + H, :]], axis=0)
    half = (own_k.shape[2] + 2 * H) // 2
    faces = lax.fori_loop(0, cx, body, jnp.zeros((half, 128), f32), unroll=4)
    for t in range(tiles):
        out_ref[t, 0:half, :] = faces
    for q in range(2):
        base = half + q * 4 * SLOT_ROWS
        for n, which in enumerate((FAR_X, FAR_TILE, FAR_Z, WEIGHT)):
            for t in range(tiles):
                put_rows(out_ref, t, base + n * SLOT_ROWS, slot_row(row_ref, q, which))
    for move in moves:
        move.wait()


def emit(a8_ref, planes, faces, row_ref, pick_ref, far_x):
    tiles = a8_ref.shape[0]
    cx = planes.shape[1]
    half = faces.shape[0]
    slots = row_ref.shape[2]
    for t in range(tiles):
        a8_ref[t, 0:half, :] = faces
    for q in range(2):
        base = half + q * 2 * SLOT_ROWS
        near = gather(
            planes[2 * q + 1], picks(slot_row(row_ref, q, NEAR_Z)), rows_hit(slot_row(row_ref, q, NEAR_X), cx)
        )
        near = slot_row(row_ref, q, WEIGHT) * near
        for t in range(tiles):
            at = slice(t * slots, (t + 1) * slots)
            far = gather(planes[2 * q], pick_ref[q, :, at], rows_hit(far_x[q : q + 1, at], cx))
            put_rows(a8_ref, t, base, near)
            put_rows(a8_ref, t, base + SLOT_ROWS, far)


def keep_planes(planes, slab, x):
    last = slab.shape[0] - H - 1
    for n, y in enumerate((H - 1, H, last, last + 1)):
        planes[n, pl.ds(x, 1), :] = slab[y : y + 1, :]


def with_fault(total, fault, x):
    y = lax.broadcasted_iota(jnp.int32, total.shape, 0)
    last = total.shape[0] - H - 1
    extra = jnp.zeros_like(total)
    for n, at in enumerate((H - 1, H, last, last + 1)):
        extra = jnp.where(y == at, fault[n, pl.ds(x, 1), :], extra)
    return total + extra


def neighbour_faces(l_ref, a8, base, half):
    tiles = a8.shape[0]
    l = l_ref[0]
    low = a8[jnp.maximum(l - 1, 0), base : base + half, :]
    high = a8[jnp.minimum(l + 1, tiles - 1), base : base + half, :]
    return low, high


def near_sum(row_ref, q, values, cx):
    return scatter(
        values, picks(slot_row(row_ref, q, NEAR_Z)), rows_hit(slot_row(row_ref, q, NEAR_X), cx)
    )


def weights_kernel(l_ref, a8, row_ref, fault, pick_ref, far_x):
    tiles, rows = a8.shape[0], a8.shape[1]
    cx = fault.shape[1]
    slots = row_ref.shape[2]
    here = l_ref[0].astype(f32)
    for q in range(2):
        base = rows - (2 - q) * 4 * SLOT_ROWS
        far = jnp.zeros((cx, 128), f32)
        for t in range(tiles):
            at = slice(t * slots, (t + 1) * slots)
            x, tile, z, weight = [get_rows(a8, t, base + n * SLOT_ROWS, SLOT_ROWS) for n in range(4)]
            x = jnp.where(tile == here, x, -1.0)
            pick = picks(z)
            pick_ref[q, :, at] = pick
            far_x[q : q + 1, at] = x
            far = far + scatter(weight, pick, rows_hit(x, cx))
        fault[2 * q] = far
        fault[2 * q + 1] = near_sum(row_ref, q, slot_row(row_ref, q, WEIGHT), cx)


def fault_kernel(a8, row_ref, pick_ref, far_x, fault):
    tiles, rows = a8.shape[0], a8.shape[1]
    cx = fault.shape[1]
    slots = row_ref.shape[2]
    for q in range(2):
        base = rows - (2 - q) * 2 * SLOT_ROWS
        far = jnp.zeros((cx, 128), f32)
        near = jnp.zeros((1, slots), f32)
        for t in range(tiles):
            at = slice(t * slots, (t + 1) * slots)
            values = get_rows(a8, t, base, SLOT_ROWS)
            far = far + scatter(values, pick_ref[q, :, at], rows_hit(far_x[q : q + 1, at], cx))
            near = near + get_rows(a8, t, base + SLOT_ROWS, SLOT_ROWS)
        fault[2 * q] = far
        fault[2 * q + 1] = near_sum(row_ref, q, slot_row(row_ref, q, WEIGHT) * near, cx)


def setup_kernel(l_ref, rhs, acc, perm, before, after, kx_low, kx_high, a8, fault, row_ref, pick_ref, far_x,
                 inv, z_out, d_out, tx, tym, typ, tzm, tzp, d_first, d_last, a8_out, planes):
    cx, cy = rhs.shape[0], rhs.shape[1]
    ye = cy + 2 * H
    half = ye // 2
    tiles = a8.shape[0]
    l = l_ref[0]
    low_faces, high_faces = neighbour_faces(l_ref, a8, 0, half)
    low_faces = jnp.where(l > 0, low_faces, 0.0)
    high_faces = jnp.where(l < tiles - 1, high_faces, 0.0)

    def ext(a, own, x):
        at = pl.multiple_of((a * cx + x) * H, H)
        return jnp.concatenate([before[pl.ds(at, H), :], own, after[pl.ds(at, H), :]], axis=0)

    def body(x, carry):
        faces, t_low, kx = carry
        nxt = jnp.minimum(x + 1, cx - 1)
        kx_next = jnp.where(x == cx - 1, kx_high[...], ext(2, perm[0, nxt], nxt))
        ky = ext(3, perm[1, x], x)
        kz = ext(4, perm[2, x], x)
        t_high = harmonic(kx, kx_next)
        ym = harmonic(ky, pltpu.roll(ky, 1, 0))
        yp = harmonic(ky, pltpu.roll(ky, ye - 1, 0))
        kz_low, kz_high = unpacked(low_faces, high_faces, kz, x)
        zm = harmonic(kz, kz_low)
        zp = harmonic(kz, kz_high)
        diag = ext(1, acc[x], x) + t_low + t_high + ym + yp + zm + zp
        diag = with_fault(diag, fault, x)
        live = diag > 0.0
        inverse = jnp.where(live, 1.0 / jnp.where(live, diag, 1.0), 0.0)
        z = inverse * ext(0, rhs[x], x)
        d = z / theta
        inv[x] = inverse
        z_out[x] = z
        d_out[x] = d
        tx[x] = t_low
        tx[x + 1] = t_high
        tym[x] = ym
        typ[x] = yp
        tzm[x] = zm
        tzp[x] = zp
        keep_planes(planes, d, x)
        return pack_faces(faces, d, x), t_high, kx_next

    kx0 = ext(2, perm[0, 0], 0)
    init = (jnp.zeros((half, 128), f32), harmonic(kx_low[...], kx0), kx0)
    faces, _, _ = lax.fori_loop(0, cx, body, init, unroll=4)
    d_first[...] = d_out[0]
    d_last[...] = d_out[cx - 1]
    emit(a8_out, planes, faces, row_ref, pick_ref, far_x)


def sweep_kernel(c1, c2, first, last, l_ref, d_in, z_in, *refs):
    refs = list(refs)
    corr_in = None if first else refs.pop(0)
    xlow, xhigh, a8, fault, inv, tx, tym, typ, tzm, tzp = refs[:10]
    refs = refs[10:]
    if not last:
        row_ref, pick_ref, far_x = refs[:3]
        refs = refs[3:]
    outs = refs
    if last:
        (corr_out,) = outs
    else:
        d_out, z_out, corr_out, d_first, d_last, a8_out, planes = outs
    cx, ye = d_in.shape[0], d_in.shape[1]
    cy = ye - 2 * H
    half = ye // 2
    low_faces, high_faces = neighbour_faces(l_ref, a8, 0, half)

    def body(x, carry):
        faces, d_prev, d = carry
        d_next = jnp.where(x == cx - 1, xhigh[...], d_in[jnp.minimum(x + 1, cx - 1)])
        z_low, z_high = unpacked(low_faces, high_faces, d, x)
        flow = tx[x] * d_prev + tx[x + 1] * d_next
        flow = flow + (tym[x] * pltpu.roll(d, 1, 0) + typ[x] * pltpu.roll(d, ye - 1, 0))
        flow = flow + (tzm[x] * z_low + tzp[x] * z_high)
        flow = with_fault(flow, fault, x)
        z = z_in[x] - d + inv[x] * flow
        new = c1 * d + c2 * z
        before = d[H : H + cy] if first else corr_in[x]
        corr_out[x] = before + new[H : H + cy]
        if last:
            return faces, d, d_next
        d_out[x] = new
        z_out[x] = z
        keep_planes(planes, new, x)
        return pack_faces(faces, new, x), d, d_next

    init = (jnp.zeros((half, 128), f32), xlow[...], d_in[0])
    faces, _, _ = lax.fori_loop(0, cx, body, init, unroll=4)
    if not last:
        d_first[...] = d_out[0]
        d_last[...] = d_out[cx - 1]
        emit(a8_out, planes, faces, row_ref, pick_ref, far_x)


VMEM = pl.BlockSpec(memory_space=pltpu.VMEM)
SMEM = pl.BlockSpec(memory_space=pltpu.SMEM)
PARAMS = pltpu.CompilerParams(vmem_limit_bytes=24 << 20)


def steps(axis):
    peers = lax.axis_size(axis)
    up = [(i, i + 1) for i in range(peers - 1)]
    return up, [(j, i) for i, j in up]


def exchange(step, a8, first, last, operands, cx):
    up_x, down_x = steps("gx")
    cz = a8.shape[-1]
    fault = jax.ShapeDtypeStruct((4, cx, cz), f32)
    low = lax.ppermute(last, "gx", up_x)
    high = lax.ppermute(first, "gx", down_x)
    a8 = lax.all_to_all(a8, "gz", 0, 0, tiled=True)
    if step:
        fault = pl.pallas_call(
            fault_kernel,
            out_shape=fault,
            in_specs=[VMEM] * 4,
            out_specs=VMEM,
            compiler_params=PARAMS,
        )(a8, *operands)
    else:
        l, row = operands
        every = a8.shape[0] * row.shape[-1]
        fault = pl.pallas_call(
            weights_kernel,
            out_shape=(
                fault,
                jax.ShapeDtypeStruct((2, cz, every), bf16),
                jax.ShapeDtypeStruct((2, every), f32),
            ),
            in_specs=[SMEM, VMEM, VMEM],
            out_specs=(VMEM,) * 3,
            compiler_params=PARAMS,
        )(l, a8, row)
    return a8, low, high, fault


def local(rhs, accumulation, permeability, nnc_cell, nnc_remote, nnc_mask, nnc_trans):
    cx, cy, cz = rhs.shape
    tiles = lax.axis_size("gz")
    slots = nnc_cell.shape[-1]
    ye = cy + 2 * H
    half = ye // 2
    up_y, down_y = steps("gy")

    def struct(*shape):
        return jax.ShapeDtypeStruct(shape, f32)

    weight = nnc_trans.reshape(-1) * nnc_mask.reshape(-1).astype(f32)
    mine = jnp.stack([nnc_cell.reshape(-1).astype(f32), nnc_remote.reshape(-1).astype(f32), weight])
    bottom = [rhs[None, :, :H], accumulation[None, :, :H], permeability[:, :, :H]]
    top = [rhs[None, :, cy - H :], accumulation[None, :, cy - H :], permeability[:, :, cy - H :]]
    bottom = jnp.concatenate(bottom, axis=0).reshape(-1, cz)
    top = jnp.concatenate(top, axis=0).reshape(-1, cz)
    flat = jnp.pad(mine.reshape(-1, cz), ((0, 4), (0, 0)))
    before = lax.ppermute(top, "gy", up_y)
    after = lax.ppermute(jnp.concatenate([bottom, flat], axis=0), "gy", down_y)
    count = bottom.shape[0]
    above = after[count : count + 3 * slots // cz].reshape(3, slots)
    lists = jnp.stack([mine, above])
    cell = lists[:, 0].astype(jnp.int32)
    remote = lists[:, 1].astype(jnp.int32)
    column = cz * tiles
    far_z = remote % column
    table = [
        (cell % cz).astype(f32),
        (cell // cz).astype(f32),
        lists[:, 2],
        (remote // column).astype(f32),
        (far_z // cz).astype(f32),
        (far_z % cz).astype(f32),
    ]
    row = jnp.stack(table + [jnp.zeros_like(lists[:, 2])] * 2, axis=1)

    edge = struct(ye, cz)
    l = lax.axis_index("gz").reshape(1).astype(jnp.int32)
    l, row = lax.optimization_barrier((l, row))
    small = struct(cx, cy, cz)
    a8, kx_first, kx_last, rhs, accumulation = pl.pallas_call(
        first_kernel,
        out_shape=(struct(tiles, half + 8 * SLOT_ROWS, cz), edge, edge, small, small),
        in_specs=[VMEM] * 4 + [pl.BlockSpec(memory_space=pltpu.HBM)] * 2,
        out_specs=(VMEM,) * 5,
        scratch_shapes=[pltpu.SemaphoreType.DMA((2,))],
        compiler_params=PARAMS,
    )(permeability, before, after, row, rhs, accumulation)
    a8, kx_low, kx_high, (fault, pick, far_x) = exchange(0, a8, kx_first, kx_last, (l, row), cx)

    big = struct(cx, ye, cz)
    tall = struct(cx + 1, ye, cz)
    sent = struct(tiles, half + 4 * SLOT_ROWS, cz)
    scratch = [pltpu.VMEM((4, cx, cz), f32)]
    inv, z, d, tx, tym, typ, tzm, tzp, d_first, d_last, a8 = pl.pallas_call(
        setup_kernel,
        out_shape=(big, big, big, tall, big, big, big, big, edge, edge, sent),
        in_specs=[SMEM] + [VMEM] * 12,
        out_specs=(VMEM,) * 11,
        scratch_shapes=scratch,
        compiler_params=PARAMS,
    )(l, rhs, accumulation, permeability, before, after, kx_low, kx_high, a8, fault, row, pick, far_x)

    rho = 1.0 / sigma
    corr = None
    for sweep in range(1, SWEEPS):
        first, last = sweep == 1, sweep == SWEEPS - 1
        rho_next = 1.0 / (2.0 * sigma - rho)
        c1, c2 = rho_next * rho, 2.0 * rho_next / delta
        rho = rho_next
        a8, xlow, xhigh, fault = exchange(sweep, a8, d_first, d_last, (row, pick, far_x), cx)
        args = [l, d, z] + ([] if first else [corr])
        args += [xlow, xhigh, a8, fault, inv, tx, tym, typ, tzm, tzp]
        args += [] if last else [row, pick, far_x]

        def kernel(*refs, c1=c1, c2=c2, first=first, last=last):
            sweep_kernel(c1, c2, first, last, *refs)

        out = pl.pallas_call(
            kernel,
            out_shape=small if last else (big, big, small, edge, edge, sent),
            in_specs=[SMEM] + [VMEM] * (len(args) - 1),
            out_specs=VMEM if last else (VMEM,) * 6,
            scratch_shapes=[] if last else scratch,
            compiler_params=PARAMS,
        )(*args)
        if last:
            corr = out
        else:
            d, z, corr, d_first, d_last, a8 = out
    return corr


def solution(mesh):
    split = P("gx", "gy", "gz")
    slots = P("gx", "gy", "gz", None)
    return jax.shard_map(
        local,
        mesh=mesh,
        in_specs=(split, split, P(None, "gx", "gy", "gz"), slots, slots, slots, slots),
        out_specs=split,
        check_vma=False,
    )
```

```python
import jax
import jax.numpy as jnp
from jax import lax
from jax.experimental import pallas as pl
from jax.experimental.pallas import tpu as pltpu
from jax.sharding import PartitionSpec as P

SWEEPS = 6
lam_low = 0.1
lam_high = 2.0
theta = (lam_high + lam_low) / 2.0
delta = (lam_high - lam_low) / 2.0
sigma = theta / delta

SLOT_ROWS = 4
LIST_ROWS = 24
H = 8
f32 = jnp.float32
bf16 = jnp.bfloat16


def harmonic(left, right):
    total = left + right
    live = total > 0.0
    return jnp.where(live, 2.0 * (left * right) / jnp.where(live, total, 1.0), 0.0)


def split3(v):
    hi = v.astype(bf16).astype(f32)
    rest = v - hi
    mid = rest.astype(bf16).astype(f32)
    return hi, mid, rest - mid


def dot(a, b, dims):
    return lax.dot_general(a, b, (dims, ((), ())), preferred_element_type=f32)


def lane_iota(shape):
    return lax.broadcasted_iota(jnp.int32, shape, len(shape) - 1)


def rows_hit(codes, count):
    shape = (count, codes.shape[1])
    return lax.broadcasted_iota(jnp.int32, shape, 0).astype(f32) == codes


def picks(codes):
    return jnp.where(rows_hit(codes, 128), 1.0, 0.0).astype(bf16)


def thirds(out):
    n = out.shape[0] // 3
    return out[:n] + out[n : 2 * n] + out[2 * n :]


def gather(table, pick, x_hit):
    parts = jnp.concatenate(split3(table), axis=0).astype(bf16)
    got = thirds(dot(parts, pick, ((1,), (0,))))
    return jnp.sum(jnp.where(x_hit, got, 0.0), axis=0, keepdims=True)


def scatter(u, pick, x_hit):
    parts = [jnp.where(x_hit, p, 0.0) for p in split3(u)]
    return thirds(dot(jnp.concatenate(parts, axis=0).astype(bf16), pick, ((1,), (1,))))


def get_rows(ref, t, base, count):
    return jnp.concatenate([ref[t, base + k : base + k + 1, :] for k in range(count)], axis=1)


def put_rows(ref, t, base, values):
    for k in range(values.shape[1] // 128):
        ref[t, base + k : base + k + 1, :] = values[:, 128 * k : 128 * (k + 1)]


NEAR_Z, NEAR_X, WEIGHT, FAR_X, FAR_TILE, FAR_Z = range(6)


def slot_row(row_ref, q, which):
    return row_ref[q, which : which + 1, :]


FACE_ROWS = 16


def pack_faces(faces, slab, x, cx):
    low, high = faces
    lane = lane_iota(low.shape)
    for part in range(slab.shape[0] // FACE_ROWS):
        rows = slab[part * FACE_ROWS : (part + 1) * FACE_ROWS]
        here = lane == cx * part + x
        low = jnp.where(here, rows[:, 0:1], low)
        high = jnp.where(here, rows[:, 127:128], high)
    return low, high


def no_faces():
    return jnp.zeros((FACE_ROWS, 128), f32), jnp.zeros((FACE_ROWS, 128), f32)


def put_faces(l, ref, faces):
    for t in range(ref.shape[0]):
        ref[t, 0:FACE_ROWS, :] = jnp.where(t > l, faces[1], faces[0])


def get_faces(l, ref):
    tiles = ref.shape[0]
    low = ref[jnp.maximum(l - 1, 0), 0:FACE_ROWS, :]
    high = ref[jnp.minimum(l + 1, tiles - 1), 0:FACE_ROWS, :]
    return low, high


def unpacked(faces, slab, x, cx):
    lane = lane_iota(slab.shape)
    parts = slab.shape[0] // FACE_ROWS

    def column(packed, to):
        return jnp.concatenate(
            [pltpu.roll(packed, (to + 128 - cx * part - x) % 128, 1) for part in range(parts)], axis=0
        )

    low = jnp.where(lane == 0, column(faces[0], 0), pltpu.roll(slab, 1, 1))
    high = jnp.where(lane == 127, column(faces[1], 127), pltpu.roll(slab, 127, 1))
    return low, high


def pack_kernel(l_ref, rhs, acc, perm, cell, remote, mask, trans,
                top, bottom, a8, kx_first, kx_last, kz, sem):
    tiles = a8.shape[0]
    cx, cy = rhs.shape[0], rhs.shape[1]
    sources = [rhs, acc] + [perm.at[n] for n in range(3)]
    moves = [pltpu.make_async_copy(perm.at[2], kz, sem.at[0])]
    for n, source in enumerate(sources):
        moves.append(pltpu.make_async_copy(source.at[:, cy - H :, :], top.at[n], sem.at[1 + 2 * n]))
        moves.append(pltpu.make_async_copy(source.at[:, :H, :], bottom.at[n], sem.at[2 + 2 * n]))
    count = 2 * len(sources) + 1
    moves.append(pltpu.make_async_copy(perm.at[0, 0], kx_first, sem.at[count]))
    moves.append(pltpu.make_async_copy(perm.at[0, cx - 1], kx_last, sem.at[count + 1]))
    for move in moves:
        move.start()
    weight = trans[...] * mask[...].astype(f32)
    own, far = cell[...], remote[...]
    column = tiles * 128
    far_z = far & (column - 1)
    table = [
        (own & 127).astype(f32),
        (own >> 7).astype(f32),
        weight,
        (far >> (column.bit_length() - 1)).astype(f32),
        (far_z >> 7).astype(f32),
        (far_z & 127).astype(f32),
    ]
    for n, values in enumerate(table):
        for t in range(tiles):
            put_rows(a8, t, FACE_ROWS + n * SLOT_ROWS, values)
    moves[0].wait()

    def body(x, faces):
        return pack_faces(faces, kz[x], x, cx)

    put_faces(l_ref[0], a8, lax.fori_loop(0, cx, body, no_faces(), unroll=4))
    for move in moves[1:]:
        move.wait()


def relay_kernel(l_ref, a8, faces, lists):
    tiles = a8.shape[0]
    l = l_ref[0]
    low, high = get_faces(l, a8)
    faces[0:FACE_ROWS, :] = jnp.where(l > 0, low, 0.0)
    faces[FACE_ROWS:, :] = jnp.where(l < tiles - 1, high, 0.0)
    for t in range(tiles):
        lists[LIST_ROWS * t : LIST_ROWS * (t + 1), :] = a8[t, FACE_ROWS:, :]


def join_kernel(faces, lists, kx_low, kx_high, up, down):
    cy = kx_low.shape[0]
    base = 2 * FACE_ROWS
    for out in (up, down):
        out[0:base, :] = faces[...]
        out[base : base + cy, :] = kx_low[...]
        out[base + cy : base + 2 * cy, :] = kx_high[...]
    down[base + 2 * cy :, :] = lists[...]


def emit(l_ref, a8_ref, planes, faces, row_ref, pick_ref, far_x):
    tiles = a8_ref.shape[0]
    cx = planes.shape[1]
    slots = row_ref.shape[2]
    put_faces(l_ref[0], a8_ref, faces)
    for q in range(2):
        base = FACE_ROWS + q * 2 * SLOT_ROWS
        near = gather(
            planes[2 * q + 1], picks(slot_row(row_ref, q, NEAR_Z)), rows_hit(slot_row(row_ref, q, NEAR_X), cx)
        )
        near = slot_row(row_ref, q, WEIGHT) * near
        for t in range(tiles):
            at = slice(t * slots, (t + 1) * slots)
            far = gather(planes[2 * q], pick_ref[q, :, at], rows_hit(far_x[q : q + 1, at], cx))
            put_rows(a8_ref, t, base, near)
            put_rows(a8_ref, t, base + SLOT_ROWS, far)


def keep_planes(planes, slab, x):
    last = slab.shape[0] - H - 1
    for n, y in enumerate((H - 1, H, last, last + 1)):
        planes[n, pl.ds(x, 1), :] = slab[y : y + 1, :]


def with_fault(total, fault, x):
    tiles = [total[8 * n : 8 * (n + 1)] for n in range(total.shape[0] // 8)]
    y = lax.broadcasted_iota(jnp.int32, tiles[0].shape, 0)
    last = total.shape[0] - H - 1
    for n, at in enumerate((H - 1, H, last, last + 1)):
        tiles[at // 8] += jnp.where(y == at % 8, fault[n, pl.ds(x, 1), :], 0.0)
    return jnp.concatenate(tiles, axis=0)


def near_sum(row_ref, q, values, cx):
    return scatter(
        values, picks(slot_row(row_ref, q, NEAR_Z)), rows_hit(slot_row(row_ref, q, NEAR_X), cx)
    )


def weights(l, a8, above, row_ref, pick_ref, far_x, fault):
    tiles = a8.shape[0]
    cx = fault.shape[1]
    slots = row_ref.shape[2]
    first = above.shape[0] - tiles * LIST_ROWS

    def codes(block):
        parts = [block[n : n + 1] for n in range(LIST_ROWS)]
        return [
            jnp.concatenate(parts[SLOT_ROWS * n : SLOT_ROWS * (n + 1)], axis=1) for n in range(6)
        ]

    def block(q, t):
        if q == 0:
            return a8[t, FACE_ROWS : FACE_ROWS + LIST_ROWS, :]
        return above[pl.ds(pl.multiple_of(first + t * LIST_ROWS, 8), LIST_ROWS), :]

    for q in range(2):
        mine = codes(block(q, l))
        for n in range(3):
            row_ref[q, n : n + 1, :] = mine[n]
        far = jnp.zeros((cx, 128), f32)
        for t in range(tiles):
            at = slice(t * slots, (t + 1) * slots)
            table = codes(block(q, t))
            x = jnp.where(table[FAR_TILE] == l.astype(f32), table[FAR_X], -1.0)
            pick = picks(table[FAR_Z])
            pick_ref[q, :, at] = pick
            far_x[q : q + 1, at] = x
            far = far + scatter(table[WEIGHT], pick, rows_hit(x, cx))
        fault[2 * q] = far
        fault[2 * q + 1] = near_sum(row_ref, q, slot_row(row_ref, q, WEIGHT), cx)


def fault_kernel(a8, row_ref, pick_ref, far_x, fault):
    tiles, rows = a8.shape[0], a8.shape[1]
    cx = fault.shape[1]
    slots = row_ref.shape[2]
    for q in range(2):
        base = rows - (2 - q) * 2 * SLOT_ROWS
        far = jnp.zeros((cx, 128), f32)
        near = jnp.zeros((1, slots), f32)
        for t in range(tiles):
            at = slice(t * slots, (t + 1) * slots)
            values = get_rows(a8, t, base, SLOT_ROWS)
            far = far + scatter(values, pick_ref[q, :, at], rows_hit(far_x[q : q + 1, at], cx))
            near = near + get_rows(a8, t, base + SLOT_ROWS, SLOT_ROWS)
        fault[2 * q] = far
        fault[2 * q + 1] = near_sum(row_ref, q, slot_row(row_ref, q, WEIGHT) * near, cx)


def setup_kernel(l_ref, rhs, acc, perm, before, after, below, above, kx_low, kx_high, a8,
                 inv, z_out, d_out, tx, tym, typ, tzm, tzp, d_first, d_last, a8_out,
                 row_ref, pick_ref, far_x, planes, fault):
    cx, cy = rhs.shape[0], rhs.shape[1]
    ye = cy + 2 * H
    tiles = a8.shape[0]
    l = l_ref[0]
    weights(l, a8, above, row_ref, pick_ref, far_x, fault)
    low, high = get_faces(l, a8)
    faces_in = []
    for n, own in enumerate((jnp.where(l > 0, low, 0.0), jnp.where(l < tiles - 1, high, 0.0))):
        at = n * FACE_ROWS
        lane = lane_iota((8, 128))
        under, over = below[at + 8 : at + 16, :], above[at : at + 8, :]
        first = jnp.where(lane < cx, pltpu.roll(under, 128 - cx, 1), pltpu.roll(own[8:16], cx, 1))
        second = jnp.where(lane < 2 * cx, own[0:8], pltpu.roll(over, 2 * cx, 1))
        faces_in.append(jnp.concatenate([first, second], axis=0))

    def ext_face(n, own):
        at = 2 * FACE_ROWS + n * cy
        return jnp.concatenate([below[at + cy - H : at + cy, :], own[...], above[at : at + H, :]], axis=0)

    kx_under, kx_over = ext_face(0, kx_low), ext_face(1, kx_high)

    def ext(a, own, x):
        return jnp.concatenate([before[a, x], own, after[a, x]], axis=0)

    def body(x, carry):
        faces, t_low, kx = carry
        nxt = jnp.minimum(x + 1, cx - 1)
        kx_next = jnp.where(x == cx - 1, kx_over, ext(2, perm[0, nxt], nxt))
        ky = ext(3, perm[1, x], x)
        kz = ext(4, perm[2, x], x)
        t_high = harmonic(kx, kx_next)
        ym = harmonic(ky, pltpu.roll(ky, 1, 0))
        yp = harmonic(ky, pltpu.roll(ky, ye - 1, 0))
        kz_low, kz_high = unpacked(faces_in, kz, x, cx)
        zm = harmonic(kz, kz_low)
        zp = harmonic(kz, kz_high)
        diag = ext(1, acc[x], x) + t_low + t_high + ym + yp + zm + zp
        diag = with_fault(diag, fault, x)
        live = diag > 0.0
        inverse = jnp.where(live, 1.0 / jnp.where(live, diag, 1.0), 0.0)
        z = inverse * ext(0, rhs[x], x)
        d = z / theta
        inv[x] = inverse
        z_out[x] = z
        d_out[x] = d
        tx[x] = t_low
        tx[x + 1] = t_high
        tym[x] = ym
        typ[x] = yp
        tzm[x] = zm
        tzp[x] = zp
        keep_planes(planes, d, x)
        return pack_faces(faces, d, x, cx), t_high, kx_next

    kx0 = ext(2, perm[0, 0], 0)
    init = (no_faces(), harmonic(kx_under, kx0), kx0)
    faces, _, _ = lax.fori_loop(0, cx, body, init, unroll=4)
    d_first[...] = d_out[0]
    d_last[...] = d_out[cx - 1]
    emit(l_ref, a8_out, planes, faces, row_ref, pick_ref, far_x)


def sweep_kernel(c1, c2, first, last, l_ref, d_in, z_in, *refs):
    refs = list(refs)
    corr_in = None if first else refs.pop(0)
    xlow, xhigh, a8, fault, inv, tx, tym, typ, tzm, tzp = refs[:10]
    refs = refs[10:]
    if not last:
        row_ref, pick_ref, far_x = refs[:3]
        refs = refs[3:]
    outs = refs
    if last:
        (corr_out,) = outs
    else:
        d_out, z_out, corr_out, d_first, d_last, a8_out, planes = outs
    cx, ye = d_in.shape[0], d_in.shape[1]
    cy = ye - 2 * H
    faces_in = get_faces(l_ref[0], a8)

    def body(x, carry):
        faces, d_prev, d = carry
        d_next = jnp.where(x == cx - 1, xhigh[...], d_in[jnp.minimum(x + 1, cx - 1)])
        z_low, z_high = unpacked(faces_in, d, x, cx)
        flow = tx[x] * d_prev + tx[x + 1] * d_next
        flow = flow + (tym[x] * pltpu.roll(d, 1, 0) + typ[x] * pltpu.roll(d, ye - 1, 0))
        flow = flow + (tzm[x] * z_low + tzp[x] * z_high)
        flow = with_fault(flow, fault, x)
        z = z_in[x] - d + inv[x] * flow
        new = c1 * d + c2 * z
        before = d[H : H + cy] if first else corr_in[x]
        corr_out[x] = before + new[H : H + cy]
        if last:
            return faces, d, d_next
        d_out[x] = new
        z_out[x] = z
        keep_planes(planes, new, x)
        return pack_faces(faces, new, x, cx), d, d_next

    init = (no_faces(), xlow[...], d_in[0])
    faces, _, _ = lax.fori_loop(0, cx, body, init, unroll=4)
    if not last:
        d_first[...] = d_out[0]
        d_last[...] = d_out[cx - 1]
        emit(l_ref, a8_out, planes, faces, row_ref, pick_ref, far_x)


VMEM = pl.BlockSpec(memory_space=pltpu.VMEM)
SMEM = pl.BlockSpec(memory_space=pltpu.SMEM)
HBM = pl.BlockSpec(memory_space=pltpu.HBM)
PARAMS = pltpu.CompilerParams(vmem_limit_bytes=24 << 20)


def steps(axis):
    peers = lax.axis_size(axis)
    up = [(i, i + 1) for i in range(peers - 1)]
    return up, [(j, i) for i, j in up]


def local(rhs, accumulation, permeability, nnc_cell, nnc_remote, nnc_mask, nnc_trans):
    cx, cy, cz = rhs.shape
    tiles = lax.axis_size("gz")
    slots = nnc_cell.shape[-1]
    ye = cy + 2 * H
    up_y, down_y = steps("gy")
    up_x, down_x = steps("gx")

    def struct(*shape, dtype=f32):
        return jax.ShapeDtypeStruct(shape, dtype)

    l = lax.axis_index("gz").reshape(1).astype(jnp.int32)
    flats = [a.reshape(1, slots) for a in (nnc_cell, nnc_remote, nnc_mask, nnc_trans)]
    halo = struct(5, cx, H, cz)
    top, bottom, a8, kx_first, kx_last = pl.pallas_call(
        pack_kernel,
        out_shape=(halo, halo, struct(tiles, FACE_ROWS + LIST_ROWS, cz), struct(cy, cz), struct(cy, cz)),
        in_specs=[SMEM] + [HBM] * 3 + [VMEM] * 4,
        out_specs=(VMEM,) * 5,
        scratch_shapes=[pltpu.VMEM((cx, cy, cz), f32), pltpu.SemaphoreType.DMA((13,))],
    )(l, rhs, accumulation, permeability, *flats)
    kx_low = lax.ppermute(kx_last, "gx", up_x)
    kx_high = lax.ppermute(kx_first, "gx", down_x)
    before = lax.ppermute(top, "gy", up_y)
    after = lax.ppermute(bottom, "gy", down_y)
    a8 = lax.all_to_all(a8, "gz", 0, 0, tiled=True)
    faces, group = pl.pallas_call(
        relay_kernel,
        out_shape=(struct(2 * FACE_ROWS, cz), struct(tiles * LIST_ROWS, cz)),
        in_specs=[SMEM, VMEM],
        out_specs=(VMEM,) * 2,
        compiler_params=PARAMS,
    )(l, a8)
    small = 2 * FACE_ROWS + 2 * cy
    below, above = pl.pallas_call(
        join_kernel,
        out_shape=(struct(small, cz), struct(small + tiles * LIST_ROWS, cz)),
        in_specs=[VMEM] * 4,
        out_specs=(VMEM,) * 2,
        compiler_params=PARAMS,
    )(faces, group, kx_low, kx_high)
    below = lax.ppermute(below, "gy", up_y)
    above = lax.ppermute(above, "gy", down_y)

    big = struct(cx, ye, cz)
    tall = struct(cx + 1, ye, cz)
    edge = struct(ye, cz)
    small = struct(cx, cy, cz)
    sent = struct(tiles, FACE_ROWS + 4 * SLOT_ROWS, cz)
    scratch = [pltpu.VMEM((4, cx, cz), f32)]
    every = tiles * slots
    lists = (struct(2, 8, slots), struct(2, cz, every, dtype=bf16), struct(2, every))
    inv, z, d, tx, tym, typ, tzm, tzp, d_first, d_last, a8, row, pick, far_x = pl.pallas_call(
        setup_kernel,
        out_shape=(big, big, big, tall, big, big, big, big, edge, edge, sent) + lists,
        in_specs=[SMEM] + [VMEM] * 10,
        out_specs=(VMEM,) * 14,
        scratch_shapes=scratch * 2,
        compiler_params=PARAMS,
    )(l, rhs, accumulation, permeability, before, after, below, above, kx_low, kx_high, a8)

    rho = 1.0 / sigma
    corr = None
    for sweep in range(1, SWEEPS):
        first, last = sweep == 1, sweep == SWEEPS - 1
        rho_next = 1.0 / (2.0 * sigma - rho)
        c1, c2 = rho_next * rho, 2.0 * rho_next / delta
        rho = rho_next
        xlow = lax.ppermute(d_last, "gx", up_x)
        xhigh = lax.ppermute(d_first, "gx", down_x)
        a8 = lax.all_to_all(a8, "gz", 0, 0, tiled=True)
        fault = pl.pallas_call(
            fault_kernel,
            out_shape=struct(4, cx, cz),
            in_specs=[VMEM] * 4,
            out_specs=VMEM,
            compiler_params=PARAMS,
        )(a8, row, pick, far_x)
        args = [l, d, z] + ([] if first else [corr])
        args += [xlow, xhigh, a8, fault, inv, tx, tym, typ, tzm, tzp]
        args += [] if last else [row, pick, far_x]

        def kernel(*refs, c1=c1, c2=c2, first=first, last=last):
            sweep_kernel(c1, c2, first, last, *refs)

        out = pl.pallas_call(
            kernel,
            out_shape=small if last else (big, big, small, edge, edge, sent),
            in_specs=[SMEM] + [VMEM] * (len(args) - 1),
            out_specs=VMEM if last else (VMEM,) * 6,
            scratch_shapes=[] if last else scratch,
            compiler_params=PARAMS,
        )(*args)
        if last:
            corr = out
        else:
            d, z, corr, d_first, d_last, a8 = out
    return corr


def solution(mesh):
    split = P("gx", "gy", "gz")
    slots = P("gx", "gy", "gz", None)
    return jax.shard_map(
        local,
        mesh=mesh,
        in_specs=(split, split, P(None, "gx", "gy", "gz"), slots, slots, slots, slots),
        out_specs=split,
        check_vma=False,
    )
```

```python
import jax
import jax.numpy as jnp
from jax import lax
from jax.experimental import pallas as pl
from jax.experimental.pallas import tpu as pltpu
from jax.sharding import PartitionSpec as P

SWEEPS = 6
lam_low = 0.1
lam_high = 2.0
theta = (lam_high + lam_low) / 2.0
delta = (lam_high - lam_low) / 2.0
sigma = theta / delta

SLOT_ROWS = 4
LIST_ROWS = 24
H = 8
f32 = jnp.float32
bf16 = jnp.bfloat16


def harmonic(left, right):
    total = left + right
    live = total > 0.0
    return jnp.where(live, 2.0 * (left * right) / jnp.where(live, total, 1.0), 0.0)


def split3(v):
    hi = v.astype(bf16).astype(f32)
    rest = v - hi
    mid = rest.astype(bf16).astype(f32)
    return hi, mid, rest - mid


def dot(a, b, dims):
    return lax.dot_general(a, b, (dims, ((), ())), preferred_element_type=f32)


def lane_iota(shape):
    return lax.broadcasted_iota(jnp.int32, shape, len(shape) - 1)


def rows_hit(codes, count):
    shape = (count, codes.shape[1])
    return lax.broadcasted_iota(jnp.int32, shape, 0).astype(f32) == codes


def picks(codes):
    return jnp.where(rows_hit(codes, 128), 1.0, 0.0).astype(bf16)


def thirds(out):
    n = out.shape[0] // 3
    return out[:n] + out[n : 2 * n] + out[2 * n :]


def gather(table, pick, x_hit):
    parts = jnp.concatenate(split3(table), axis=0).astype(bf16)
    got = thirds(dot(parts, pick, ((1,), (0,))))
    return jnp.sum(jnp.where(x_hit, got, 0.0), axis=0, keepdims=True)


def scatter(u, pick, x_hit):
    parts = [jnp.where(x_hit, p, 0.0) for p in split3(u)]
    return thirds(dot(jnp.concatenate(parts, axis=0).astype(bf16), pick, ((1,), (1,))))


def get_rows(ref, t, base, count):
    return jnp.concatenate([ref[t, base + k : base + k + 1, :] for k in range(count)], axis=1)


def put_rows(ref, t, base, values):
    for k in range(values.shape[1] // 128):
        ref[t, base + k : base + k + 1, :] = values[:, 128 * k : 128 * (k + 1)]


NEAR_Z, NEAR_X, WEIGHT, FAR_X, FAR_TILE, FAR_Z = range(6)


def slot_row(row_ref, q, which):
    return row_ref[q, which : which + 1, :]


FACE_ROWS = 24


def pack_faces(faces, tiles, x):
    faces = list(faces)
    lane = lane_iota((8, 128))
    for half in range(2):
        at = 64 * half + 2 * x + 2
        here = ((lane - (at - 1)) & 127) < 2
        for n in range(3):
            tile = tiles[3 * half + n]
            if tile is not None:
                faces[n] = jnp.where(here, pltpu.roll(tile, at % 128, 1), faces[n])
    return tuple(faces)


def no_faces():
    return (jnp.zeros((8, 128), f32),) * 3


def y_tiles(slab):
    return [slab[8 * n : 8 * (n + 1)] for n in range(slab.shape[0] // 8)]


def put_faces(ref, faces):
    packed = jnp.concatenate(faces, axis=0)
    for t in range(ref.shape[0]):
        ref[t, 0:FACE_ROWS, :] = packed


def get_faces(l, ref):
    tiles = ref.shape[0]
    low = jnp.where(l > 0, ref[jnp.maximum(l - 1, 0), 0:FACE_ROWS, :], 0.0)
    high = jnp.where(l < tiles - 1, ref[jnp.minimum(l + 1, tiles - 1), 0:FACE_ROWS, :], 0.0)
    odd = (lane_iota(low.shape) & 1) == 1
    return jnp.where(odd, low, pltpu.roll(high, 126, 1))


def unpacked(faces, slab, x):
    lane = lane_iota((8, 128))
    lows, highs = [], []
    for n, tile in enumerate(y_tiles(slab)):
        packed = faces[8 * (n % 3) : 8 * (n % 3) + 8]
        outer = pltpu.roll(packed, (127 - 64 * (n // 3) - 2 * x) % 128, 1)
        lows.append(jnp.where(lane == 0, outer, pltpu.roll(tile, 1, 1)))
        highs.append(jnp.where(lane == 127, outer, pltpu.roll(tile, 127, 1)))
    return jnp.concatenate(lows, axis=0), jnp.concatenate(highs, axis=0)


def pack_kernel(rhs, acc, perm, cell, remote, mask, trans,
                top, bottom, a8, kx_first, kx_last, kz, sem):
    tiles = a8.shape[0]
    cx, cy = rhs.shape[0], rhs.shape[1]
    sources = [rhs, acc] + [perm.at[n] for n in range(3)]
    moves = [pltpu.make_async_copy(perm.at[2], kz, sem.at[0])]
    for n, source in enumerate(sources):
        moves.append(pltpu.make_async_copy(source.at[:, cy - H :, :], top.at[n], sem.at[1 + 2 * n]))
        moves.append(pltpu.make_async_copy(source.at[:, :H, :], bottom.at[n], sem.at[2 + 2 * n]))
    count = 2 * len(sources) + 1
    moves.append(pltpu.make_async_copy(perm.at[0, 0], kx_first, sem.at[count]))
    moves.append(pltpu.make_async_copy(perm.at[0, cx - 1], kx_last, sem.at[count + 1]))
    for move in moves:
        move.start()
    weight = trans[...] * mask[...].astype(f32)
    own, far = cell[...], remote[...]
    column = tiles * 128
    far_z = far & (column - 1)
    table = [
        (own & 127).astype(f32),
        (own >> 7).astype(f32),
        weight,
        (far >> (column.bit_length() - 1)).astype(f32),
        (far_z >> 7).astype(f32),
        (far_z & 127).astype(f32),
    ]
    for n, values in enumerate(table):
        for t in range(tiles):
            put_rows(a8, t, FACE_ROWS + n * SLOT_ROWS, values)
    moves[0].wait()

    def body(x, faces):
        return pack_faces(faces, [None] + y_tiles(kz[x]) + [None], x)

    put_faces(a8, lax.fori_loop(0, cx, body, no_faces(), unroll=4))
    for move in moves[1:]:
        move.wait()


def relay_kernel(l_ref, a8, faces, lists):
    tiles = a8.shape[0]
    l = l_ref[0]
    faces[...] = get_faces(l, a8)
    for t in range(tiles):
        lists[LIST_ROWS * t : LIST_ROWS * (t + 1), :] = a8[t, FACE_ROWS:, :]


def join_kernel(faces, lists, kx_low, kx_high, up, down):
    cy = kx_low.shape[0]
    base = FACE_ROWS
    for out in (up, down):
        out[0:base, :] = faces[...]
        out[base : base + cy, :] = kx_low[...]
        out[base + cy : base + 2 * cy, :] = kx_high[...]
    down[base + 2 * cy :, :] = lists[...]


def emit(a8_ref, planes, faces, row_ref, pick_ref, far_x):
    tiles = a8_ref.shape[0]
    cx = planes.shape[1]
    slots = row_ref.shape[2]
    put_faces(a8_ref, faces)
    for q in range(2):
        base = FACE_ROWS + q * 2 * SLOT_ROWS
        near = gather(
            planes[2 * q + 1], picks(slot_row(row_ref, q, NEAR_Z)), rows_hit(slot_row(row_ref, q, NEAR_X), cx)
        )
        near = slot_row(row_ref, q, WEIGHT) * near
        for t in range(tiles):
            at = slice(t * slots, (t + 1) * slots)
            far = gather(planes[2 * q], pick_ref[q, :, at], rows_hit(far_x[q : q + 1, at], cx))
            put_rows(a8_ref, t, base, near)
            put_rows(a8_ref, t, base + SLOT_ROWS, far)


def keep_planes(planes, slab, x):
    last = slab.shape[0] - H - 1
    for n, y in enumerate((H - 1, H, last, last + 1)):
        planes[n, pl.ds(x, 1), :] = slab[y : y + 1, :]


def with_fault(total, fault, x):
    tiles = y_tiles(total)
    y = lax.broadcasted_iota(jnp.int32, tiles[0].shape, 0)
    last = total.shape[0] - H - 1
    for n, at in enumerate((H - 1, H, last, last + 1)):
        tiles[at // 8] += jnp.where(y == at % 8, fault[n, pl.ds(x, 1), :], 0.0)
    return jnp.concatenate(tiles, axis=0)


def near_sum(row_ref, q, values, cx):
    return scatter(
        values, picks(slot_row(row_ref, q, NEAR_Z)), rows_hit(slot_row(row_ref, q, NEAR_X), cx)
    )


def weights(l, a8, above, row_ref, pick_ref, far_x, fault):
    tiles = a8.shape[0]
    cx = fault.shape[1]
    slots = row_ref.shape[2]
    first = above.shape[0] - tiles * LIST_ROWS

    def codes(block):
        parts = [block[n : n + 1] for n in range(LIST_ROWS)]
        return [
            jnp.concatenate(parts[SLOT_ROWS * n : SLOT_ROWS * (n + 1)], axis=1) for n in range(6)
        ]

    def block(q, t):
        if q == 0:
            return a8[t, FACE_ROWS : FACE_ROWS + LIST_ROWS, :]
        return above[pl.ds(pl.multiple_of(first + t * LIST_ROWS, 8), LIST_ROWS), :]

    for q in range(2):
        mine = codes(block(q, l))
        for n in range(3):
            row_ref[q, n : n + 1, :] = mine[n]
        far = jnp.zeros((cx, 128), f32)
        for t in range(tiles):
            at = slice(t * slots, (t + 1) * slots)
            table = codes(block(q, t))
            x = jnp.where(table[FAR_TILE] == l.astype(f32), table[FAR_X], -1.0)
            pick = picks(table[FAR_Z])
            pick_ref[q, :, at] = pick
            far_x[q : q + 1, at] = x
            far = far + scatter(table[WEIGHT], pick, rows_hit(x, cx))
        fault[2 * q] = far
        fault[2 * q + 1] = near_sum(row_ref, q, slot_row(row_ref, q, WEIGHT), cx)


def fault_kernel(a8, row_ref, pick_ref, far_x, fault):
    tiles, rows = a8.shape[0], a8.shape[1]
    cx = fault.shape[1]
    slots = row_ref.shape[2]
    for q in range(2):
        base = rows - (2 - q) * 2 * SLOT_ROWS
        far = jnp.zeros((cx, 128), f32)
        near = jnp.zeros((1, slots), f32)
        for t in range(tiles):
            at = slice(t * slots, (t + 1) * slots)
            values = get_rows(a8, t, base, SLOT_ROWS)
            far = far + scatter(values, pick_ref[q, :, at], rows_hit(far_x[q : q + 1, at], cx))
            near = near + get_rows(a8, t, base + SLOT_ROWS, SLOT_ROWS)
        fault[2 * q] = far
        fault[2 * q + 1] = near_sum(row_ref, q, slot_row(row_ref, q, WEIGHT) * near, cx)


def setup_kernel(l_ref, rhs, acc, perm, before, after, below, above, kx_low, kx_high, a8,
                 inv, z_out, d_out, tx, tym, typ, tzm, tzp, d_first, d_last, a8_out,
                 row_ref, pick_ref, far_x, planes, fault):
    cx, cy = rhs.shape[0], rhs.shape[1]
    ye = cy + 2 * H
    l = l_ref[0]
    weights(l, a8, above, row_ref, pick_ref, far_x, fault)
    own = get_faces(l, a8)
    left = lane_iota((8, 128)) < 64
    faces_in = jnp.concatenate(
        [
            jnp.where(left, pltpu.roll(below[8:16, :], 64, 1), own[0:8]),
            own[8:16],
            jnp.where(left, own[16:24], pltpu.roll(above[8:16, :], 64, 1)),
        ],
        axis=0,
    )

    def ext_face(n, own):
        at = FACE_ROWS + n * cy
        return jnp.concatenate([below[at + cy - H : at + cy, :], own[...], above[at : at + H, :]], axis=0)

    kx_under, kx_over = ext_face(0, kx_low), ext_face(1, kx_high)

    def ext(a, own, x):
        return jnp.concatenate([before[a, x], own, after[a, x]], axis=0)

    def body(x, carry):
        faces, t_low, kx = carry
        nxt = jnp.minimum(x + 1, cx - 1)
        kx_next = jnp.where(x == cx - 1, kx_over, ext(2, perm[0, nxt], nxt))
        ky = ext(3, perm[1, x], x)
        kz = ext(4, perm[2, x], x)
        t_high = harmonic(kx, kx_next)
        ym = harmonic(ky, pltpu.roll(ky, 1, 0))
        yp = harmonic(ky, pltpu.roll(ky, ye - 1, 0))
        kz_low, kz_high = unpacked(faces_in, kz, x)
        zm = harmonic(kz, kz_low)
        zp = harmonic(kz, kz_high)
        diag = ext(1, acc[x], x) + t_low + t_high + ym + yp + zm + zp
        diag = with_fault(diag, fault, x)
        live = diag > 0.0
        inverse = jnp.where(live, 1.0 / jnp.where(live, diag, 1.0), 0.0)
        z = inverse * ext(0, rhs[x], x)
        d = z / theta
        inv[x] = inverse
        z_out[x] = z
        d_out[x] = d
        tx[x] = t_low
        tx[x + 1] = t_high
        tym[x] = ym
        typ[x] = yp
        tzm[x] = zm
        tzp[x] = zp
        keep_planes(planes, d, x)
        return pack_faces(faces, y_tiles(d), x), t_high, kx_next

    kx0 = ext(2, perm[0, 0], 0)
    init = (no_faces(), harmonic(kx_under, kx0), kx0)
    faces, _, _ = lax.fori_loop(0, cx, body, init, unroll=4)
    d_first[...] = d_out[0]
    d_last[...] = d_out[cx - 1]
    emit(a8_out, planes, faces, row_ref, pick_ref, far_x)


def sweep_kernel(c1, c2, first, last, l_ref, d_in, z_in, *refs):
    refs = list(refs)
    corr_in = None if first else refs.pop(0)
    xlow, xhigh, a8, fault, inv, tx, tym, typ, tzm, tzp = refs[:10]
    refs = refs[10:]
    if not last:
        row_ref, pick_ref, far_x = refs[:3]
        refs = refs[3:]
    outs = refs
    if last:
        (corr_out,) = outs
    else:
        d_out, z_out, corr_out, d_first, d_last, a8_out, planes = outs
    cx, ye = d_in.shape[0], d_in.shape[1]
    cy = ye - 2 * H
    faces_in = get_faces(l_ref[0], a8)

    def body(x, carry):
        faces, d_prev, d = carry
        d_next = jnp.where(x == cx - 1, xhigh[...], d_in[jnp.minimum(x + 1, cx - 1)])
        z_low, z_high = unpacked(faces_in, d, x)
        flow = tx[x] * d_prev + tx[x + 1] * d_next
        flow = flow + (tym[x] * pltpu.roll(d, 1, 0) + typ[x] * pltpu.roll(d, ye - 1, 0))
        flow = flow + (tzm[x] * z_low + tzp[x] * z_high)
        flow = with_fault(flow, fault, x)
        z = z_in[x] - d + inv[x] * flow
        new = c1 * d + c2 * z
        before = d[H : H + cy] if first else corr_in[x]
        corr_out[x] = before + new[H : H + cy]
        if last:
            return faces, d, d_next
        d_out[x] = new
        z_out[x] = z
        keep_planes(planes, new, x)
        return pack_faces(faces, y_tiles(new), x), d, d_next

    init = (no_faces(), xlow[...], d_in[0])
    faces, _, _ = lax.fori_loop(0, cx, body, init, unroll=4)
    if not last:
        d_first[...] = d_out[0]
        d_last[...] = d_out[cx - 1]
        emit(a8_out, planes, faces, row_ref, pick_ref, far_x)


VMEM = pl.BlockSpec(memory_space=pltpu.VMEM)
SMEM = pl.BlockSpec(memory_space=pltpu.SMEM)
HBM = pl.BlockSpec(memory_space=pltpu.HBM)
PARAMS = pltpu.CompilerParams(vmem_limit_bytes=24 << 20)


def steps(axis):
    peers = lax.axis_size(axis)
    up = [(i, i + 1) for i in range(peers - 1)]
    return up, [(j, i) for i, j in up]


def local(rhs, accumulation, permeability, nnc_cell, nnc_remote, nnc_mask, nnc_trans):
    cx, cy, cz = rhs.shape
    tiles = lax.axis_size("gz")
    slots = nnc_cell.shape[-1]
    ye = cy + 2 * H
    up_y, down_y = steps("gy")
    up_x, down_x = steps("gx")

    def struct(*shape, dtype=f32):
        return jax.ShapeDtypeStruct(shape, dtype)

    l = lax.axis_index("gz").reshape(1).astype(jnp.int32)
    flats = [a.reshape(1, slots) for a in (nnc_cell, nnc_remote, nnc_mask, nnc_trans)]
    l, *flats = lax.optimization_barrier((l, *flats))
    halo = struct(5, cx, H, cz)
    top, bottom, a8, kx_first, kx_last = pl.pallas_call(
        pack_kernel,
        out_shape=(halo, halo, struct(tiles, FACE_ROWS + LIST_ROWS, cz), struct(cy, cz), struct(cy, cz)),
        in_specs=[HBM] * 3 + [VMEM] * 4,
        out_specs=(VMEM,) * 5,
        scratch_shapes=[pltpu.VMEM((cx, cy, cz), f32), pltpu.SemaphoreType.DMA((13,))],
    )(rhs, accumulation, permeability, *flats)
    kx_low = lax.ppermute(kx_last, "gx", up_x)
    kx_high = lax.ppermute(kx_first, "gx", down_x)
    before = lax.ppermute(top, "gy", up_y)
    after = lax.ppermute(bottom, "gy", down_y)
    a8 = lax.all_to_all(a8, "gz", 0, 0, tiled=True)
    faces, group = pl.pallas_call(
        relay_kernel,
        out_shape=(struct(FACE_ROWS, cz), struct(tiles * LIST_ROWS, cz)),
        in_specs=[SMEM, VMEM],
        out_specs=(VMEM,) * 2,
        compiler_params=PARAMS,
    )(l, a8)
    small = FACE_ROWS + 2 * cy
    below, above = pl.pallas_call(
        join_kernel,
        out_shape=(struct(small, cz), struct(small + tiles * LIST_ROWS, cz)),
        in_specs=[VMEM] * 4,
        out_specs=(VMEM,) * 2,
        compiler_params=PARAMS,
    )(faces, group, kx_low, kx_high)
    below = lax.ppermute(below, "gy", up_y)
    above = lax.ppermute(above, "gy", down_y)

    big = struct(cx, ye, cz)
    tall = struct(cx + 1, ye, cz)
    edge = struct(ye, cz)
    small = struct(cx, cy, cz)
    sent = struct(tiles, FACE_ROWS + 4 * SLOT_ROWS, cz)
    scratch = [pltpu.VMEM((4, cx, cz), f32)]
    every = tiles * slots
    lists = (struct(2, 8, slots), struct(2, cz, every, dtype=bf16), struct(2, every))
    inv, z, d, tx, tym, typ, tzm, tzp, d_first, d_last, a8, row, pick, far_x = pl.pallas_call(
        setup_kernel,
        out_shape=(big, big, big, tall, big, big, big, big, edge, edge, sent) + lists,
        in_specs=[SMEM] + [VMEM] * 10,
        out_specs=(VMEM,) * 14,
        scratch_shapes=scratch * 2,
        compiler_params=PARAMS,
    )(l, rhs, accumulation, permeability, before, after, below, above, kx_low, kx_high, a8)

    rho = 1.0 / sigma
    corr = None
    for sweep in range(1, SWEEPS):
        first, last = sweep == 1, sweep == SWEEPS - 1
        rho_next = 1.0 / (2.0 * sigma - rho)
        c1, c2 = rho_next * rho, 2.0 * rho_next / delta
        rho = rho_next
        xlow = lax.ppermute(d_last, "gx", up_x)
        xhigh = lax.ppermute(d_first, "gx", down_x)
        a8 = lax.all_to_all(a8, "gz", 0, 0, tiled=True)
        fault = pl.pallas_call(
            fault_kernel,
            out_shape=struct(4, cx, cz),
            in_specs=[VMEM] * 4,
            out_specs=VMEM,
            compiler_params=PARAMS,
        )(a8, row, pick, far_x)
        args = [l, d, z] + ([] if first else [corr])
        args += [xlow, xhigh, a8, fault, inv, tx, tym, typ, tzm, tzp]
        args += [] if last else [row, pick, far_x]

        def kernel(*refs, c1=c1, c2=c2, first=first, last=last):
            sweep_kernel(c1, c2, first, last, *refs)

        out = pl.pallas_call(
            kernel,
            out_shape=small if last else (big, big, small, edge, edge, sent),
            in_specs=[SMEM] + [VMEM] * (len(args) - 1),
            out_specs=VMEM if last else (VMEM,) * 6,
            scratch_shapes=[] if last else scratch,
            compiler_params=PARAMS,
        )(*args)
        if last:
            corr = out
        else:
            d, z, corr, d_first, d_last, a8 = out
    return corr


def solution(mesh):
    split = P("gx", "gy", "gz")
    slots = P("gx", "gy", "gz", None)
    return jax.shard_map(
        local,
        mesh=mesh,
        in_specs=(split, split, P(None, "gx", "gy", "gz"), slots, slots, slots, slots),
        out_specs=split,
        check_vma=False,
    )
```

```python
import jax
import jax.numpy as jnp
from jax import lax
from jax.experimental import pallas as pl
from jax.experimental.pallas import tpu as pltpu
from jax.sharding import PartitionSpec as P

SWEEPS = 6
lam_low = 0.1
lam_high = 2.0
theta = (lam_high + lam_low) / 2.0
delta = (lam_high - lam_low) / 2.0
sigma = theta / delta

SLOT_ROWS = 4
LIST_ROWS = 24
H = 8
f32 = jnp.float32
bf16 = jnp.bfloat16


def harmonic(left, right):
    total = left + right
    live = total > 0.0
    return jnp.where(live, 2.0 * (left * right) / jnp.where(live, total, 1.0), 0.0)


def split3(v):
    hi = v.astype(bf16).astype(f32)
    rest = v - hi
    mid = rest.astype(bf16).astype(f32)
    return hi, mid, rest - mid


def dot(a, b, dims):
    return lax.dot_general(a, b, (dims, ((), ())), preferred_element_type=f32)


def lane_iota(shape):
    return lax.broadcasted_iota(jnp.int32, shape, len(shape) - 1)


def rows_hit(codes, count):
    shape = (count, codes.shape[1])
    return lax.broadcasted_iota(jnp.int32, shape, 0).astype(f32) == codes


def picks(codes):
    return jnp.where(rows_hit(codes, 128), 1.0, 0.0).astype(bf16)


def thirds(out):
    n = out.shape[0] // 3
    return out[:n] + out[n : 2 * n] + out[2 * n :]


def gather(table, pick, x_hit):
    parts = jnp.concatenate(split3(table), axis=0).astype(bf16)
    got = thirds(dot(parts, pick, ((1,), (0,))))
    return jnp.sum(jnp.where(x_hit, got, 0.0), axis=0, keepdims=True)


def scatter(u, pick, x_hit):
    parts = [jnp.where(x_hit, p, 0.0) for p in split3(u)]
    return thirds(dot(jnp.concatenate(parts, axis=0).astype(bf16), pick, ((1,), (1,))))


def get_rows(ref, t, base, count):
    return jnp.concatenate([ref[t, base + k : base + k + 1, :] for k in range(count)], axis=1)


def put_rows(ref, t, base, values):
    for k in range(values.shape[1] // 128):
        ref[t, base + k : base + k + 1, :] = values[:, 128 * k : 128 * (k + 1)]


NEAR_Z, NEAR_X, WEIGHT, FAR_X, FAR_TILE, FAR_Z = range(6)


def slot_row(row_ref, q, which):
    return row_ref[q, which : which + 1, :]


FACE_ROWS = 16
BOTH_ROWS = 24


def pack_faces(faces, tiles, x):
    faces = list(faces)
    lane = lane_iota((8, 128))
    for half in range(2):
        at = 64 * half + 2 * x + 2
        here = ((lane - (at - 1)) & 127) < 2
        for n in range(3):
            tile = tiles[3 * half + n]
            if tile is not None:
                faces[n] = jnp.where(here, pltpu.roll(tile, at % 128, 1), faces[n])
    return tuple(faces)


def no_faces():
    return (jnp.zeros((8, 128), f32),) * 3


def y_tiles(slab):
    return [slab[8 * n : 8 * (n + 1)] for n in range(slab.shape[0] // 8)]


def put_faces(l, ref, faces):
    odd = (lane_iota((8, 128)) & 1) == 1
    first, second, third = faces
    above = jnp.where(odd, first, pltpu.roll(second, 127, 1))
    below = jnp.where(odd, pltpu.roll(second, 1, 1), first)
    for t in range(ref.shape[0]):
        ref[t, 0:8, :] = jnp.where(t > l, above, below)
        ref[t, 8:16, :] = third


def get_faces(l, ref):
    tiles = ref.shape[0]
    low = jnp.where(l > 0, ref[jnp.maximum(l - 1, 0), 0:16, :], 0.0)
    high = jnp.where(l < tiles - 1, ref[jnp.minimum(l + 1, tiles - 1), 0:16, :], 0.0)
    odd = (lane_iota((8, 128)) & 1) == 1
    high = pltpu.roll(high, 126, 1)
    first = jnp.where(odd, low[0:8], high[0:8])
    second = jnp.where(odd, pltpu.roll(low[0:8], 1, 1), pltpu.roll(high[0:8], 127, 1))
    third = jnp.where(odd, low[8:16], high[8:16])
    return jnp.concatenate([first, second, third], axis=0)


def unpacked(faces, slab, x):
    lane = lane_iota((8, 128))
    lows, highs = [], []
    for n, tile in enumerate(y_tiles(slab)):
        packed = faces[8 * (n % 3) : 8 * (n % 3) + 8]
        outer = pltpu.roll(packed, (127 - 64 * (n // 3) - 2 * x) % 128, 1)
        lows.append(jnp.where(lane == 0, outer, pltpu.roll(tile, 1, 1)))
        highs.append(jnp.where(lane == 127, outer, pltpu.roll(tile, 127, 1)))
    return jnp.concatenate(lows, axis=0), jnp.concatenate(highs, axis=0)


def pack_kernel(l_ref, rhs, acc, perm, cell, remote, mask, trans,
                top, bottom, a8, kx_first, kx_last, kz, sem):
    tiles = a8.shape[0]
    cx, cy = rhs.shape[0], rhs.shape[1]
    sources = [rhs, acc] + [perm.at[n] for n in range(3)]
    moves = [pltpu.make_async_copy(perm.at[2], kz, sem.at[0])]
    for n, source in enumerate(sources):
        moves.append(pltpu.make_async_copy(source.at[:, cy - H :, :], top.at[n], sem.at[1 + 2 * n]))
        moves.append(pltpu.make_async_copy(source.at[:, :H, :], bottom.at[n], sem.at[2 + 2 * n]))
    count = 2 * len(sources) + 1
    moves.append(pltpu.make_async_copy(perm.at[0, 0], kx_first, sem.at[count]))
    moves.append(pltpu.make_async_copy(perm.at[0, cx - 1], kx_last, sem.at[count + 1]))
    for move in moves:
        move.start()
    weight = trans[...] * mask[...].astype(f32)
    own, far = cell[...], remote[...]
    column = tiles * 128
    far_z = far & (column - 1)
    table = [
        (own & 127).astype(f32),
        (own >> 7).astype(f32),
        weight,
        (far >> (column.bit_length() - 1)).astype(f32),
        (far_z >> 7).astype(f32),
        (far_z & 127).astype(f32),
    ]
    for n, values in enumerate(table):
        for t in range(tiles):
            put_rows(a8, t, FACE_ROWS + n * SLOT_ROWS, values)
    moves[0].wait()

    def body(x, faces):
        return pack_faces(faces, [None] + y_tiles(kz[x]) + [None], x)

    put_faces(l_ref[0], a8, lax.fori_loop(0, cx, body, no_faces(), unroll=4))
    for move in moves[1:]:
        move.wait()


def relay_kernel(l_ref, a8, faces, lists):
    tiles = a8.shape[0]
    l = l_ref[0]
    faces[...] = get_faces(l, a8)
    for t in range(tiles):
        lists[LIST_ROWS * t : LIST_ROWS * (t + 1), :] = a8[t, FACE_ROWS:, :]


def join_kernel(faces, lists, kx_low, kx_high, up, down):
    cy = kx_low.shape[0]
    base = BOTH_ROWS
    for out in (up, down):
        out[0:base, :] = faces[...]
        out[base : base + cy, :] = kx_low[...]
        out[base + cy : base + 2 * cy, :] = kx_high[...]
    down[base + 2 * cy :, :] = lists[...]


def emit(l_ref, a8_ref, planes, faces, row_ref, pick_ref, far_x):
    tiles = a8_ref.shape[0]
    cx = planes.shape[1]
    slots = row_ref.shape[2]
    put_faces(l_ref[0], a8_ref, faces)
    for q in range(2):
        base = FACE_ROWS + q * 2 * SLOT_ROWS
        near = gather(
            planes[2 * q + 1], picks(slot_row(row_ref, q, NEAR_Z)), rows_hit(slot_row(row_ref, q, NEAR_X), cx)
        )
        near = slot_row(row_ref, q, WEIGHT) * near
        for t in range(tiles):
            at = slice(t * slots, (t + 1) * slots)
            far = gather(planes[2 * q], pick_ref[q, :, at], rows_hit(far_x[q : q + 1, at], cx))
            put_rows(a8_ref, t, base, near)
            put_rows(a8_ref, t, base + SLOT_ROWS, far)


def keep_planes(planes, slab, x):
    last = slab.shape[0] - H - 1
    for n, y in enumerate((H - 1, H, last, last + 1)):
        planes[n, pl.ds(x, 1), :] = slab[y : y + 1, :]


def with_fault(total, fault, x):
    tiles = y_tiles(total)
    y = lax.broadcasted_iota(jnp.int32, tiles[0].shape, 0)
    last = total.shape[0] - H - 1
    for n, at in enumerate((H - 1, H, last, last + 1)):
        tiles[at // 8] += jnp.where(y == at % 8, fault[n, pl.ds(x, 1), :], 0.0)
    return jnp.concatenate(tiles, axis=0)


def near_sum(row_ref, q, values, cx):
    return scatter(
        values, picks(slot_row(row_ref, q, NEAR_Z)), rows_hit(slot_row(row_ref, q, NEAR_X), cx)
    )


def weights(l, a8, above, row_ref, pick_ref, far_x, fault):
    tiles = a8.shape[0]
    cx = fault.shape[1]
    slots = row_ref.shape[2]
    first = above.shape[0] - tiles * LIST_ROWS

    def codes(block):
        parts = [block[n : n + 1] for n in range(LIST_ROWS)]
        return [
            jnp.concatenate(parts[SLOT_ROWS * n : SLOT_ROWS * (n + 1)], axis=1) for n in range(6)
        ]

    def block(q, t):
        if q == 0:
            return a8[t, FACE_ROWS : FACE_ROWS + LIST_ROWS, :]
        return above[pl.ds(pl.multiple_of(first + t * LIST_ROWS, 8), LIST_ROWS), :]

    for q in range(2):
        mine = codes(block(q, l))
        for n in range(3):
            row_ref[q, n : n + 1, :] = mine[n]
        far = jnp.zeros((cx, 128), f32)
        for t in range(tiles):
            at = slice(t * slots, (t + 1) * slots)
            table = codes(block(q, t))
            x = jnp.where(table[FAR_TILE] == l.astype(f32), table[FAR_X], -1.0)
            pick = picks(table[FAR_Z])
            pick_ref[q, :, at] = pick
            far_x[q : q + 1, at] = x
            far = far + scatter(table[WEIGHT], pick, rows_hit(x, cx))
        fault[2 * q] = far
        fault[2 * q + 1] = near_sum(row_ref, q, slot_row(row_ref, q, WEIGHT), cx)


def fault_kernel(a8, row_ref, pick_ref, far_x, fault):
    tiles, rows = a8.shape[0], a8.shape[1]
    cx = fault.shape[1]
    slots = row_ref.shape[2]
    for q in range(2):
        base = rows - (2 - q) * 2 * SLOT_ROWS
        far = jnp.zeros((cx, 128), f32)
        near = jnp.zeros((1, slots), f32)
        for t in range(tiles):
            at = slice(t * slots, (t + 1) * slots)
            values = get_rows(a8, t, base, SLOT_ROWS)
            far = far + scatter(values, pick_ref[q, :, at], rows_hit(far_x[q : q + 1, at], cx))
            near = near + get_rows(a8, t, base + SLOT_ROWS, SLOT_ROWS)
        fault[2 * q] = far
        fault[2 * q + 1] = near_sum(row_ref, q, slot_row(row_ref, q, WEIGHT) * near, cx)


def setup_kernel(l_ref, rhs, acc, perm, before, after, below, above, kx_low, kx_high, a8,
                 inv, z_out, d_out, tx, tym, typ, tzm, tzp, d_first, d_last, a8_out,
                 row_ref, pick_ref, far_x, planes, fault):
    cx, cy = rhs.shape[0], rhs.shape[1]
    ye = cy + 2 * H
    l = l_ref[0]
    weights(l, a8, above, row_ref, pick_ref, far_x, fault)
    own = get_faces(l, a8)
    left = lane_iota((8, 128)) < 64
    faces_in = jnp.concatenate(
        [
            jnp.where(left, pltpu.roll(below[8:16, :], 64, 1), own[0:8]),
            own[8:16],
            jnp.where(left, own[16:24], pltpu.roll(above[8:16, :], 64, 1)),
        ],
        axis=0,
    )

    def ext_face(n, own):
        at = BOTH_ROWS + n * cy
        return jnp.concatenate([below[at + cy - H : at + cy, :], own[...], above[at : at + H, :]], axis=0)

    kx_under, kx_over = ext_face(0, kx_low), ext_face(1, kx_high)

    def ext(a, own, x):
        return jnp.concatenate([before[a, x], own, after[a, x]], axis=0)

    def body(x, carry):
        faces, t_low, kx = carry
        nxt = jnp.minimum(x + 1, cx - 1)
        kx_next = jnp.where(x == cx - 1, kx_over, ext(2, perm[0, nxt], nxt))
        ky = ext(3, perm[1, x], x)
        kz = ext(4, perm[2, x], x)
        t_high = harmonic(kx, kx_next)
        ym = harmonic(ky, pltpu.roll(ky, 1, 0))
        yp = harmonic(ky, pltpu.roll(ky, ye - 1, 0))
        kz_low, kz_high = unpacked(faces_in, kz, x)
        zm = harmonic(kz, kz_low)
        zp = harmonic(kz, kz_high)
        diag = ext(1, acc[x], x) + t_low + t_high + ym + yp + zm + zp
        diag = with_fault(diag, fault, x)
        live = diag > 0.0
        inverse = jnp.where(live, 1.0 / jnp.where(live, diag, 1.0), 0.0)
        z = inverse * ext(0, rhs[x], x)
        d = z / theta
        inv[x] = inverse
        z_out[x] = z
        d_out[x] = d
        tx[x] = t_low
        tx[x + 1] = t_high
        tym[x] = ym
        typ[x] = yp
        tzm[x] = zm
        tzp[x] = zp
        keep_planes(planes, d, x)
        return pack_faces(faces, y_tiles(d), x), t_high, kx_next

    kx0 = ext(2, perm[0, 0], 0)
    init = (no_faces(), harmonic(kx_under, kx0), kx0)
    faces, _, _ = lax.fori_loop(0, cx, body, init, unroll=4)
    d_first[...] = d_out[0]
    d_last[...] = d_out[cx - 1]
    emit(l_ref, a8_out, planes, faces, row_ref, pick_ref, far_x)


def sweep_kernel(c1, c2, first, last, l_ref, d_in, z_in, *refs):
    refs = list(refs)
    corr_in = None if first else refs.pop(0)
    xlow, xhigh, a8, fault, inv, tx, tym, typ, tzm, tzp = refs[:10]
    refs = refs[10:]
    if not last:
        row_ref, pick_ref, far_x = refs[:3]
        refs = refs[3:]
    outs = refs
    if last:
        (corr_out,) = outs
    else:
        d_out, z_out, corr_out, d_first, d_last, a8_out, planes = outs
    cx, ye = d_in.shape[0], d_in.shape[1]
    cy = ye - 2 * H
    faces_in = get_faces(l_ref[0], a8)

    def body(x, carry):
        faces, d_prev, d, t_low = carry
        t_high = tx[x + 1]
        d_next = jnp.where(x == cx - 1, xhigh[...], d_in[jnp.minimum(x + 1, cx - 1)])
        z_low, z_high = unpacked(faces_in, d, x)
        flow = t_low * d_prev + t_high * d_next
        flow = flow + (tym[x] * pltpu.roll(d, 1, 0) + typ[x] * pltpu.roll(d, ye - 1, 0))
        flow = flow + (tzm[x] * z_low + tzp[x] * z_high)
        flow = with_fault(flow, fault, x)
        z = z_in[x] - d + inv[x] * flow
        new = c1 * d + c2 * z
        before = d[H : H + cy] if first else corr_in[x]
        corr_out[x] = before + new[H : H + cy]
        if last:
            return faces, d, d_next, t_high
        d_out[x] = new
        z_out[x] = z
        keep_planes(planes, new, x)
        return pack_faces(faces, y_tiles(new), x), d, d_next, t_high

    init = (no_faces(), xlow[...], d_in[0], tx[0])
    faces, _, _, _ = lax.fori_loop(0, cx, body, init, unroll=4)
    if not last:
        d_first[...] = d_out[0]
        d_last[...] = d_out[cx - 1]
        emit(l_ref, a8_out, planes, faces, row_ref, pick_ref, far_x)


VMEM = pl.BlockSpec(memory_space=pltpu.VMEM)
SMEM = pl.BlockSpec(memory_space=pltpu.SMEM)
HBM = pl.BlockSpec(memory_space=pltpu.HBM)
PARAMS = pltpu.CompilerParams(vmem_limit_bytes=24 << 20)


def steps(axis):
    peers = lax.axis_size(axis)
    up = [(i, i + 1) for i in range(peers - 1)]
    return up, [(j, i) for i, j in up]


def local(rhs, accumulation, permeability, nnc_cell, nnc_remote, nnc_mask, nnc_trans):
    cx, cy, cz = rhs.shape
    tiles = lax.axis_size("gz")
    slots = nnc_cell.shape[-1]
    ye = cy + 2 * H
    up_y, down_y = steps("gy")
    up_x, down_x = steps("gx")

    def struct(*shape, dtype=f32):
        return jax.ShapeDtypeStruct(shape, dtype)

    l = lax.axis_index("gz").reshape(1).astype(jnp.int32)
    flats = [a.reshape(1, slots) for a in (nnc_cell, nnc_remote, nnc_mask, nnc_trans)]
    l, *flats = lax.optimization_barrier((l, *flats))
    halo = struct(5, cx, H, cz)
    top, bottom, a8, kx_first, kx_last = pl.pallas_call(
        pack_kernel,
        out_shape=(halo, halo, struct(tiles, FACE_ROWS + LIST_ROWS, cz), struct(cy, cz), struct(cy, cz)),
        in_specs=[SMEM] + [HBM] * 3 + [VMEM] * 4,
        out_specs=(VMEM,) * 5,
        scratch_shapes=[pltpu.VMEM((cx, cy, cz), f32), pltpu.SemaphoreType.DMA((13,))],
    )(l, rhs, accumulation, permeability, *flats)
    kx_low = lax.ppermute(kx_last, "gx", up_x)
    kx_high = lax.ppermute(kx_first, "gx", down_x)
    before = lax.ppermute(top, "gy", up_y)
    after = lax.ppermute(bottom, "gy", down_y)
    a8 = lax.all_to_all(a8, "gz", 0, 0, tiled=True)
    faces, group = pl.pallas_call(
        relay_kernel,
        out_shape=(struct(BOTH_ROWS, cz), struct(tiles * LIST_ROWS, cz)),
        in_specs=[SMEM, VMEM],
        out_specs=(VMEM,) * 2,
        compiler_params=PARAMS,
    )(l, a8)
    small = BOTH_ROWS + 2 * cy
    below, above = pl.pallas_call(
        join_kernel,
        out_shape=(struct(small, cz), struct(small + tiles * LIST_ROWS, cz)),
        in_specs=[VMEM] * 4,
        out_specs=(VMEM,) * 2,
        compiler_params=PARAMS,
    )(faces, group, kx_low, kx_high)
    below = lax.ppermute(below, "gy", up_y)
    above = lax.ppermute(above, "gy", down_y)

    big = struct(cx, ye, cz)
    tall = struct(cx + 1, ye, cz)
    edge = struct(ye, cz)
    small = struct(cx, cy, cz)
    sent = struct(tiles, FACE_ROWS + 4 * SLOT_ROWS, cz)
    scratch = [pltpu.VMEM((4, cx, cz), f32)]
    every = tiles * slots
    lists = (struct(2, 8, slots), struct(2, cz, every, dtype=bf16), struct(2, every))
    inv, z, d, tx, tym, typ, tzm, tzp, d_first, d_last, a8, row, pick, far_x = pl.pallas_call(
        setup_kernel,
        out_shape=(big, big, big, tall, big, big, big, big, edge, edge, sent) + lists,
        in_specs=[SMEM] + [VMEM] * 10,
        out_specs=(VMEM,) * 14,
        scratch_shapes=scratch * 2,
        compiler_params=PARAMS,
    )(l, rhs, accumulation, permeability, before, after, below, above, kx_low, kx_high, a8)

    rho = 1.0 / sigma
    corr = None
    for sweep in range(1, SWEEPS):
        first, last = sweep == 1, sweep == SWEEPS - 1
        rho_next = 1.0 / (2.0 * sigma - rho)
        c1, c2 = rho_next * rho, 2.0 * rho_next / delta
        rho = rho_next
        xlow = lax.ppermute(d_last, "gx", up_x)
        xhigh = lax.ppermute(d_first, "gx", down_x)
        a8 = lax.all_to_all(a8, "gz", 0, 0, tiled=True)
        fault = pl.pallas_call(
            fault_kernel,
            out_shape=struct(4, cx, cz),
            in_specs=[VMEM] * 4,
            out_specs=VMEM,
            compiler_params=PARAMS,
        )(a8, row, pick, far_x)
        args = [l, d, z] + ([] if first else [corr])
        args += [xlow, xhigh, a8, fault, inv, tx, tym, typ, tzm, tzp]
        args += [] if last else [row, pick, far_x]

        def kernel(*refs, c1=c1, c2=c2, first=first, last=last):
            sweep_kernel(c1, c2, first, last, *refs)

        out = pl.pallas_call(
            kernel,
            out_shape=small if last else (big, big, small, edge, edge, sent),
            in_specs=[SMEM] + [VMEM] * (len(args) - 1),
            out_specs=VMEM if last else (VMEM,) * 6,
            scratch_shapes=[] if last else scratch,
            compiler_params=PARAMS,
        )(*args)
        if last:
            corr = out
        else:
            d, z, corr, d_first, d_last, a8 = out
    return corr


def solution(mesh):
    split = P("gx", "gy", "gz")
    slots = P("gx", "gy", "gz", None)
    return jax.shard_map(
        local,
        mesh=mesh,
        in_specs=(split, split, P(None, "gx", "gy", "gz"), slots, slots, slots, slots),
        out_specs=split,
        check_vma=False,
    )
```

```python
import jax
import jax.numpy as jnp
from jax import lax
from jax.experimental import pallas as pl
from jax.experimental.pallas import tpu as pltpu
from jax.sharding import PartitionSpec as P

SWEEPS = 6
lam_low = 0.1
lam_high = 2.0
theta = (lam_high + lam_low) / 2.0
delta = (lam_high - lam_low) / 2.0
sigma = theta / delta

SLOT_ROWS = 4
LIST_ROWS = 24
H = 8
f32 = jnp.float32
bf16 = jnp.bfloat16


def harmonic(left, right):
    total = left + right
    live = total > 0.0
    return jnp.where(live, 2.0 * (left * right) / jnp.where(live, total, 1.0), 0.0)


def split3(v):
    hi = v.astype(bf16).astype(f32)
    rest = v - hi
    mid = rest.astype(bf16).astype(f32)
    return hi, mid, rest - mid


def dot(a, b, dims):
    return lax.dot_general(a, b, (dims, ((), ())), preferred_element_type=f32)


def lane_iota(shape):
    return lax.broadcasted_iota(jnp.int32, shape, len(shape) - 1)


def rows_hit(codes, count):
    shape = (count, codes.shape[1])
    return lax.broadcasted_iota(jnp.int32, shape, 0).astype(f32) == codes


def picks(codes):
    return jnp.where(rows_hit(codes, 128), 1.0, 0.0).astype(bf16)


def thirds(out):
    n = out.shape[0] // 3
    return out[:n] + out[n : 2 * n] + out[2 * n :]


def gather(table, pick, x_hit):
    parts = jnp.concatenate(split3(table), axis=0).astype(bf16)
    got = thirds(dot(parts, pick, ((1,), (0,))))
    return jnp.sum(jnp.where(x_hit, got, 0.0), axis=0, keepdims=True)


def scatter(u, pick, x_hit):
    parts = [jnp.where(x_hit, p, 0.0) for p in split3(u)]
    return thirds(dot(jnp.concatenate(parts, axis=0).astype(bf16), pick, ((1,), (1,))))


def get_rows(ref, t, base, count):
    return jnp.concatenate([ref[t, base + k : base + k + 1, :] for k in range(count)], axis=1)


def put_rows(ref, t, base, values):
    for k in range(values.shape[1] // 128):
        ref[t, base + k : base + k + 1, :] = values[:, 128 * k : 128 * (k + 1)]


NEAR_Z, NEAR_X, WEIGHT, FAR_X, FAR_TILE, FAR_Z = range(6)


def slot_row(row_ref, q, which):
    return row_ref[q, which : which + 1, :]


FACE_ROWS = 16
BOTH_ROWS = 24


def pack_faces(faces, tiles, x):
    faces = list(faces)
    lane = lane_iota((8, 128))
    for half in range(2):
        at = 64 * half + 2 * x + 2
        here = ((lane - (at - 1)) & 127) < 2
        for n in range(3):
            tile = tiles[3 * half + n]
            if tile is not None:
                faces[n] = jnp.where(here, pltpu.roll(tile, at % 128, 1), faces[n])
    return tuple(faces)


def no_faces():
    return (jnp.zeros((8, 128), f32),) * 3


def y_tiles(slab):
    return [slab[8 * n : 8 * (n + 1)] for n in range(slab.shape[0] // 8)]


def put_faces(l, ref, faces):
    odd = (lane_iota((8, 128)) & 1) == 1
    first, second, third = faces
    above = jnp.where(odd, first, pltpu.roll(second, 127, 1))
    below = jnp.where(odd, pltpu.roll(second, 1, 1), first)
    for t in range(ref.shape[0]):
        ref[t, 0:8, :] = jnp.where(t > l, above, below)
        ref[t, 8:16, :] = third


def get_faces(l, ref):
    tiles = ref.shape[0]
    low = jnp.where(l > 0, ref[jnp.maximum(l - 1, 0), 0:16, :], 0.0)
    high = jnp.where(l < tiles - 1, ref[jnp.minimum(l + 1, tiles - 1), 0:16, :], 0.0)
    odd = (lane_iota((8, 128)) & 1) == 1
    high = pltpu.roll(high, 126, 1)
    first = jnp.where(odd, low[0:8], high[0:8])
    second = jnp.where(odd, pltpu.roll(low[0:8], 1, 1), pltpu.roll(high[0:8], 127, 1))
    third = jnp.where(odd, low[8:16], high[8:16])
    return jnp.concatenate([first, second, third], axis=0)


def unpacked(faces, slab, x):
    lane = lane_iota((8, 128))
    lows, highs = [], []
    for n, tile in enumerate(y_tiles(slab)):
        packed = faces[8 * (n % 3) : 8 * (n % 3) + 8]
        outer = pltpu.roll(packed, (127 - 64 * (n // 3) - 2 * x) % 128, 1)
        lows.append(jnp.where(lane == 0, outer, pltpu.roll(tile, 1, 1)))
        highs.append(jnp.where(lane == 127, outer, pltpu.roll(tile, 127, 1)))
    return jnp.concatenate(lows, axis=0), jnp.concatenate(highs, axis=0)


def pack_kernel(l_ref, rhs, acc, perm, cell_in, remote_in, mask_in, trans_in,
                top, bottom, a8, kz, cell, remote, mask, trans, sem):
    tiles = a8.shape[0]
    cx, cy = rhs.shape[0], rhs.shape[1]
    sources = [rhs, acc] + [perm.at[n] for n in range(3)]
    moves = [pltpu.make_async_copy(perm.at[2], kz, sem.at[0])]
    for n, source in enumerate(sources):
        moves.append(pltpu.make_async_copy(source.at[:, cy - H :, :], top.at[n], sem.at[1 + 2 * n]))
        moves.append(pltpu.make_async_copy(source.at[:, :H, :], bottom.at[n], sem.at[2 + 2 * n]))
    count = 2 * len(sources) + 1
    slots = ((cell_in, cell), (remote_in, remote), (mask_in, mask), (trans_in, trans))
    lists = [pltpu.make_async_copy(a, b, sem.at[count + n]) for n, (a, b) in enumerate(slots)]
    for move in lists + moves:
        move.start()
    for move in lists:
        move.wait()
    weight = trans[...] * mask[...].astype(f32)
    own, far = cell[...], remote[...]
    column = tiles * 128
    far_z = far & (column - 1)
    table = [
        (own & 127).astype(f32),
        (own >> 7).astype(f32),
        weight,
        (far >> (column.bit_length() - 1)).astype(f32),
        (far_z >> 7).astype(f32),
        (far_z & 127).astype(f32),
    ]
    for n, values in enumerate(table):
        for t in range(tiles):
            put_rows(a8, t, FACE_ROWS + n * SLOT_ROWS, values)
    moves[0].wait()

    def body(x, faces):
        return pack_faces(faces, [None] + y_tiles(kz[x]) + [None], x)

    put_faces(l_ref[0], a8, lax.fori_loop(0, cx, body, no_faces(), unroll=4))
    for move in moves[1:]:
        move.wait()


def relay_kernel(l_ref, a8, up, down):
    tiles = a8.shape[0]
    faces = get_faces(l_ref[0], a8)
    up[...] = faces
    down[0:BOTH_ROWS, :] = faces
    for t in range(tiles):
        at = BOTH_ROWS + LIST_ROWS * t
        down[at : at + LIST_ROWS, :] = a8[t, FACE_ROWS:, :]


def emit(l_ref, a8_ref, planes, faces, row_ref, pick_ref, far_x):
    tiles = a8_ref.shape[0]
    cx = planes.shape[1]
    slots = row_ref.shape[2]
    put_faces(l_ref[0], a8_ref, faces)
    for q in range(2):
        base = FACE_ROWS + q * 2 * SLOT_ROWS
        near = gather(
            planes[2 * q + 1], picks(slot_row(row_ref, q, NEAR_Z)), rows_hit(slot_row(row_ref, q, NEAR_X), cx)
        )
        near = slot_row(row_ref, q, WEIGHT) * near
        for t in range(tiles):
            at = slice(t * slots, (t + 1) * slots)
            far = gather(planes[2 * q], pick_ref[q, :, at], rows_hit(far_x[q : q + 1, at], cx))
            put_rows(a8_ref, t, base, near)
            put_rows(a8_ref, t, base + SLOT_ROWS, far)


def keep_planes(planes, slab, x):
    last = slab.shape[0] - H - 1
    for n, y in enumerate((H - 1, H, last, last + 1)):
        planes[n, pl.ds(x, 1), :] = slab[y : y + 1, :]


def with_fault(total, fault, x):
    tiles = y_tiles(total)
    y = lax.broadcasted_iota(jnp.int32, tiles[0].shape, 0)
    last = total.shape[0] - H - 1
    for n, at in enumerate((H - 1, H, last, last + 1)):
        tiles[at // 8] += jnp.where(y == at % 8, fault[n, pl.ds(x, 1), :], 0.0)
    return jnp.concatenate(tiles, axis=0)


def near_sum(row_ref, q, values, cx):
    return scatter(
        values, picks(slot_row(row_ref, q, NEAR_Z)), rows_hit(slot_row(row_ref, q, NEAR_X), cx)
    )


def weights(l, a8, above, row_ref, pick_ref, far_x, fault):
    tiles = a8.shape[0]
    cx = fault.shape[1]
    slots = row_ref.shape[2]
    first = above.shape[0] - tiles * LIST_ROWS

    def codes(block):
        parts = [block[n : n + 1] for n in range(LIST_ROWS)]
        return [
            jnp.concatenate(parts[SLOT_ROWS * n : SLOT_ROWS * (n + 1)], axis=1) for n in range(6)
        ]

    def block(q, t):
        if q == 0:
            return a8[t, FACE_ROWS : FACE_ROWS + LIST_ROWS, :]
        return above[pl.ds(pl.multiple_of(first + t * LIST_ROWS, 8), LIST_ROWS), :]

    for q in range(2):
        mine = codes(block(q, l))
        for n in range(3):
            row_ref[q, n : n + 1, :] = mine[n]
        far = jnp.zeros((cx, 128), f32)
        for t in range(tiles):
            at = slice(t * slots, (t + 1) * slots)
            table = codes(block(q, t))
            x = jnp.where(table[FAR_TILE] == l.astype(f32), table[FAR_X], -1.0)
            pick = picks(table[FAR_Z])
            pick_ref[q, :, at] = pick
            far_x[q : q + 1, at] = x
            far = far + scatter(table[WEIGHT], pick, rows_hit(x, cx))
        fault[2 * q] = far
        fault[2 * q + 1] = near_sum(row_ref, q, slot_row(row_ref, q, WEIGHT), cx)


def fault_kernel(a8, row_ref, pick_ref, far_x, fault):
    tiles, rows = a8.shape[0], a8.shape[1]
    cx = fault.shape[1]
    slots = row_ref.shape[2]
    for q in range(2):
        base = rows - (2 - q) * 2 * SLOT_ROWS
        far = jnp.zeros((cx, 128), f32)
        near = jnp.zeros((1, slots), f32)
        for t in range(tiles):
            at = slice(t * slots, (t + 1) * slots)
            values = get_rows(a8, t, base, SLOT_ROWS)
            far = far + scatter(values, pick_ref[q, :, at], rows_hit(far_x[q : q + 1, at], cx))
            near = near + get_rows(a8, t, base + SLOT_ROWS, SLOT_ROWS)
        fault[2 * q] = far
        fault[2 * q + 1] = near_sum(row_ref, q, slot_row(row_ref, q, WEIGHT) * near, cx)


def extended(before, after, n, own, x):
    return jnp.concatenate([before[n, x], own, after[n, x]], axis=0)


def side_faces(ky, kz, faces, x):
    ye = ky.shape[0]
    low, high = unpacked(faces, kz, x)
    return (
        harmonic(ky, pltpu.roll(ky, 1, 0)),
        harmonic(ky, pltpu.roll(ky, ye - 1, 0)),
        harmonic(kz, low),
        harmonic(kz, high),
    )


def inverse_of(diag):
    live = diag > 0.0
    return jnp.where(live, 1.0 / jnp.where(live, diag, 1.0), 0.0)


def edge_kernel(l_ref, rhs, acc, perm, before, after, below, above, a8,
                fault, row_ref, pick_ref, far_x, faces, low_edge, high_edge):
    cx = rhs.shape[0]
    l = l_ref[0]
    weights(l, a8, above, row_ref, pick_ref, far_x, fault)
    own = get_faces(l, a8)
    left = lane_iota((8, 128)) < 64
    faces[0:8, :] = jnp.where(left, pltpu.roll(below[8:16, :], 64, 1), own[0:8])
    faces[8:16, :] = own[8:16]
    faces[16:24, :] = jnp.where(left, own[16:24], pltpu.roll(above[8:16, :], 64, 1))

    def slab(n, source, x):
        return extended(before, after, n, source[x], x)

    for edge, x, inner in ((low_edge, 0, 1), (high_edge, cx - 1, cx - 2)):
        kx, kx_inner = slab(2, perm.at[0], x), slab(2, perm.at[0], inner)
        sides = side_faces(slab(3, perm.at[1], x), slab(4, perm.at[2], x), faces[...], x)
        edge[0] = kx
        edge[1] = with_fault(slab(1, acc, x) + harmonic(kx, kx_inner) + sum(sides), fault, x)
        edge[2] = slab(0, rhs, x)


def setup_kernel(l_ref, rhs, acc, perm, before, after, faces_in, fault, low_edge, high_edge,
                 row_ref, pick_ref, far_x,
                 inv, z_out, d_out, tx, tym, typ, tzm, tzp, x_low, x_high, a8_out, planes):
    cx = rhs.shape[0]

    def ext(n, own, x):
        return extended(before, after, n, own, x)

    def body(x, carry):
        faces, t_low, kx = carry
        nxt = jnp.minimum(x + 1, cx - 1)
        kx_next = jnp.where(x == cx - 1, high_edge[0], ext(2, perm[0, nxt], nxt))
        t_high = harmonic(kx, kx_next)
        ym, yp, zm, zp = side_faces(ext(3, perm[1, x], x), ext(4, perm[2, x], x), faces_in[...], x)
        diag = ext(1, acc[x], x) + t_low + t_high + ym + yp + zm + zp
        inverse = inverse_of(with_fault(diag, fault, x))
        z = inverse * ext(0, rhs[x], x)
        d = z / theta
        inv[x] = inverse
        z_out[x] = z
        d_out[x] = d
        tx[x] = t_low
        tx[x + 1] = t_high
        tym[x] = ym
        typ[x] = yp
        tzm[x] = zm
        tzp[x] = zp
        keep_planes(planes, d, x)
        return pack_faces(faces, y_tiles(d), x), t_high, kx_next

    kx0 = ext(2, perm[0, 0], 0)
    init = (no_faces(), harmonic(low_edge[0], kx0), kx0)
    faces, _, _ = lax.fori_loop(0, cx, body, init, unroll=4)
    for out, edge, at in ((x_low, low_edge, 0), (x_high, high_edge, cx)):
        out[...] = inverse_of(edge[1] + tx[at]) * edge[2] / theta
    emit(l_ref, a8_out, planes, faces, row_ref, pick_ref, far_x)


def sweep_kernel(c1, c2, first, last, l_ref, d_in, z_in, *refs):
    refs = list(refs)
    corr_in = None if first else refs.pop(0)
    xlow, xhigh, a8, fault, inv, tx, tym, typ, tzm, tzp = refs[:10]
    refs = refs[10:]
    if not last:
        row_ref, pick_ref, far_x = refs[:3]
        refs = refs[3:]
    outs = refs
    if last:
        (corr_out,) = outs
    else:
        d_out, z_out, corr_out, d_first, d_last, a8_out, planes = outs
    cx, ye = d_in.shape[0], d_in.shape[1]
    cy = ye - 2 * H
    faces_in = get_faces(l_ref[0], a8)

    def body(x, carry):
        faces, d_prev, d, t_low = carry
        t_high = tx[x + 1]
        d_next = jnp.where(x == cx - 1, xhigh[...], d_in[jnp.minimum(x + 1, cx - 1)])
        z_low, z_high = unpacked(faces_in, d, x)
        flow = t_low * d_prev + t_high * d_next
        flow = flow + (tym[x] * pltpu.roll(d, 1, 0) + typ[x] * pltpu.roll(d, ye - 1, 0))
        flow = flow + (tzm[x] * z_low + tzp[x] * z_high)
        flow = with_fault(flow, fault, x)
        z = z_in[x] - d + inv[x] * flow
        new = c1 * d + c2 * z
        before = d[H : H + cy] if first else corr_in[x]
        corr_out[x] = before + new[H : H + cy]
        if last:
            return faces, d, d_next, t_high
        d_out[x] = new
        z_out[x] = z
        keep_planes(planes, new, x)
        return pack_faces(faces, y_tiles(new), x), d, d_next, t_high

    init = (no_faces(), xlow[...], d_in[0], tx[0])
    faces, _, _, _ = lax.fori_loop(0, cx, body, init, unroll=4)
    if not last:
        d_first[...] = d_out[0]
        d_last[...] = d_out[cx - 1]
        emit(l_ref, a8_out, planes, faces, row_ref, pick_ref, far_x)


VMEM = pl.BlockSpec(memory_space=pltpu.VMEM)
SMEM = pl.BlockSpec(memory_space=pltpu.SMEM)
HBM = pl.BlockSpec(memory_space=pltpu.HBM)
PARAMS = pltpu.CompilerParams(vmem_limit_bytes=24 << 20)


def steps(axis):
    peers = lax.axis_size(axis)
    up = [(i, i + 1) for i in range(peers - 1)]
    return up, [(j, i) for i, j in up]


def local(rhs, accumulation, permeability, nnc_cell, nnc_remote, nnc_mask, nnc_trans):
    cx, cy, cz = rhs.shape
    tiles = lax.axis_size("gz")
    slots = nnc_cell.shape[-1]
    ye = cy + 2 * H
    up_y, down_y = steps("gy")
    up_x, down_x = steps("gx")

    def struct(*shape, dtype=f32):
        return jax.ShapeDtypeStruct(shape, dtype)

    l = lax.axis_index("gz").reshape(1).astype(jnp.int32)
    flats = [a.reshape(1, slots) for a in (nnc_cell, nnc_remote, nnc_mask, nnc_trans)]
    l, *flats = lax.optimization_barrier((l, *flats))
    halo = struct(5, cx, H, cz)
    top, bottom, a8 = pl.pallas_call(
        pack_kernel,
        out_shape=(halo, halo, struct(tiles, FACE_ROWS + LIST_ROWS, cz)),
        in_specs=[SMEM] + [HBM] * 7,
        out_specs=(VMEM,) * 3,
        scratch_shapes=[pltpu.VMEM((cx, cy, cz), f32)]
        + [pltpu.VMEM((1, slots), jnp.int32)] * 3
        + [pltpu.VMEM((1, slots), f32), pltpu.SemaphoreType.DMA((15,))],
    )(l, rhs, accumulation, permeability, *flats)
    before = lax.ppermute(top, "gy", up_y)
    after = lax.ppermute(bottom, "gy", down_y)
    a8 = lax.all_to_all(a8, "gz", 0, 0, tiled=True)
    below, above = pl.pallas_call(
        relay_kernel,
        out_shape=(struct(BOTH_ROWS, cz), struct(BOTH_ROWS + tiles * LIST_ROWS, cz)),
        in_specs=[SMEM, VMEM],
        out_specs=(VMEM,) * 2,
        compiler_params=PARAMS,
    )(l, a8)
    below = lax.ppermute(below, "gy", up_y)
    above = lax.ppermute(above, "gy", down_y)

    big = struct(cx, ye, cz)
    tall = struct(cx + 1, ye, cz)
    edge = struct(ye, cz)
    small = struct(cx, cy, cz)
    sent = struct(tiles, FACE_ROWS + 4 * SLOT_ROWS, cz)
    scratch = [pltpu.VMEM((4, cx, cz), f32)]
    every = tiles * slots
    lists = (struct(2, 8, slots), struct(2, cz, every, dtype=bf16), struct(2, every))
    fault, row, pick, far_x, faces, low_edge, high_edge = pl.pallas_call(
        edge_kernel,
        out_shape=(struct(4, cx, cz),) + lists + (struct(BOTH_ROWS, cz),) + (struct(3, ye, cz),) * 2,
        in_specs=[SMEM] + [VMEM] * 8,
        out_specs=(VMEM,) * 7,
        compiler_params=PARAMS,
    )(l, rhs, accumulation, permeability, before, after, below, above, a8)
    low_got = lax.ppermute(high_edge, "gx", up_x)
    high_got = lax.ppermute(low_edge, "gx", down_x)
    inv, z, d, tx, tym, typ, tzm, tzp, xlow, xhigh, a8 = pl.pallas_call(
        setup_kernel,
        out_shape=(big, big, big, tall, big, big, big, big, edge, edge, sent),
        in_specs=[SMEM] + [VMEM] * 12,
        out_specs=(VMEM,) * 11,
        scratch_shapes=scratch,
        compiler_params=PARAMS,
    )(l, rhs, accumulation, permeability, before, after, faces, fault, low_got, high_got, row, pick, far_x)

    rho = 1.0 / sigma
    corr = None
    for sweep in range(1, SWEEPS):
        first, last = sweep == 1, sweep == SWEEPS - 1
        rho_next = 1.0 / (2.0 * sigma - rho)
        c1, c2 = rho_next * rho, 2.0 * rho_next / delta
        rho = rho_next
        if not first:
            xlow = lax.ppermute(d_last, "gx", up_x)
            xhigh = lax.ppermute(d_first, "gx", down_x)
        a8 = lax.all_to_all(a8, "gz", 0, 0, tiled=True)
        fault = pl.pallas_call(
            fault_kernel,
            out_shape=struct(4, cx, cz),
            in_specs=[VMEM] * 4,
            out_specs=VMEM,
            compiler_params=PARAMS,
        )(a8, row, pick, far_x)
        args = [l, d, z] + ([] if first else [corr])
        args += [xlow, xhigh, a8, fault, inv, tx, tym, typ, tzm, tzp]
        args += [] if last else [row, pick, far_x]

        def kernel(*refs, c1=c1, c2=c2, first=first, last=last):
            sweep_kernel(c1, c2, first, last, *refs)

        out = pl.pallas_call(
            kernel,
            out_shape=small if last else (big, big, small, edge, edge, sent),
            in_specs=[SMEM] + [VMEM] * (len(args) - 1),
            out_specs=VMEM if last else (VMEM,) * 6,
            scratch_shapes=[] if last else scratch,
            compiler_params=PARAMS,
        )(*args)
        if last:
            corr = out
        else:
            d, z, corr, d_first, d_last, a8 = out
    return corr


def solution(mesh):
    split = P("gx", "gy", "gz")
    slots = P("gx", "gy", "gz", None)
    return jax.shard_map(
        local,
        mesh=mesh,
        in_specs=(split, split, P(None, "gx", "gy", "gz"), slots, slots, slots, slots),
        out_specs=split,
        check_vma=False,
    )
```

```python
import jax
import jax.numpy as jnp
from jax import lax
from jax.experimental import pallas as pl
from jax.experimental.pallas import tpu as pltpu
from jax.sharding import PartitionSpec as P

SWEEPS = 6
lam_low = 0.1
lam_high = 2.0
theta = (lam_high + lam_low) / 2.0
delta = (lam_high - lam_low) / 2.0
sigma = theta / delta

SLOT_ROWS = 4
LIST_ROWS = 24
H = 8
f32 = jnp.float32
bf16 = jnp.bfloat16


def harmonic(left, right):
    total = left + right
    live = total > 0.0
    return jnp.where(live, 2.0 * (left * right) / jnp.where(live, total, 1.0), 0.0)


def split3(v):
    hi = v.astype(bf16).astype(f32)
    rest = v - hi
    mid = rest.astype(bf16).astype(f32)
    return hi, mid, rest - mid


def dot(a, b, dims):
    return lax.dot_general(a, b, (dims, ((), ())), preferred_element_type=f32)


def lane_iota(shape):
    return lax.broadcasted_iota(jnp.int32, shape, len(shape) - 1)


def rows_hit(codes, count):
    shape = (count, codes.shape[1])
    return lax.broadcasted_iota(jnp.int32, shape, 0).astype(f32) == codes


def picks(codes):
    return jnp.where(rows_hit(codes, 128), 1.0, 0.0).astype(bf16)


def thirds(out):
    n = out.shape[0] // 3
    return out[:n] + out[n : 2 * n] + out[2 * n :]


def gather(table, pick, x_hit):
    parts = jnp.concatenate(split3(table), axis=0).astype(bf16)
    got = thirds(dot(parts, pick, ((1,), (0,))))
    return jnp.sum(jnp.where(x_hit, got, 0.0), axis=0, keepdims=True)


def scatter(u, pick, x_hit):
    parts = [jnp.where(x_hit, p, 0.0) for p in split3(u)]
    return thirds(dot(jnp.concatenate(parts, axis=0).astype(bf16), pick, ((1,), (1,))))


def get_rows(ref, t, base, count):
    return jnp.concatenate([ref[t, base + k : base + k + 1, :] for k in range(count)], axis=1)


def put_rows(ref, t, base, values):
    for k in range(values.shape[1] // 128):
        ref[t, base + k : base + k + 1, :] = values[:, 128 * k : 128 * (k + 1)]


NEAR_Z, NEAR_X, WEIGHT, FAR_X, FAR_TILE, FAR_Z = range(6)


def slot_row(row_ref, q, which):
    return row_ref[q, which : which + 1, :]


FACE_ROWS = 16
BOTH_ROWS = 24


def pack_faces(faces, tiles, x):
    faces = list(faces)
    lane = lane_iota((8, 128))
    for half in range(2):
        at = 64 * half + 2 * x + 2
        here = ((lane - (at - 1)) & 127) < 2
        for n in range(3):
            tile = tiles[3 * half + n]
            if tile is not None:
                faces[n] = jnp.where(here, pltpu.roll(tile, at % 128, 1), faces[n])
    return tuple(faces)


def no_faces():
    return (jnp.zeros((8, 128), f32),) * 3


def y_tiles(slab):
    return [slab[8 * n : 8 * (n + 1)] for n in range(slab.shape[0] // 8)]


def put_faces(l, ref, faces):
    odd = (lane_iota((8, 128)) & 1) == 1
    first, second, third = faces
    above = jnp.where(odd, first, pltpu.roll(second, 127, 1))
    below = jnp.where(odd, pltpu.roll(second, 1, 1), first)
    for t in range(ref.shape[0]):
        ref[t, 0:8, :] = jnp.where(t > l, above, below)
        ref[t, 8:16, :] = third


def get_faces(l, ref):
    tiles = ref.shape[0]
    low = jnp.where(l > 0, ref[jnp.maximum(l - 1, 0), 0:16, :], 0.0)
    high = jnp.where(l < tiles - 1, ref[jnp.minimum(l + 1, tiles - 1), 0:16, :], 0.0)
    odd = (lane_iota((8, 128)) & 1) == 1
    high = pltpu.roll(high, 126, 1)
    first = jnp.where(odd, low[0:8], high[0:8])
    second = jnp.where(odd, pltpu.roll(low[0:8], 1, 1), pltpu.roll(high[0:8], 127, 1))
    third = jnp.where(odd, low[8:16], high[8:16])
    return jnp.concatenate([first, second, third], axis=0)


def unpacked(faces, slab, x):
    lane = lane_iota((8, 128))
    lows, highs = [], []
    for n, tile in enumerate(y_tiles(slab)):
        packed = faces[8 * (n % 3) : 8 * (n % 3) + 8]
        outer = pltpu.roll(packed, (127 - 64 * (n // 3) - 2 * x) % 128, 1)
        lows.append(jnp.where(lane == 0, outer, pltpu.roll(tile, 1, 1)))
        highs.append(jnp.where(lane == 127, outer, pltpu.roll(tile, 127, 1)))
    return jnp.concatenate(lows, axis=0), jnp.concatenate(highs, axis=0)


def pack_kernel(l_ref, rhs, acc, perm, cell_in, remote_in, mask_in, trans_in,
                top, bottom, a8, kz, cell, remote, mask, trans, sem):
    tiles = a8.shape[0]
    cx, cy = rhs.shape[0], rhs.shape[1]
    sources = [rhs, acc] + [perm.at[n] for n in range(3)]
    moves = [pltpu.make_async_copy(perm.at[2], kz, sem.at[0])]
    for n, source in enumerate(sources):
        moves.append(pltpu.make_async_copy(source.at[:, cy - H :, :], top.at[n], sem.at[1 + 2 * n]))
        moves.append(pltpu.make_async_copy(source.at[:, :H, :], bottom.at[n], sem.at[2 + 2 * n]))
    count = 2 * len(sources) + 1
    slots = ((cell_in, cell), (remote_in, remote), (mask_in, mask), (trans_in, trans))
    lists = [pltpu.make_async_copy(a, b, sem.at[count + n]) for n, (a, b) in enumerate(slots)]
    for move in lists + moves:
        move.start()
    for move in lists:
        move.wait()
    weight = trans[...] * mask[...].astype(f32)
    own, far = cell[...], remote[...]
    column = tiles * 128
    far_z = far & (column - 1)
    table = [
        (own & 127).astype(f32),
        (own >> 7).astype(f32),
        weight,
        (far >> (column.bit_length() - 1)).astype(f32),
        (far_z >> 7).astype(f32),
        (far_z & 127).astype(f32),
    ]
    for n, values in enumerate(table):
        for t in range(tiles):
            put_rows(a8, t, FACE_ROWS + n * SLOT_ROWS, values)
    moves[0].wait()

    def body(x, faces):
        return pack_faces(faces, [None] + y_tiles(kz[x]) + [None], x)

    put_faces(l_ref[0], a8, lax.fori_loop(0, cx, body, no_faces(), unroll=4))
    for move in moves[1:]:
        move.wait()


def relay_kernel(l_ref, a8, up, down):
    tiles = a8.shape[0]
    faces = get_faces(l_ref[0], a8)
    up[...] = faces
    down[0:BOTH_ROWS, :] = faces
    for t in range(tiles):
        at = BOTH_ROWS + LIST_ROWS * t
        down[at : at + LIST_ROWS, :] = a8[t, FACE_ROWS:, :]


def emit(l_ref, a8_ref, planes, faces, row_ref, pick_ref, far_x):
    tiles = a8_ref.shape[0]
    cx = planes.shape[1]
    slots = row_ref.shape[2]
    put_faces(l_ref[0], a8_ref, faces)
    for q in range(2):
        base = FACE_ROWS + q * 2 * SLOT_ROWS
        near = gather(
            planes[2 * q + 1], picks(slot_row(row_ref, q, NEAR_Z)), rows_hit(slot_row(row_ref, q, NEAR_X), cx)
        )
        near = slot_row(row_ref, q, WEIGHT) * near
        for t in range(tiles):
            at = slice(t * slots, (t + 1) * slots)
            far = gather(planes[2 * q], pick_ref[q, :, at], rows_hit(far_x[q : q + 1, at], cx))
            put_rows(a8_ref, t, base, near)
            put_rows(a8_ref, t, base + SLOT_ROWS, far)


def keep_planes(planes, slab, x):
    last = slab.shape[0] - H - 1
    for n, y in enumerate((H - 1, H, last, last + 1)):
        planes[n, pl.ds(x, 1), :] = slab[y : y + 1, :]


def with_fault(total, fault, x):
    tiles = y_tiles(total)
    y = lax.broadcasted_iota(jnp.int32, tiles[0].shape, 0)
    last = total.shape[0] - H - 1
    for n, at in enumerate((H - 1, H, last, last + 1)):
        tiles[at // 8] += jnp.where(y == at % 8, fault[n, pl.ds(x, 1), :], 0.0)
    return jnp.concatenate(tiles, axis=0)


def near_sum(row_ref, q, values, cx):
    return scatter(
        values, picks(slot_row(row_ref, q, NEAR_Z)), rows_hit(slot_row(row_ref, q, NEAR_X), cx)
    )


def weights(l, a8, above, row_ref, pick_ref, far_x, fault):
    tiles = a8.shape[0]
    cx = fault.shape[1]
    slots = row_ref.shape[2]
    first = above.shape[0] - tiles * LIST_ROWS

    def codes(block):
        parts = [block[n : n + 1] for n in range(LIST_ROWS)]
        return [
            jnp.concatenate(parts[SLOT_ROWS * n : SLOT_ROWS * (n + 1)], axis=1) for n in range(6)
        ]

    def block(q, t):
        if q == 0:
            return a8[t, FACE_ROWS : FACE_ROWS + LIST_ROWS, :]
        return above[pl.ds(pl.multiple_of(first + t * LIST_ROWS, 8), LIST_ROWS), :]

    for q in range(2):
        mine = codes(block(q, l))
        for n in range(3):
            row_ref[q, n : n + 1, :] = mine[n]
        far = jnp.zeros((cx, 128), f32)
        for t in range(tiles):
            at = slice(t * slots, (t + 1) * slots)
            table = codes(block(q, t))
            x = jnp.where(table[FAR_TILE] == l.astype(f32), table[FAR_X], -1.0)
            pick = picks(table[FAR_Z])
            pick_ref[q, :, at] = pick
            far_x[q : q + 1, at] = x
            far = far + scatter(table[WEIGHT], pick, rows_hit(x, cx))
        fault[2 * q] = far
        fault[2 * q + 1] = near_sum(row_ref, q, slot_row(row_ref, q, WEIGHT), cx)


def fault_kernel(a8, row_ref, pick_ref, far_x, fault):
    tiles, rows = a8.shape[0], a8.shape[1]
    cx = fault.shape[1]
    slots = row_ref.shape[2]
    for q in range(2):
        base = rows - (2 - q) * 2 * SLOT_ROWS
        far = jnp.zeros((cx, 128), f32)
        near = jnp.zeros((1, slots), f32)
        for t in range(tiles):
            at = slice(t * slots, (t + 1) * slots)
            values = get_rows(a8, t, base, SLOT_ROWS)
            far = far + scatter(values, pick_ref[q, :, at], rows_hit(far_x[q : q + 1, at], cx))
            near = near + get_rows(a8, t, base + SLOT_ROWS, SLOT_ROWS)
        fault[2 * q] = far
        fault[2 * q + 1] = near_sum(row_ref, q, slot_row(row_ref, q, WEIGHT) * near, cx)


def extended(before, after, n, own, x):
    return jnp.concatenate([before[n, x], own, after[n, x]], axis=0)


def side_faces(ky, kz, faces, x):
    ye = ky.shape[0]
    low, high = unpacked(faces, kz, x)
    return (
        harmonic(ky, pltpu.roll(ky, 1, 0)),
        harmonic(ky, pltpu.roll(ky, ye - 1, 0)),
        harmonic(kz, low),
        harmonic(kz, high),
    )


def inverse_of(diag):
    live = diag > 0.0
    return jnp.where(live, 1.0 / jnp.where(live, diag, 1.0), 0.0)


def edge_kernel(l_ref, rhs, acc, perm, before, after, below, above, a8,
                fault, row_ref, pick_ref, far_x, faces, low_edge, high_edge):
    cx = rhs.shape[0]
    l = l_ref[0]
    weights(l, a8, above, row_ref, pick_ref, far_x, fault)
    own = get_faces(l, a8)
    left = lane_iota((8, 128)) < 64
    faces[0:8, :] = jnp.where(left, pltpu.roll(below[8:16, :], 64, 1), own[0:8])
    faces[8:16, :] = own[8:16]
    faces[16:24, :] = jnp.where(left, own[16:24], pltpu.roll(above[8:16, :], 64, 1))

    def slab(n, source, x):
        return extended(before, after, n, source[x], x)

    for edge, x, inner in ((low_edge, 0, 1), (high_edge, cx - 1, cx - 2)):
        kx, kx_inner = slab(2, perm.at[0], x), slab(2, perm.at[0], inner)
        sides = side_faces(slab(3, perm.at[1], x), slab(4, perm.at[2], x), faces[...], x)
        edge[0] = kx
        edge[1] = with_fault(slab(1, acc, x) + harmonic(kx, kx_inner) + sum(sides), fault, x)
        edge[2] = slab(0, rhs, x)


def setup_kernel(rhs, acc, perm, before, after, faces_in, fault,
                 inv, z_out, d_out, tx, tym, typ, tzm, tzp, faces_out, planes):
    cx = rhs.shape[0]

    def ext(n, own, x):
        return extended(before, after, n, own, x)

    def body(x, carry):
        faces, t_low, kx = carry
        nxt = jnp.minimum(x + 1, cx - 1)
        kx_next = ext(2, perm[0, nxt], nxt)
        t_high = harmonic(kx, kx_next)
        ym, yp, zm, zp = side_faces(ext(3, perm[1, x], x), ext(4, perm[2, x], x), faces_in[...], x)
        diag = ext(1, acc[x], x) + t_low + t_high + ym + yp + zm + zp
        inverse = inverse_of(with_fault(diag, fault, x))
        z = inverse * ext(0, rhs[x], x)
        d = z / theta
        inv[x] = inverse
        z_out[x] = z
        d_out[x] = d
        tx[x] = t_low
        tx[x + 1] = t_high
        tym[x] = ym
        typ[x] = yp
        tzm[x] = zm
        tzp[x] = zp
        keep_planes(planes, d, x)
        return pack_faces(faces, y_tiles(d), x), t_high, kx_next

    kx0 = ext(2, perm[0, 0], 0)
    faces, _, _ = lax.fori_loop(0, cx, body, (no_faces(), jnp.zeros_like(kx0), kx0), unroll=4)
    faces_out[...] = jnp.concatenate(faces, axis=0)


def finish_kernel(l_ref, low_own, high_own, low_got, high_got, faces_in, planes_in,
                  row_ref, pick_ref, far_x, *refs):
    inv, z_out, d_out, tx, x_low, x_high, a8_out, planes, slabs, sem = refs[4:]
    cx = planes.shape[1]
    planes[...] = planes_in[...]
    faces = (faces_in[0:8, :], faces_in[8:16, :], faces_in[16:24, :])
    moves = []
    sides = ((low_own, low_got, x_low, 0, 0), (high_own, high_got, x_high, cx - 1, cx))
    for n, (own, got, out, x, at) in enumerate(sides):
        t = harmonic(own[0], got[0])
        inverse = inverse_of(own[1] + t)
        z = inverse * own[2]
        d = z / theta
        out[...] = inverse_of(got[1] + t) * got[2] / theta
        keep_planes(planes, d, x)
        faces = pack_faces(faces, y_tiles(d), x)
        for m, (value, ref, to) in enumerate(((inverse, inv, x), (z, z_out, x), (d, d_out, x), (t, tx, at))):
            slabs[4 * n + m] = value
            moves.append(pltpu.make_async_copy(slabs.at[4 * n + m], ref.at[to], sem.at[4 * n + m]))
            moves[-1].start()
    emit(l_ref, a8_out, planes, faces, row_ref, pick_ref, far_x)
    for move in moves:
        move.wait()


def sweep_kernel(c1, c2, first, last, l_ref, d_in, z_in, *refs):
    refs = list(refs)
    corr_in = None if first else refs.pop(0)
    xlow, xhigh, a8, fault, inv, tx, tym, typ, tzm, tzp = refs[:10]
    refs = refs[10:]
    if not last:
        row_ref, pick_ref, far_x = refs[:3]
        refs = refs[3:]
    outs = refs
    if last:
        (corr_out,) = outs
    else:
        d_out, z_out, corr_out, d_first, d_last, a8_out, planes = outs
    cx, ye = d_in.shape[0], d_in.shape[1]
    cy = ye - 2 * H
    faces_in = get_faces(l_ref[0], a8)

    def body(x, carry):
        faces, d_prev, d, t_low = carry
        t_high = tx[x + 1]
        d_next = jnp.where(x == cx - 1, xhigh[...], d_in[jnp.minimum(x + 1, cx - 1)])
        z_low, z_high = unpacked(faces_in, d, x)
        flow = t_low * d_prev + t_high * d_next
        flow = flow + (tym[x] * pltpu.roll(d, 1, 0) + typ[x] * pltpu.roll(d, ye - 1, 0))
        flow = flow + (tzm[x] * z_low + tzp[x] * z_high)
        flow = with_fault(flow, fault, x)
        z = z_in[x] - d + inv[x] * flow
        new = c1 * d + c2 * z
        before = d[H : H + cy] if first else corr_in[x]
        corr_out[x] = before + new[H : H + cy]
        if last:
            return faces, d, d_next, t_high
        d_out[x] = new
        z_out[x] = z
        keep_planes(planes, new, x)
        return pack_faces(faces, y_tiles(new), x), d, d_next, t_high

    init = (no_faces(), xlow[...], d_in[0], tx[0])
    faces, _, _, _ = lax.fori_loop(0, cx, body, init, unroll=4)
    if not last:
        d_first[...] = d_out[0]
        d_last[...] = d_out[cx - 1]
        emit(l_ref, a8_out, planes, faces, row_ref, pick_ref, far_x)


VMEM = pl.BlockSpec(memory_space=pltpu.VMEM)
SMEM = pl.BlockSpec(memory_space=pltpu.SMEM)
ANY = pl.BlockSpec(memory_space=pl.ANY)
HBM = pl.BlockSpec(memory_space=pltpu.HBM)
PARAMS = pltpu.CompilerParams(vmem_limit_bytes=24 << 20)


def steps(axis):
    peers = lax.axis_size(axis)
    up = [(i, i + 1) for i in range(peers - 1)]
    return up, [(j, i) for i, j in up]


def local(rhs, accumulation, permeability, nnc_cell, nnc_remote, nnc_mask, nnc_trans):
    cx, cy, cz = rhs.shape
    tiles = lax.axis_size("gz")
    slots = nnc_cell.shape[-1]
    ye = cy + 2 * H
    up_y, down_y = steps("gy")
    up_x, down_x = steps("gx")

    def struct(*shape, dtype=f32):
        return jax.ShapeDtypeStruct(shape, dtype)

    l = lax.axis_index("gz").reshape(1).astype(jnp.int32)
    flats = [a.reshape(1, slots) for a in (nnc_cell, nnc_remote, nnc_mask, nnc_trans)]
    l, *flats = lax.optimization_barrier((l, *flats))
    halo = struct(5, cx, H, cz)
    top, bottom, a8 = pl.pallas_call(
        pack_kernel,
        out_shape=(halo, halo, struct(tiles, FACE_ROWS + LIST_ROWS, cz)),
        in_specs=[SMEM] + [HBM] * 7,
        out_specs=(VMEM,) * 3,
        scratch_shapes=[pltpu.VMEM((cx, cy, cz), f32)]
        + [pltpu.VMEM((1, slots), jnp.int32)] * 3
        + [pltpu.VMEM((1, slots), f32), pltpu.SemaphoreType.DMA((15,))],
    )(l, rhs, accumulation, permeability, *flats)
    before = lax.ppermute(top, "gy", up_y)
    after = lax.ppermute(bottom, "gy", down_y)
    a8 = lax.all_to_all(a8, "gz", 0, 0, tiled=True)
    below, above = pl.pallas_call(
        relay_kernel,
        out_shape=(struct(BOTH_ROWS, cz), struct(BOTH_ROWS + tiles * LIST_ROWS, cz)),
        in_specs=[SMEM, VMEM],
        out_specs=(VMEM,) * 2,
        compiler_params=PARAMS,
    )(l, a8)
    below = lax.ppermute(below, "gy", up_y)
    above = lax.ppermute(above, "gy", down_y)

    big = struct(cx, ye, cz)
    tall = struct(cx + 1, ye, cz)
    edge = struct(ye, cz)
    small = struct(cx, cy, cz)
    sent = struct(tiles, FACE_ROWS + 4 * SLOT_ROWS, cz)
    scratch = [pltpu.VMEM((4, cx, cz), f32)]
    every = tiles * slots
    lists = (struct(2, 8, slots), struct(2, cz, every, dtype=bf16), struct(2, every))
    fault, row, pick, far_x, faces, low_edge, high_edge = pl.pallas_call(
        edge_kernel,
        out_shape=(struct(4, cx, cz),) + lists + (struct(BOTH_ROWS, cz),) + (struct(3, ye, cz),) * 2,
        in_specs=[SMEM] + [VMEM] * 8,
        out_specs=(VMEM,) * 7,
        compiler_params=PARAMS,
    )(l, rhs, accumulation, permeability, before, after, below, above, a8)
    low_got = lax.ppermute(high_edge, "gx", up_x)
    high_got = lax.ppermute(low_edge, "gx", down_x)
    inv, z, d, tx, tym, typ, tzm, tzp, faces, planes = pl.pallas_call(
        setup_kernel,
        out_shape=(big, big, big, tall, big, big, big, big)
        + (struct(BOTH_ROWS, cz), struct(4, cx, cz)),
        in_specs=[VMEM] * 7,
        out_specs=(VMEM,) * 10,
        compiler_params=PARAMS,
    )(rhs, accumulation, permeability, before, after, faces, fault)
    inv, z, d, tx, xlow, xhigh, a8 = pl.pallas_call(
        finish_kernel,
        out_shape=(big, big, big, tall, edge, edge, sent),
        in_specs=[SMEM] + [VMEM] * 9 + [ANY] * 4,
        out_specs=(ANY,) * 4 + (VMEM,) * 3,
        scratch_shapes=scratch + [pltpu.VMEM((8, ye, cz), f32), pltpu.SemaphoreType.DMA((8,))],
        input_output_aliases={10: 0, 11: 1, 12: 2, 13: 3},
        compiler_params=PARAMS,
    )(l, low_edge, high_edge, low_got, high_got, faces, planes, row, pick, far_x, inv, z, d, tx)

    rho = 1.0 / sigma
    corr = None
    for sweep in range(1, SWEEPS):
        first, last = sweep == 1, sweep == SWEEPS - 1
        rho_next = 1.0 / (2.0 * sigma - rho)
        c1, c2 = rho_next * rho, 2.0 * rho_next / delta
        rho = rho_next
        if not first:
            xlow = lax.ppermute(d_last, "gx", up_x)
            xhigh = lax.ppermute(d_first, "gx", down_x)
        a8 = lax.all_to_all(a8, "gz", 0, 0, tiled=True)
        fault = pl.pallas_call(
            fault_kernel,
            out_shape=struct(4, cx, cz),
            in_specs=[VMEM] * 4,
            out_specs=VMEM,
            compiler_params=PARAMS,
        )(a8, row, pick, far_x)
        args = [l, d, z] + ([] if first else [corr])
        args += [xlow, xhigh, a8, fault, inv, tx, tym, typ, tzm, tzp]
        args += [] if last else [row, pick, far_x]

        def kernel(*refs, c1=c1, c2=c2, first=first, last=last):
            sweep_kernel(c1, c2, first, last, *refs)

        out = pl.pallas_call(
            kernel,
            out_shape=small if last else (big, big, small, edge, edge, sent),
            in_specs=[SMEM] + [VMEM] * (len(args) - 1),
            out_specs=VMEM if last else (VMEM,) * 6,
            scratch_shapes=[] if last else scratch,
            compiler_params=PARAMS,
        )(*args)
        if last:
            corr = out
        else:
            d, z, corr, d_first, d_last, a8 = out
    return corr


def solution(mesh):
    split = P("gx", "gy", "gz")
    slots = P("gx", "gy", "gz", None)
    return jax.shard_map(
        local,
        mesh=mesh,
        in_specs=(split, split, P(None, "gx", "gy", "gz"), slots, slots, slots, slots),
        out_specs=split,
        check_vma=False,
    )
```

```python
import jax
import jax.numpy as jnp
from jax import lax
from jax.experimental import pallas as pl
from jax.experimental.pallas import tpu as pltpu
from jax.sharding import PartitionSpec as P

SWEEPS = 6
lam_low = 0.1
lam_high = 2.0
theta = (lam_high + lam_low) / 2.0
delta = (lam_high - lam_low) / 2.0
sigma = theta / delta

SLOT_ROWS = 4
LIST_ROWS = 24
H = 8
f32 = jnp.float32
bf16 = jnp.bfloat16


def harmonic(left, right):
    total = left + right
    live = total > 0.0
    return jnp.where(live, 2.0 * (left * right) / jnp.where(live, total, 1.0), 0.0)


def split3(v):
    hi = v.astype(bf16).astype(f32)
    rest = v - hi
    mid = rest.astype(bf16).astype(f32)
    return hi, mid, rest - mid


def dot(a, b, dims):
    return lax.dot_general(a, b, (dims, ((), ())), preferred_element_type=f32)


def lane_iota(shape):
    return lax.broadcasted_iota(jnp.int32, shape, len(shape) - 1)


def rows_hit(codes, count):
    shape = (count, codes.shape[1])
    return lax.broadcasted_iota(jnp.int32, shape, 0).astype(f32) == codes


def picks(codes):
    return jnp.where(rows_hit(codes, 128), 1.0, 0.0).astype(bf16)


def thirds(out):
    n = out.shape[0] // 3
    return out[:n] + out[n : 2 * n] + out[2 * n :]


def gather(table, pick, x_hit):
    parts = jnp.concatenate(split3(table), axis=0).astype(bf16)
    got = thirds(dot(parts, pick, ((1,), (0,))))
    return jnp.sum(jnp.where(x_hit, got, 0.0), axis=0, keepdims=True)


def scatter(u, pick, x_hit):
    parts = [jnp.where(x_hit, p, 0.0) for p in split3(u)]
    return thirds(dot(jnp.concatenate(parts, axis=0).astype(bf16), pick, ((1,), (1,))))


def get_rows(ref, t, base, count):
    return jnp.concatenate([ref[t, base + k : base + k + 1, :] for k in range(count)], axis=1)


def put_rows(ref, t, base, values):
    for k in range(values.shape[1] // 128):
        ref[t, base + k : base + k + 1, :] = values[:, 128 * k : 128 * (k + 1)]


NEAR_Z, NEAR_X, WEIGHT, FAR_X, FAR_TILE, FAR_Z = range(6)


def slot_row(row_ref, q, which):
    return row_ref[q, which : which + 1, :]


FACE_ROWS = 16
BOTH_ROWS = 24


def pack_faces(faces, tiles, x):
    faces = list(faces)
    lane = lane_iota((8, 128))
    for half in range(2):
        at = 64 * half + 2 * x + 2
        here = ((lane - (at - 1)) & 127) < 2
        for n in range(3):
            tile = tiles[3 * half + n]
            if tile is not None:
                faces[n] = jnp.where(here, pltpu.roll(tile, at % 128, 1), faces[n])
    return tuple(faces)


def no_faces():
    return (jnp.zeros((8, 128), f32),) * 3


def y_tiles(slab):
    return [slab[8 * n : 8 * (n + 1)] for n in range(slab.shape[0] // 8)]


def put_faces(l, ref, faces):
    odd = (lane_iota((8, 128)) & 1) == 1
    first, second, third = faces
    above = jnp.where(odd, first, pltpu.roll(second, 127, 1))
    below = jnp.where(odd, pltpu.roll(second, 1, 1), first)
    for t in range(ref.shape[0]):
        ref[t, 0:8, :] = jnp.where(t > l, above, below)
        ref[t, 8:16, :] = third


def get_faces(l, ref):
    tiles = ref.shape[0]
    low = jnp.where(l > 0, ref[jnp.maximum(l - 1, 0), 0:16, :], 0.0)
    high = jnp.where(l < tiles - 1, ref[jnp.minimum(l + 1, tiles - 1), 0:16, :], 0.0)
    odd = (lane_iota((8, 128)) & 1) == 1
    high = pltpu.roll(high, 126, 1)
    first = jnp.where(odd, low[0:8], high[0:8])
    second = jnp.where(odd, pltpu.roll(low[0:8], 1, 1), pltpu.roll(high[0:8], 127, 1))
    third = jnp.where(odd, low[8:16], high[8:16])
    return jnp.concatenate([first, second, third], axis=0)


def unpacked(faces, slab, x, skip=0):
    lane = lane_iota((8, 128))
    lows, highs = [], []
    tiles = y_tiles(slab)
    for n in range(skip, len(tiles) - skip):
        tile = tiles[n]
        packed = faces[8 * (n % 3) : 8 * (n % 3) + 8]
        outer = pltpu.roll(packed, (127 - 64 * (n // 3) - 2 * x) % 128, 1)
        lows.append(jnp.where(lane == 0, outer, pltpu.roll(tile, 1, 1)))
        highs.append(jnp.where(lane == 127, outer, pltpu.roll(tile, 127, 1)))
    return jnp.concatenate(lows, axis=0), jnp.concatenate(highs, axis=0)


def pack_kernel(l_ref, rhs, acc, perm, cell_in, remote_in, mask_in, trans_in,
                top, bottom, a8, kz, cell, remote, mask, trans, sem):
    tiles = a8.shape[0]
    cx, cy = rhs.shape[0], rhs.shape[1]
    sources = [rhs, acc] + [perm.at[n] for n in range(3)]
    moves = [pltpu.make_async_copy(perm.at[2], kz, sem.at[0])]
    for n, source in enumerate(sources):
        moves.append(pltpu.make_async_copy(source.at[:, cy - H :, :], top.at[n], sem.at[1 + 2 * n]))
        moves.append(pltpu.make_async_copy(source.at[:, :H, :], bottom.at[n], sem.at[2 + 2 * n]))
    count = 2 * len(sources) + 1
    slots = ((cell_in, cell), (remote_in, remote), (mask_in, mask), (trans_in, trans))
    lists = [pltpu.make_async_copy(a, b, sem.at[count + n]) for n, (a, b) in enumerate(slots)]
    for move in lists + moves:
        move.start()
    for move in lists:
        move.wait()
    weight = trans[...] * mask[...].astype(f32)
    own, far = cell[...], remote[...]
    column = tiles * 128
    far_z = far & (column - 1)
    table = [
        (own & 127).astype(f32),
        (own >> 7).astype(f32),
        weight,
        (far >> (column.bit_length() - 1)).astype(f32),
        (far_z >> 7).astype(f32),
        (far_z & 127).astype(f32),
    ]
    for n, values in enumerate(table):
        for t in range(tiles):
            put_rows(a8, t, FACE_ROWS + n * SLOT_ROWS, values)
    moves[0].wait()

    def body(x, faces):
        return pack_faces(faces, [None] + y_tiles(kz[x]) + [None], x)

    put_faces(l_ref[0], a8, lax.fori_loop(0, cx, body, no_faces(), unroll=4))
    for move in moves[1:]:
        move.wait()


def relay_kernel(l_ref, a8, up, down):
    tiles = a8.shape[0]
    faces = get_faces(l_ref[0], a8)
    up[...] = faces
    down[0:BOTH_ROWS, :] = faces
    for t in range(tiles):
        at = BOTH_ROWS + LIST_ROWS * t
        down[at : at + LIST_ROWS, :] = a8[t, FACE_ROWS:, :]


def emit(l_ref, a8_ref, planes, faces, row_ref, pick_ref, far_x, final=False):
    tiles = a8_ref.shape[0]
    cx = planes.shape[1]
    slots = row_ref.shape[2]
    put_faces(l_ref[0], a8_ref, faces)
    base = FACE_ROWS
    for q in range(2):
        if not final or q == 1:
            near = gather(
                planes[2 * q + 1], picks(slot_row(row_ref, q, NEAR_Z)), rows_hit(slot_row(row_ref, q, NEAR_X), cx)
            )
            near = slot_row(row_ref, q, WEIGHT) * near
            for t in range(tiles):
                put_rows(a8_ref, t, base, near)
            base = base + SLOT_ROWS
        if not final or q == 0:
            for t in range(tiles):
                at = slice(t * slots, (t + 1) * slots)
                far = gather(planes[2 * q], pick_ref[q, :, at], rows_hit(far_x[q : q + 1, at], cx))
                put_rows(a8_ref, t, base, far)
            base = base + SLOT_ROWS


def keep_planes(planes, slab, x):
    last = slab.shape[0] - H - 1
    for n, y in enumerate((H - 1, H, last, last + 1)):
        planes[n, pl.ds(x, 1), :] = slab[y : y + 1, :]


def with_fault(total, fault, x, first=0):
    tiles = y_tiles(total)
    y = lax.broadcasted_iota(jnp.int32, tiles[0].shape, 0)
    last = total.shape[0] + 2 * first - H - 1
    for n, at in enumerate((H - 1, H, last, last + 1)):
        at = at - first
        if 0 <= at < total.shape[0]:
            tiles[at // 8] += jnp.where(y == at % 8, fault[n, pl.ds(x, 1), :], 0.0)
    return jnp.concatenate(tiles, axis=0)


def near_sum(row_ref, q, values, cx):
    return scatter(
        values, picks(slot_row(row_ref, q, NEAR_Z)), rows_hit(slot_row(row_ref, q, NEAR_X), cx)
    )


def weights(l, a8, above, row_ref, pick_ref, far_x, fault):
    tiles = a8.shape[0]
    cx = fault.shape[1]
    slots = row_ref.shape[2]
    first = above.shape[0] - tiles * LIST_ROWS

    def codes(block):
        parts = [block[n : n + 1] for n in range(LIST_ROWS)]
        return [
            jnp.concatenate(parts[SLOT_ROWS * n : SLOT_ROWS * (n + 1)], axis=1) for n in range(6)
        ]

    def block(q, t):
        if q == 0:
            return a8[t, FACE_ROWS : FACE_ROWS + LIST_ROWS, :]
        return above[pl.ds(pl.multiple_of(first + t * LIST_ROWS, 8), LIST_ROWS), :]

    for q in range(2):
        mine = codes(block(q, l))
        for n in range(3):
            row_ref[q, n : n + 1, :] = mine[n]
        far = jnp.zeros((cx, 128), f32)
        for t in range(tiles):
            at = slice(t * slots, (t + 1) * slots)
            table = codes(block(q, t))
            x = jnp.where(table[FAR_TILE] == l.astype(f32), table[FAR_X], -1.0)
            pick = picks(table[FAR_Z])
            pick_ref[q, :, at] = pick
            far_x[q : q + 1, at] = x
            far = far + scatter(table[WEIGHT], pick, rows_hit(x, cx))
        fault[2 * q] = far
        fault[2 * q + 1] = near_sum(row_ref, q, slot_row(row_ref, q, WEIGHT), cx)


def fault_kernel(final, a8, row_ref, pick_ref, far_x, fault):
    tiles = a8.shape[0]
    cx = fault.shape[1]
    slots = row_ref.shape[2]
    base = FACE_ROWS
    for q in range(2):
        if not final or q == 1:
            far = jnp.zeros((cx, 128), f32)
            for t in range(tiles):
                at = slice(t * slots, (t + 1) * slots)
                values = get_rows(a8, t, base, SLOT_ROWS)
                far = far + scatter(values, pick_ref[q, :, at], rows_hit(far_x[q : q + 1, at], cx))
            fault[2 * q] = far
            base = base + SLOT_ROWS
        if not final or q == 0:
            near = jnp.zeros((1, slots), f32)
            for t in range(tiles):
                near = near + get_rows(a8, t, base, SLOT_ROWS)
            fault[2 * q + 1] = near_sum(row_ref, q, slot_row(row_ref, q, WEIGHT) * near, cx)
            base = base + SLOT_ROWS


def extended(before, after, n, own, x):
    return jnp.concatenate([before[n, x], own, after[n, x]], axis=0)


def side_faces(ky, kz, faces, x):
    ye = ky.shape[0]
    low, high = unpacked(faces, kz, x)
    return (
        harmonic(ky, pltpu.roll(ky, 1, 0)),
        harmonic(ky, pltpu.roll(ky, ye - 1, 0)),
        harmonic(kz, low),
        harmonic(kz, high),
    )


def inverse_of(diag):
    live = diag > 0.0
    return jnp.where(live, 1.0 / jnp.where(live, diag, 1.0), 0.0)


def edge_kernel(l_ref, rhs, acc, perm, before, after, below, above, a8,
                fault, row_ref, pick_ref, far_x, faces, low_edge, high_edge):
    cx = rhs.shape[0]
    l = l_ref[0]
    weights(l, a8, above, row_ref, pick_ref, far_x, fault)
    own = get_faces(l, a8)
    left = lane_iota((8, 128)) < 64
    faces[0:8, :] = jnp.where(left, pltpu.roll(below[8:16, :], 64, 1), own[0:8])
    faces[8:16, :] = own[8:16]
    faces[16:24, :] = jnp.where(left, own[16:24], pltpu.roll(above[8:16, :], 64, 1))

    def slab(n, source, x):
        return extended(before, after, n, source[x], x)

    for edge, x, inner in ((low_edge, 0, 1), (high_edge, cx - 1, cx - 2)):
        kx, kx_inner = slab(2, perm.at[0], x), slab(2, perm.at[0], inner)
        sides = side_faces(slab(3, perm.at[1], x), slab(4, perm.at[2], x), faces[...], x)
        edge[0] = kx
        edge[1] = with_fault(slab(1, acc, x) + harmonic(kx, kx_inner) + sum(sides), fault, x)
        edge[2] = slab(0, rhs, x)


def setup_kernel(rhs, acc, perm, before, after, faces_in, fault,
                 inv, z_out, d_out, tx, tym, typ, tzm, tzp, faces_out, planes):
    cx = rhs.shape[0]

    def ext(n, own, x):
        return extended(before, after, n, own, x)

    def body(x, carry):
        faces, t_low, kx = carry
        nxt = jnp.minimum(x + 1, cx - 1)
        kx_next = ext(2, perm[0, nxt], nxt)
        t_high = harmonic(kx, kx_next)
        ym, yp, zm, zp = side_faces(ext(3, perm[1, x], x), ext(4, perm[2, x], x), faces_in[...], x)
        diag = ext(1, acc[x], x) + t_low + t_high + ym + yp + zm + zp
        inverse = inverse_of(with_fault(diag, fault, x))
        z = inverse * ext(0, rhs[x], x)
        d = z / theta
        inv[x] = inverse
        z_out[x] = z
        d_out[x] = d
        tx[x] = t_low
        tx[x + 1] = t_high
        tym[x] = ym
        typ[x] = yp
        tzm[x] = zm
        tzp[x] = zp
        keep_planes(planes, d, x)
        return pack_faces(faces, y_tiles(d), x), t_high, kx_next

    kx0 = ext(2, perm[0, 0], 0)
    faces, _, _ = lax.fori_loop(0, cx, body, (no_faces(), jnp.zeros_like(kx0), kx0), unroll=4)
    faces_out[...] = jnp.concatenate(faces, axis=0)


def finish_kernel(l_ref, low_own, high_own, low_got, high_got, faces_in, planes_in,
                  row_ref, pick_ref, far_x, *refs):
    inv, z_out, d_out, tx, x_low, x_high, a8_out, planes, slabs, sem = refs[4:]
    cx = planes.shape[1]
    planes[...] = planes_in[...]
    faces = (faces_in[0:8, :], faces_in[8:16, :], faces_in[16:24, :])
    moves = []
    sides = ((low_own, low_got, x_low, 0, 0), (high_own, high_got, x_high, cx - 1, cx))
    for n, (own, got, out, x, at) in enumerate(sides):
        t = harmonic(own[0], got[0])
        inverse = inverse_of(own[1] + t)
        z = inverse * own[2]
        d = z / theta
        out[...] = inverse_of(got[1] + t) * got[2] / theta
        keep_planes(planes, d, x)
        faces = pack_faces(faces, y_tiles(d), x)
        for m, (value, ref, to) in enumerate(((inverse, inv, x), (z, z_out, x), (d, d_out, x), (t, tx, at))):
            slabs[4 * n + m] = value
            moves.append(pltpu.make_async_copy(slabs.at[4 * n + m], ref.at[to], sem.at[4 * n + m]))
            moves[-1].start()
    emit(l_ref, a8_out, planes, faces, row_ref, pick_ref, far_x)
    for move in moves:
        move.wait()


def sweep_kernel(c1, c2, first, last, final, l_ref, d_in, z_in, *refs):
    refs = list(refs)
    corr_in = None if first else refs.pop(0)
    xlow, xhigh, a8, fault, inv, tx, tym, typ, tzm, tzp = refs[:10]
    refs = refs[10:]
    if not last:
        row_ref, pick_ref, far_x = refs[:3]
        refs = refs[3:]
    outs = refs
    if last:
        (corr_out,) = outs
    else:
        d_out, z_out, corr_out, d_first, d_last, a8_out, planes = outs
    cx, ye = d_in.shape[0], d_in.shape[1]
    cy = ye - 2 * H
    faces_in = get_faces(l_ref[0], a8)

    def body(x, carry):
        faces, d_prev, d, t_low = carry
        t_high = tx[x + 1]
        d_next = jnp.where(x == cx - 1, xhigh[...], d_in[jnp.minimum(x + 1, cx - 1)])
        skip = 1 if last else 0
        rows = slice(8 * skip, ye - 8 * skip)
        z_low, z_high = unpacked(faces_in, d, x, skip)
        below, above = pltpu.roll(d, 1, 0)[rows], pltpu.roll(d, ye - 1, 0)[rows]
        flow = t_low[rows] * d_prev[rows] + t_high[rows] * d_next[rows]
        flow = flow + (tym[x, rows, :] * below + typ[x, rows, :] * above)
        flow = flow + (tzm[x, rows, :] * z_low + tzp[x, rows, :] * z_high)
        flow = with_fault(flow, fault, x, 8 * skip)
        z = z_in[x, rows, :] - d[rows] + inv[x, rows, :] * flow
        new = c1 * d[rows] + c2 * z
        own = slice(H - 8 * skip, H - 8 * skip + cy)
        corr_out[x] = (d[H : H + cy] if first else corr_in[x]) + new[own]
        if last:
            return faces, d, d_next, t_high
        d_out[x] = new
        z_out[x] = z
        keep_planes(planes, new, x)
        return pack_faces(faces, y_tiles(new), x), d, d_next, t_high

    init = (no_faces(), xlow[...], d_in[0], tx[0])
    faces, _, _, _ = lax.fori_loop(0, cx, body, init, unroll=4)
    if not last:
        d_first[...] = d_out[0]
        d_last[...] = d_out[cx - 1]
        emit(l_ref, a8_out, planes, faces, row_ref, pick_ref, far_x, final)


VMEM = pl.BlockSpec(memory_space=pltpu.VMEM)
SMEM = pl.BlockSpec(memory_space=pltpu.SMEM)
ANY = pl.BlockSpec(memory_space=pl.ANY)
HBM = pl.BlockSpec(memory_space=pltpu.HBM)
PARAMS = pltpu.CompilerParams(vmem_limit_bytes=24 << 20)


def steps(axis):
    peers = lax.axis_size(axis)
    up = [(i, i + 1) for i in range(peers - 1)]
    return up, [(j, i) for i, j in up]


def local(rhs, accumulation, permeability, nnc_cell, nnc_remote, nnc_mask, nnc_trans):
    cx, cy, cz = rhs.shape
    tiles = lax.axis_size("gz")
    slots = nnc_cell.shape[-1]
    ye = cy + 2 * H
    up_y, down_y = steps("gy")
    up_x, down_x = steps("gx")

    def struct(*shape, dtype=f32):
        return jax.ShapeDtypeStruct(shape, dtype)

    l = lax.axis_index("gz").reshape(1).astype(jnp.int32)
    flats = [a.reshape(1, slots) for a in (nnc_cell, nnc_remote, nnc_mask, nnc_trans)]
    l, *flats = lax.optimization_barrier((l, *flats))
    halo = struct(5, cx, H, cz)
    top, bottom, a8 = pl.pallas_call(
        pack_kernel,
        out_shape=(halo, halo, struct(tiles, FACE_ROWS + LIST_ROWS, cz)),
        in_specs=[SMEM] + [HBM] * 7,
        out_specs=(VMEM,) * 3,
        scratch_shapes=[pltpu.VMEM((cx, cy, cz), f32)]
        + [pltpu.VMEM((1, slots), jnp.int32)] * 3
        + [pltpu.VMEM((1, slots), f32), pltpu.SemaphoreType.DMA((15,))],
    )(l, rhs, accumulation, permeability, *flats)
    before = lax.ppermute(top, "gy", up_y)
    after = lax.ppermute(bottom, "gy", down_y)
    a8 = lax.all_to_all(a8, "gz", 0, 0, tiled=True)
    below, above = pl.pallas_call(
        relay_kernel,
        out_shape=(struct(BOTH_ROWS, cz), struct(BOTH_ROWS + tiles * LIST_ROWS, cz)),
        in_specs=[SMEM, VMEM],
        out_specs=(VMEM,) * 2,
        compiler_params=PARAMS,
    )(l, a8)
    below = lax.ppermute(below, "gy", up_y)
    above = lax.ppermute(above, "gy", down_y)

    big = struct(cx, ye, cz)
    tall = struct(cx + 1, ye, cz)
    edge = struct(ye, cz)
    small = struct(cx, cy, cz)
    sent = struct(tiles, FACE_ROWS + 4 * SLOT_ROWS, cz)
    scratch = [pltpu.VMEM((4, cx, cz), f32)]
    every = tiles * slots
    lists = (struct(2, 8, slots), struct(2, cz, every, dtype=bf16), struct(2, every))
    fault, row, pick, far_x, faces, low_edge, high_edge = pl.pallas_call(
        edge_kernel,
        out_shape=(struct(4, cx, cz),) + lists + (struct(BOTH_ROWS, cz),) + (struct(3, ye, cz),) * 2,
        in_specs=[SMEM] + [VMEM] * 8,
        out_specs=(VMEM,) * 7,
        compiler_params=PARAMS,
    )(l, rhs, accumulation, permeability, before, after, below, above, a8)
    low_got = lax.ppermute(high_edge, "gx", up_x)
    high_got = lax.ppermute(low_edge, "gx", down_x)
    inv, z, d, tx, tym, typ, tzm, tzp, faces, planes = pl.pallas_call(
        setup_kernel,
        out_shape=(big, big, big, tall, big, big, big, big)
        + (struct(BOTH_ROWS, cz), struct(4, cx, cz)),
        in_specs=[VMEM] * 7,
        out_specs=(VMEM,) * 10,
        compiler_params=PARAMS,
    )(rhs, accumulation, permeability, before, after, faces, fault)
    inv, z, d, tx, xlow, xhigh, a8 = pl.pallas_call(
        finish_kernel,
        out_shape=(big, big, big, tall, edge, edge, sent),
        in_specs=[SMEM] + [VMEM] * 9 + [ANY] * 4,
        out_specs=(ANY,) * 4 + (VMEM,) * 3,
        scratch_shapes=scratch + [pltpu.VMEM((8, ye, cz), f32), pltpu.SemaphoreType.DMA((8,))],
        input_output_aliases={10: 0, 11: 1, 12: 2, 13: 3},
        compiler_params=PARAMS,
    )(l, low_edge, high_edge, low_got, high_got, faces, planes, row, pick, far_x, inv, z, d, tx)

    rho = 1.0 / sigma
    corr = None
    for sweep in range(1, SWEEPS):
        first, last = sweep == 1, sweep == SWEEPS - 1
        rho_next = 1.0 / (2.0 * sigma - rho)
        c1, c2 = rho_next * rho, 2.0 * rho_next / delta
        rho = rho_next
        if not first:
            xlow = lax.ppermute(d_last, "gx", up_x)
            xhigh = lax.ppermute(d_first, "gx", down_x)
        a8 = lax.all_to_all(a8, "gz", 0, 0, tiled=True)

        def sums(*refs, final=last):
            fault_kernel(final, *refs)

        fault = pl.pallas_call(
            sums,
            out_shape=struct(4, cx, cz),
            in_specs=[VMEM] * 4,
            out_specs=VMEM,
            compiler_params=PARAMS,
        )(a8, row, pick, far_x)
        args = [l, d, z] + ([] if first else [corr])
        args += [xlow, xhigh, a8, fault, inv, tx, tym, typ, tzm, tzp]
        args += [] if last else [row, pick, far_x]

        final = sweep == SWEEPS - 2
        rows = FACE_ROWS + (2 if final else 4) * SLOT_ROWS
        sent = struct(tiles, rows, cz)

        def kernel(*refs, c1=c1, c2=c2, first=first, last=last, final=final):
            sweep_kernel(c1, c2, first, last, final, *refs)

        out = pl.pallas_call(
            kernel,
            out_shape=small if last else (big, big, small, edge, edge, sent),
            in_specs=[SMEM] + [VMEM] * (len(args) - 1),
            out_specs=VMEM if last else (VMEM,) * 6,
            scratch_shapes=[] if last else scratch,
            compiler_params=PARAMS,
        )(*args)
        if last:
            corr = out
        else:
            d, z, corr, d_first, d_last, a8 = out
    return corr


def solution(mesh):
    split = P("gx", "gy", "gz")
    slots = P("gx", "gy", "gz", None)
    return jax.shard_map(
        local,
        mesh=mesh,
        in_specs=(split, split, P(None, "gx", "gy", "gz"), slots, slots, slots, slots),
        out_specs=split,
        check_vma=False,
    )
```

```python
import jax
import jax.numpy as jnp
from jax import lax
from jax.experimental import pallas as pl
from jax.experimental.pallas import tpu as pltpu
from jax.sharding import PartitionSpec as P

SWEEPS = 6
lam_low = 0.1
lam_high = 2.0
theta = (lam_high + lam_low) / 2.0
delta = (lam_high - lam_low) / 2.0
sigma = theta / delta

SLOT_ROWS = 4
LIST_ROWS = 24
H = 8
f32 = jnp.float32
bf16 = jnp.bfloat16


def harmonic(left, right):
    total = left + right
    live = total > 0.0
    return jnp.where(live, 2.0 * (left * right) / jnp.where(live, total, 1.0), 0.0)


def split3(v):
    hi = v.astype(bf16).astype(f32)
    rest = v - hi
    mid = rest.astype(bf16).astype(f32)
    return hi, mid, rest - mid


def dot(a, b, dims):
    return lax.dot_general(a, b, (dims, ((), ())), preferred_element_type=f32)


def lane_iota(shape):
    return lax.broadcasted_iota(jnp.int32, shape, len(shape) - 1)


def rows_hit(codes, count):
    shape = (count, codes.shape[1])
    return lax.broadcasted_iota(jnp.int32, shape, 0).astype(f32) == codes


def picks(codes):
    return jnp.where(rows_hit(codes, 128), 1.0, 0.0).astype(bf16)


def thirds(out):
    n = out.shape[0] // 3
    return out[:n] + out[n : 2 * n] + out[2 * n :]


def gather(table, pick, x_hit):
    parts = jnp.concatenate(split3(table), axis=0).astype(bf16)
    got = thirds(dot(parts, pick, ((1,), (0,))))
    return jnp.sum(jnp.where(x_hit, got, 0.0), axis=0, keepdims=True)


def scatter(u, pick, x_hit):
    parts = [jnp.where(x_hit, p, 0.0) for p in split3(u)]
    return thirds(dot(jnp.concatenate(parts, axis=0).astype(bf16), pick, ((1,), (1,))))


def get_rows(ref, t, base, count):
    return jnp.concatenate([ref[t, base + k : base + k + 1, :] for k in range(count)], axis=1)


def put_rows(ref, t, base, values):
    for k in range(values.shape[1] // 128):
        ref[t, base + k : base + k + 1, :] = values[:, 128 * k : 128 * (k + 1)]


NEAR_Z, NEAR_X, WEIGHT, FAR_X, FAR_TILE, FAR_Z = range(6)


def slot_row(row_ref, q, which):
    return row_ref[q, which : which + 1, :]


FACE_ROWS = 16
BOTH_ROWS = 24


def pack_faces(faces, tiles, x):
    faces = list(faces)
    lane = lane_iota((8, 128))
    for half in range(2):
        at = 64 * half + 2 * x + 2
        here = ((lane - (at - 1)) & 127) < 2
        for n in range(3):
            tile = tiles[3 * half + n]
            if tile is not None:
                faces[n] = jnp.where(here, pltpu.roll(tile, at % 128, 1), faces[n])
    return tuple(faces)


def no_faces():
    return (jnp.zeros((8, 128), f32),) * 3


def y_tiles(slab):
    return [slab[8 * n : 8 * (n + 1)] for n in range(slab.shape[0] // 8)]


def put_faces(l, ref, faces):
    odd = (lane_iota((8, 128)) & 1) == 1
    first, second, third = faces
    above = jnp.where(odd, first, pltpu.roll(second, 127, 1))
    below = jnp.where(odd, pltpu.roll(second, 1, 1), first)
    for t in range(ref.shape[0]):
        ref[t, 0:8, :] = jnp.where(t > l, above, below)
        ref[t, 8:16, :] = third


def get_faces(l, ref):
    tiles = ref.shape[0]
    low = jnp.where(l > 0, ref[jnp.maximum(l - 1, 0), 0:16, :], 0.0)
    high = jnp.where(l < tiles - 1, ref[jnp.minimum(l + 1, tiles - 1), 0:16, :], 0.0)
    odd = (lane_iota((8, 128)) & 1) == 1
    high = pltpu.roll(high, 126, 1)
    first = jnp.where(odd, low[0:8], high[0:8])
    second = jnp.where(odd, pltpu.roll(low[0:8], 1, 1), pltpu.roll(high[0:8], 127, 1))
    third = jnp.where(odd, low[8:16], high[8:16])
    return jnp.concatenate([first, second, third], axis=0)


def unpacked(faces, slab, x, skip=0):
    lane = lane_iota((8, 128))
    lows, highs = [], []
    tiles = y_tiles(slab)
    for n in range(skip, len(tiles) - skip):
        tile = tiles[n]
        packed = faces[8 * (n % 3) : 8 * (n % 3) + 8]
        outer = pltpu.roll(packed, (127 - 64 * (n // 3) - 2 * x) % 128, 1)
        lows.append(jnp.where(lane == 0, outer, pltpu.roll(tile, 1, 1)))
        highs.append(jnp.where(lane == 127, outer, pltpu.roll(tile, 127, 1)))
    return jnp.concatenate(lows, axis=0), jnp.concatenate(highs, axis=0)


def pack_kernel(l_ref, rhs, acc, perm, cell_in, remote_in, mask_in, trans_in,
                top, bottom, a8, kz, cell, remote, mask, trans, sem):
    tiles = a8.shape[0]
    cx, cy = rhs.shape[0], rhs.shape[1]
    sources = [rhs, acc] + [perm.at[n] for n in range(3)]
    moves = [pltpu.make_async_copy(perm.at[2], kz, sem.at[0])]
    for n, source in enumerate(sources):
        moves.append(pltpu.make_async_copy(source.at[:, cy - H :, :], top.at[n], sem.at[1 + 2 * n]))
        moves.append(pltpu.make_async_copy(source.at[:, :H, :], bottom.at[n], sem.at[2 + 2 * n]))
    count = 2 * len(sources) + 1
    slots = ((cell_in, cell), (remote_in, remote), (mask_in, mask), (trans_in, trans))
    lists = [pltpu.make_async_copy(a, b, sem.at[count + n]) for n, (a, b) in enumerate(slots)]
    for move in lists + moves:
        move.start()
    for move in lists:
        move.wait()
    weight = trans[...] * mask[...].astype(f32)
    own, far = cell[...], remote[...]
    column = tiles * 128
    far_z = far & (column - 1)
    table = [
        (own & 127).astype(f32),
        (own >> 7).astype(f32),
        weight,
        (far >> (column.bit_length() - 1)).astype(f32),
        (far_z >> 7).astype(f32),
        (far_z & 127).astype(f32),
    ]
    for n, values in enumerate(table):
        for t in range(tiles):
            put_rows(a8, t, FACE_ROWS + n * SLOT_ROWS, values)
    moves[0].wait()

    def body(x, faces):
        return pack_faces(faces, [None] + y_tiles(kz[x]) + [None], x)

    put_faces(l_ref[0], a8, lax.fori_loop(0, cx, body, no_faces(), unroll=4))
    for move in moves[1:]:
        move.wait()


def relay_kernel(l_ref, a8, up, down):
    tiles = a8.shape[0]
    faces = get_faces(l_ref[0], a8)
    up[...] = faces
    down[0:BOTH_ROWS, :] = faces
    here = l_ref[0].astype(f32)

    def part(t, which):
        at = FACE_ROWS + which * SLOT_ROWS
        return a8[t, at : at + SLOT_ROWS, :]

    at = BOTH_ROWS
    for t in range(tiles):
        x = jnp.where(part(t, FAR_TILE) == here, part(t, FAR_X), -1.0)
        for values in (x, part(t, FAR_Z), part(t, WEIGHT)):
            down[at : at + SLOT_ROWS, :] = values
            at = at + SLOT_ROWS
    for which in (NEAR_Z, NEAR_X, WEIGHT):
        down[at : at + SLOT_ROWS, :] = part(l_ref[0], which)
        at = at + SLOT_ROWS


def emit(l_ref, a8_ref, planes, faces, row_ref, pick_ref, far_x, final=False):
    tiles = a8_ref.shape[0]
    cx = planes.shape[1]
    slots = row_ref.shape[2]
    put_faces(l_ref[0], a8_ref, faces)
    base = FACE_ROWS
    for q in range(2):
        if not final or q == 1:
            near = gather(
                planes[2 * q + 1], picks(slot_row(row_ref, q, NEAR_Z)), rows_hit(slot_row(row_ref, q, NEAR_X), cx)
            )
            near = slot_row(row_ref, q, WEIGHT) * near
            for t in range(tiles):
                put_rows(a8_ref, t, base, near)
            base = base + SLOT_ROWS
        if not final or q == 0:
            for t in range(tiles):
                at = slice(t * slots, (t + 1) * slots)
                far = gather(planes[2 * q], pick_ref[q, :, at], rows_hit(far_x[q : q + 1, at], cx))
                put_rows(a8_ref, t, base, far)
            base = base + SLOT_ROWS


def keep_planes(planes, slab, x):
    last = slab.shape[0] - H - 1
    for n, y in enumerate((H - 1, H, last, last + 1)):
        planes[n, pl.ds(x, 1), :] = slab[y : y + 1, :]


def with_fault(total, fault, x, first=0):
    tiles = y_tiles(total)
    y = lax.broadcasted_iota(jnp.int32, tiles[0].shape, 0)
    last = total.shape[0] + 2 * first - H - 1
    for n, at in enumerate((H - 1, H, last, last + 1)):
        at = at - first
        if 0 <= at < total.shape[0]:
            tiles[at // 8] += jnp.where(y == at % 8, fault[n, pl.ds(x, 1), :], 0.0)
    return jnp.concatenate(tiles, axis=0)


def near_sum(row_ref, q, values, cx):
    return scatter(
        values, picks(slot_row(row_ref, q, NEAR_Z)), rows_hit(slot_row(row_ref, q, NEAR_X), cx)
    )


def weights(l, a8, above, row_ref, pick_ref, far_x, fault):
    tiles = a8.shape[0]
    cx = fault.shape[1]
    slots = row_ref.shape[2]
    here = l.astype(f32)

    def codes(block):
        parts = [block[n : n + 1] for n in range(block.shape[0])]
        count = len(parts) // SLOT_ROWS
        return [
            jnp.concatenate(parts[SLOT_ROWS * n : SLOT_ROWS * (n + 1)], axis=1) for n in range(count)
        ]

    def relayed(t):
        at = BOTH_ROWS + 3 * SLOT_ROWS * t
        return codes(above[at : at + 3 * SLOT_ROWS, :])

    for q in range(2):
        mine = relayed(tiles) if q else codes(a8[l, FACE_ROWS : FACE_ROWS + LIST_ROWS, :])
        for n in range(3):
            row_ref[q, n : n + 1, :] = mine[n]
        far = jnp.zeros((cx, 128), f32)
        for t in range(tiles):
            at = slice(t * slots, (t + 1) * slots)
            if q:
                x, z, weight = relayed(t)
            else:
                table = codes(a8[t, FACE_ROWS : FACE_ROWS + LIST_ROWS, :])
                x = jnp.where(table[FAR_TILE] == here, table[FAR_X], -1.0)
                z, weight = table[FAR_Z], table[WEIGHT]
            pick = picks(z)
            pick_ref[q, :, at] = pick
            far_x[q : q + 1, at] = x
            far = far + scatter(weight, pick, rows_hit(x, cx))
        fault[2 * q] = far
        fault[2 * q + 1] = near_sum(row_ref, q, slot_row(row_ref, q, WEIGHT), cx)


def fault_kernel(final, a8, row_ref, pick_ref, far_x, fault):
    tiles = a8.shape[0]
    cx = fault.shape[1]
    slots = row_ref.shape[2]
    base = FACE_ROWS
    for q in range(2):
        if not final or q == 1:
            far = jnp.zeros((cx, 128), f32)
            for t in range(tiles):
                at = slice(t * slots, (t + 1) * slots)
                values = get_rows(a8, t, base, SLOT_ROWS)
                far = far + scatter(values, pick_ref[q, :, at], rows_hit(far_x[q : q + 1, at], cx))
            fault[2 * q] = far
            base = base + SLOT_ROWS
        if not final or q == 0:
            near = jnp.zeros((1, slots), f32)
            for t in range(tiles):
                near = near + get_rows(a8, t, base, SLOT_ROWS)
            fault[2 * q + 1] = near_sum(row_ref, q, slot_row(row_ref, q, WEIGHT) * near, cx)
            base = base + SLOT_ROWS


def extended(before, after, n, own, x):
    return jnp.concatenate([before[n, x], own, after[n, x]], axis=0)


def side_faces(ky, kz, faces, x):
    ye = ky.shape[0]
    low, high = unpacked(faces, kz, x)
    return (
        harmonic(ky, pltpu.roll(ky, 1, 0)),
        harmonic(ky, pltpu.roll(ky, ye - 1, 0)),
        harmonic(kz, low),
        harmonic(kz, high),
    )


def inverse_of(diag):
    live = diag > 0.0
    return jnp.where(live, 1.0 / jnp.where(live, diag, 1.0), 0.0)


def edge_kernel(l_ref, rhs, acc, perm, before, after, below, above, a8,
                fault, row_ref, pick_ref, far_x, faces, low_edge, high_edge):
    cx = rhs.shape[0]
    l = l_ref[0]
    weights(l, a8, above, row_ref, pick_ref, far_x, fault)
    own = get_faces(l, a8)
    left = lane_iota((8, 128)) < 64
    faces[0:8, :] = jnp.where(left, pltpu.roll(below[8:16, :], 64, 1), own[0:8])
    faces[8:16, :] = own[8:16]
    faces[16:24, :] = jnp.where(left, own[16:24], pltpu.roll(above[8:16, :], 64, 1))

    def slab(n, source, x):
        return extended(before, after, n, source[x], x)

    for edge, x, inner in ((low_edge, 0, 1), (high_edge, cx - 1, cx - 2)):
        kx, kx_inner = slab(2, perm.at[0], x), slab(2, perm.at[0], inner)
        sides = side_faces(slab(3, perm.at[1], x), slab(4, perm.at[2], x), faces[...], x)
        edge[0] = kx
        edge[1] = with_fault(slab(1, acc, x) + harmonic(kx, kx_inner) + sum(sides), fault, x)
        edge[2] = slab(0, rhs, x)


def setup_kernel(rhs, acc, perm, before, after, faces_in, fault,
                 inv, z_out, d_out, tx, tym, typ, tzm, tzp, faces_out, planes):
    cx = rhs.shape[0]

    def ext(n, own, x):
        return extended(before, after, n, own, x)

    def body(x, carry):
        faces, t_low, kx = carry
        nxt = jnp.minimum(x + 1, cx - 1)
        kx_next = ext(2, perm[0, nxt], nxt)
        t_high = harmonic(kx, kx_next)
        ym, yp, zm, zp = side_faces(ext(3, perm[1, x], x), ext(4, perm[2, x], x), faces_in[...], x)
        diag = ext(1, acc[x], x) + t_low + t_high + ym + yp + zm + zp
        inverse = inverse_of(with_fault(diag, fault, x))
        z = inverse * ext(0, rhs[x], x)
        d = z / theta
        inv[x] = inverse
        z_out[x] = z
        d_out[x] = d
        tx[x] = t_low
        tx[x + 1] = t_high
        tym[x] = ym
        typ[x] = yp
        tzm[x] = zm
        tzp[x] = zp
        keep_planes(planes, d, x)
        return pack_faces(faces, y_tiles(d), x), t_high, kx_next

    kx0 = ext(2, perm[0, 0], 0)
    faces, _, _ = lax.fori_loop(0, cx, body, (no_faces(), jnp.zeros_like(kx0), kx0), unroll=4)
    faces_out[...] = jnp.concatenate(faces, axis=0)


def finish_kernel(l_ref, low_own, high_own, low_got, high_got, faces_in, planes_in,
                  row_ref, pick_ref, far_x, *refs):
    inv, z_out, d_out, tx, x_low, x_high, a8_out, planes, slabs, sem = refs[4:]
    cx = planes.shape[1]
    planes[...] = planes_in[...]
    faces = (faces_in[0:8, :], faces_in[8:16, :], faces_in[16:24, :])
    moves = []
    sides = ((low_own, low_got, x_low, 0, 0), (high_own, high_got, x_high, cx - 1, cx))
    for n, (own, got, out, x, at) in enumerate(sides):
        t = harmonic(own[0], got[0])
        inverse = inverse_of(own[1] + t)
        z = inverse * own[2]
        d = z / theta
        out[...] = inverse_of(got[1] + t) * got[2] / theta
        keep_planes(planes, d, x)
        faces = pack_faces(faces, y_tiles(d), x)
        for m, (value, ref, to) in enumerate(((inverse, inv, x), (z, z_out, x), (d, d_out, x), (t, tx, at))):
            slabs[4 * n + m] = value
            moves.append(pltpu.make_async_copy(slabs.at[4 * n + m], ref.at[to], sem.at[4 * n + m]))
            moves[-1].start()
    emit(l_ref, a8_out, planes, faces, row_ref, pick_ref, far_x)
    for move in moves:
        move.wait()


def sweep_kernel(c1, c2, first, last, final, l_ref, d_in, z_in, *refs):
    refs = list(refs)
    corr_in = None if first else refs.pop(0)
    xlow, xhigh, a8, fault, inv, tx, tym, typ, tzm, tzp = refs[:10]
    refs = refs[10:]
    if not last:
        row_ref, pick_ref, far_x = refs[:3]
        refs = refs[3:]
    outs = refs
    if last:
        (corr_out,) = outs
    else:
        d_out, z_out, corr_out, d_first, d_last, a8_out, planes = outs
    cx, ye = d_in.shape[0], d_in.shape[1]
    cy = ye - 2 * H
    faces_in = get_faces(l_ref[0], a8)

    def body(x, carry):
        faces, d_prev, d, t_low = carry
        t_high = tx[x + 1]
        d_next = jnp.where(x == cx - 1, xhigh[...], d_in[jnp.minimum(x + 1, cx - 1)])
        skip = 1 if last else 0
        rows = slice(8 * skip, ye - 8 * skip)
        z_low, z_high = unpacked(faces_in, d, x, skip)
        below, above = pltpu.roll(d, 1, 0)[rows], pltpu.roll(d, ye - 1, 0)[rows]
        flow = t_low[rows] * d_prev[rows] + t_high[rows] * d_next[rows]
        flow = flow + (tym[x, rows, :] * below + typ[x, rows, :] * above)
        flow = flow + (tzm[x, rows, :] * z_low + tzp[x, rows, :] * z_high)
        flow = with_fault(flow, fault, x, 8 * skip)
        z = z_in[x, rows, :] - d[rows] + inv[x, rows, :] * flow
        new = c1 * d[rows] + c2 * z
        own = slice(H - 8 * skip, H - 8 * skip + cy)
        corr_out[x] = (d[H : H + cy] if first else corr_in[x]) + new[own]
        if last:
            return faces, d, d_next, t_high
        d_out[x] = new
        z_out[x] = z
        keep_planes(planes, new, x)
        return pack_faces(faces, y_tiles(new), x), d, d_next, t_high

    init = (no_faces(), xlow[...], d_in[0], tx[0])
    faces, _, _, _ = lax.fori_loop(0, cx, body, init, unroll=4)
    if not last:
        d_first[...] = d_out[0]
        d_last[...] = d_out[cx - 1]
        emit(l_ref, a8_out, planes, faces, row_ref, pick_ref, far_x, final)


VMEM = pl.BlockSpec(memory_space=pltpu.VMEM)
SMEM = pl.BlockSpec(memory_space=pltpu.SMEM)
ANY = pl.BlockSpec(memory_space=pl.ANY)
HBM = pl.BlockSpec(memory_space=pltpu.HBM)
PARAMS = pltpu.CompilerParams(vmem_limit_bytes=24 << 20)


def steps(axis):
    peers = lax.axis_size(axis)
    up = [(i, i + 1) for i in range(peers - 1)]
    return up, [(j, i) for i, j in up]


def local(rhs, accumulation, permeability, nnc_cell, nnc_remote, nnc_mask, nnc_trans):
    cx, cy, cz = rhs.shape
    tiles = lax.axis_size("gz")
    slots = nnc_cell.shape[-1]
    ye = cy + 2 * H
    up_y, down_y = steps("gy")
    up_x, down_x = steps("gx")

    def struct(*shape, dtype=f32):
        return jax.ShapeDtypeStruct(shape, dtype)

    l = lax.axis_index("gz").reshape(1).astype(jnp.int32)
    flats = [a.reshape(1, slots) for a in (nnc_cell, nnc_remote, nnc_mask, nnc_trans)]
    l, *flats = lax.optimization_barrier((l, *flats))
    halo = struct(5, cx, H, cz)
    top, bottom, a8 = pl.pallas_call(
        pack_kernel,
        out_shape=(halo, halo, struct(tiles, FACE_ROWS + LIST_ROWS, cz)),
        in_specs=[SMEM] + [HBM] * 7,
        out_specs=(VMEM,) * 3,
        scratch_shapes=[pltpu.VMEM((cx, cy, cz), f32)]
        + [pltpu.VMEM((1, slots), jnp.int32)] * 3
        + [pltpu.VMEM((1, slots), f32), pltpu.SemaphoreType.DMA((15,))],
    )(l, rhs, accumulation, permeability, *flats)
    before = lax.ppermute(top, "gy", up_y)
    after = lax.ppermute(bottom, "gy", down_y)
    a8 = lax.all_to_all(a8, "gz", 0, 0, tiled=True)
    below, above = pl.pallas_call(
        relay_kernel,
        out_shape=(struct(BOTH_ROWS, cz), struct(BOTH_ROWS + 3 * SLOT_ROWS * (tiles + 1), cz)),
        in_specs=[SMEM, VMEM],
        out_specs=(VMEM,) * 2,
        compiler_params=PARAMS,
    )(l, a8)
    below = lax.ppermute(below, "gy", up_y)
    above = lax.ppermute(above, "gy", down_y)

    big = struct(cx, ye, cz)
    tall = struct(cx + 1, ye, cz)
    edge = struct(ye, cz)
    small = struct(cx, cy, cz)
    sent = struct(tiles, FACE_ROWS + 4 * SLOT_ROWS, cz)
    scratch = [pltpu.VMEM((4, cx, cz), f32)]
    every = tiles * slots
    lists = (struct(2, 8, slots), struct(2, cz, every, dtype=bf16), struct(2, every))
    fault, row, pick, far_x, faces, low_edge, high_edge = pl.pallas_call(
        edge_kernel,
        out_shape=(struct(4, cx, cz),) + lists + (struct(BOTH_ROWS, cz),) + (struct(3, ye, cz),) * 2,
        in_specs=[SMEM] + [VMEM] * 8,
        out_specs=(VMEM,) * 7,
        compiler_params=PARAMS,
    )(l, rhs, accumulation, permeability, before, after, below, above, a8)
    low_got = lax.ppermute(high_edge, "gx", up_x)
    high_got = lax.ppermute(low_edge, "gx", down_x)
    inv, z, d, tx, tym, typ, tzm, tzp, faces, planes = pl.pallas_call(
        setup_kernel,
        out_shape=(big, big, big, tall, big, big, big, big)
        + (struct(BOTH_ROWS, cz), struct(4, cx, cz)),
        in_specs=[VMEM] * 7,
        out_specs=(VMEM,) * 10,
        compiler_params=PARAMS,
    )(rhs, accumulation, permeability, before, after, faces, fault)
    inv, z, d, tx, xlow, xhigh, a8 = pl.pallas_call(
        finish_kernel,
        out_shape=(big, big, big, tall, edge, edge, sent),
        in_specs=[SMEM] + [VMEM] * 9 + [ANY] * 4,
        out_specs=(ANY,) * 4 + (VMEM,) * 3,
        scratch_shapes=scratch + [pltpu.VMEM((8, ye, cz), f32), pltpu.SemaphoreType.DMA((8,))],
        input_output_aliases={10: 0, 11: 1, 12: 2, 13: 3},
        compiler_params=PARAMS,
    )(l, low_edge, high_edge, low_got, high_got, faces, planes, row, pick, far_x, inv, z, d, tx)

    rho = 1.0 / sigma
    corr = None
    for sweep in range(1, SWEEPS):
        first, last = sweep == 1, sweep == SWEEPS - 1
        rho_next = 1.0 / (2.0 * sigma - rho)
        c1, c2 = rho_next * rho, 2.0 * rho_next / delta
        rho = rho_next
        if not first:
            xlow = lax.ppermute(d_last, "gx", up_x)
            xhigh = lax.ppermute(d_first, "gx", down_x)
        a8 = lax.all_to_all(a8, "gz", 0, 0, tiled=True)

        def sums(*refs, final=last):
            fault_kernel(final, *refs)

        fault = pl.pallas_call(
            sums,
            out_shape=struct(4, cx, cz),
            in_specs=[VMEM] * 4,
            out_specs=VMEM,
            compiler_params=PARAMS,
        )(a8, row, pick, far_x)
        args = [l, d, z] + ([] if first else [corr])
        args += [xlow, xhigh, a8, fault, inv, tx, tym, typ, tzm, tzp]
        args += [] if last else [row, pick, far_x]

        final = sweep == SWEEPS - 2
        rows = FACE_ROWS + (2 if final else 4) * SLOT_ROWS
        sent = struct(tiles, rows, cz)

        def kernel(*refs, c1=c1, c2=c2, first=first, last=last, final=final):
            sweep_kernel(c1, c2, first, last, final, *refs)

        out = pl.pallas_call(
            kernel,
            out_shape=small if last else (big, big, small, edge, edge, sent),
            in_specs=[SMEM] + [VMEM] * (len(args) - 1),
            out_specs=VMEM if last else (VMEM,) * 6,
            scratch_shapes=[] if last else scratch,
            compiler_params=PARAMS,
        )(*args)
        if last:
            corr = out
        else:
            d, z, corr, d_first, d_last, a8 = out
    return corr


def solution(mesh):
    split = P("gx", "gy", "gz")
    slots = P("gx", "gy", "gz", None)
    return jax.shard_map(
        local,
        mesh=mesh,
        in_specs=(split, split, P(None, "gx", "gy", "gz"), slots, slots, slots, slots),
        out_specs=split,
        check_vma=False,
    )
```
